32 devices in a mesh: dp: 8 (over y, x, core), tensor: 4 (over z).
Axes of the slice: x: 2, y: 2, z: 4, core: 2. Of those that a mesh axis runs over, the one named last changes fastest.
Arguments:
- inputs: bfloat16 [16384, 768], P(('dp', 'tensor')), may hold values from -6 to 6
- cotangent: bfloat16 [16384, 768], P(('dp', 'tensor')), may hold values from -6 to 6
- attn_w: float32 [3, 768, 768], P(None, 'dp', 'tensor'), may hold values from -2 to 2
- out_w: float32 [768, 768], P('tensor', 'dp'), may hold values from -2 to 2
- glu_w: float32 [2, 768, 3072], P(None, 'dp', 'tensor'), may hold values from -2 to 2
- down_w: float32 [3072, 768], P('tensor', 'dp'), may hold values from -2 to 2
- qv_bias: float32 [2, 768], P(None, ('tensor', 'dp')), may hold values from -3 to 3
- vectors: float32 [6, 768], P(None, 'dp'), may hold values from -2 to 2, as said below
- attn_mom: float32 [2, 3, 768, 768], P(None, None, 'dp', 'tensor'), as said below
- out_mom: float32 [2, 768, 768], P(None, 'tensor', 'dp'), as said below
- glu_mom: float32 [2, 2, 768, 3072], P(None, None, 'dp', 'tensor'), as said below
- down_mom: float32 [2, 3072, 768], P(None, 'tensor', 'dp'), as said below
- qv_mom: float32 [2, 2, 768], P(None, None, ('tensor', 'dp')), as said below
- vector_mom: float32 [2, 6, 768], P(None, None, ('dp', 'tensor')), as said below
Outputs:
- output: bfloat16 [16384, 768], P(('dp', 'tensor'))
- input_grad: float32 [16384, 768], P(('dp', 'tensor'))
- attn_grad: float32 [3, 768, 768], P(None, 'dp', 'tensor')
- out_grad: float32 [768, 768], P('tensor', 'dp')
- glu_grad: float32 [2, 768, 3072], P(None, 'dp', 'tensor')
- down_grad: float32 [3072, 768], P('tensor', 'dp')
- qv_grad: float32 [2, 768], P(None, ('tensor', 'dp'))
- vector_grad: float32 [6, 768], P(None, ('dp', 'tensor'))
- attn_mom_new: float32 [2, 3, 768, 768], P(None, None, 'dp', 'tensor')
- out_mom_new: float32 [2, 768, 768], P(None, 'tensor', 'dp')
- glu_mom_new: float32 [2, 2, 768, 3072], P(None, None, 'dp', 'tensor')
- down_mom_new: float32 [2, 3072, 768], P(None, 'tensor', 'dp')
- qv_mom_new: float32 [2, 2, 768], P(None, None, ('tensor', 'dp'))
- vector_mom_new: float32 [2, 6, 768], P(None, None, ('dp', 'tensor'))
- attn_new: float32 [3, 768, 768], P(None, 'dp', 'tensor')
- out_new: float32 [768, 768], P('tensor', 'dp')
- glu_new: float32 [2, 768, 3072], P(None, 'dp', 'tensor')
- down_new: float32 [3072, 768], P('tensor', 'dp')
- qv_new: float32 [2, 768], P(None, ('tensor', 'dp'))
- vector_new: float32 [6, 768], P(None, ('dp', 'tensor'))
- norm_values: float32 [2, 15], replicated
- ratios: float32 [15], replicated
The draws below stay inside these ranges and needn't reach their ends.
Inputs may be any that keep to these rules, and one draw needn't show every extreme that they name: `vectors`: rows 1 and 4 (the norms' gains) lie within 0.2 to 1.8, the other rows within -2 to 2. `attn_mom`: index 0 of the leading dimension holds first moments, index 1 root mean squares of gradients, which are positive. `out_mom`: index 0 of the leading dimension holds first moments, index 1 root mean squares of gradients, which are positive. `glu_mom`: index 0 of the leading dimension holds first moments, index 1 root mean squares of gradients, which are positive. `down_mom`: index 0 of the leading dimension holds first moments, index 1 root mean squares of gradients, which are positive. `qv_mom`: index 0 of the leading dimension holds first moments, index 1 root mean squares of gradients, which are positive. `vector_mom`: index 0 of the leading dimension holds first moments, index 1 root mean squares of gradients, which are positive.
All inputs are finite; a program needn't handle non-finite values.
Results may differ from the reference program's by a relative error of at most 0.022.
The reference program's roundings to bfloat16 on the way count: a program that leaves them out, or rounds other values in their place, can miss the bound.
Values may be sent and summed in bfloat16 or wider, within the bound.
A program may use at most 128 MiB of HBM per device.

```python
import math
import jax
import jax.numpy as jnp
from jax import lax

D = 768
HEADS = 12
HEAD = 64
FF = 3072
LEN = 2048
BLOCK = 512
TOKENS = 16384
N_DP = 8


def moment_pair(key, array_shape, marker):
    grad_scale = 0.1 * math.sqrt(TOKENS)
    own_key = jax.random.fold_in(key, marker)
    first_key, second_key = jax.random.split(own_key)
    first_part = grad_scale * jnp.clip(jax.random.normal(first_key, array_shape, jnp.float32), -4.0, 4.0)
    second_part = grad_scale * jnp.exp(jax.random.uniform(second_key, array_shape, jnp.float32, -1.0, 1.0))
    return jnp.stack([first_part, second_part])


def ramped_weight(key, array_shape, fan_total, ramp_axis, marker):
    own_key = jax.random.fold_in(key, marker)
    length_val = array_shape[ramp_axis]
    position = jnp.arange(length_val, dtype=jnp.float32) / float(length_val - 1)
    view_shape = [1] * len(array_shape)
    view_shape[ramp_axis] = length_val
    position = position.reshape(view_shape)
    base = jnp.clip(jax.random.normal(own_key, array_shape, jnp.float32), -3.5, 3.5)
    factor = 0.5 + position
    return base * factor * float(fan_total) ** (-0.5)


def draw_attn_w(key, part):
    return ramped_weight(key, (3, D, D), D, 1, 811)


def draw_out_w(key, part):
    return ramped_weight(key, (D, D), D // 16, 1, 823)


def draw_glu_w(key, part):
    return ramped_weight(key, (2, D, FF), D, 1, 829)


def draw_down_w(key, part):
    return ramped_weight(key, (FF, D), FF // 4, 1, 839)


def draw_vectors(key, part):
    own_key = jax.random.fold_in(key, 101)
    values = jnp.clip(0.5 * jax.random.normal(own_key, (6, D), jnp.float32), -2.0, 2.0)
    row_index = jnp.arange(6)[:, None]
    is_gain = (row_index == 1) | (row_index == 4)
    return jnp.where(is_gain, 1.0 + 0.4 * values, values)


def draw_attn_mom(key, part):
    return moment_pair(key, (3, D, D), 211)


def draw_out_mom(key, part):
    return moment_pair(key, (D, D), 307)


def draw_glu_mom(key, part):
    return moment_pair(key, (2, D, FF), 401)


def draw_down_mom(key, part):
    return moment_pair(key, (FF, D), 503)


def draw_qv_mom(key, part):
    return moment_pair(key, (2, D), 601)


def draw_vector_mom(key, part):
    return moment_pair(key, (6, D), 709)


def level_of(rng, shape, shards, low, largest):
    factor_of = 1.0
    for dim, parts in shards:
        heights = jax.random.uniform(jax.random.fold_in(jax.random.fold_in(rng, 6), dim), (parts,), jnp.float32, low / len(shards), largest / len(shards))
        factor_of = factor_of * jnp.repeat(jnp.exp(heights), shape[dim] // parts).reshape((-1,) + (1,) * (len(shape) - 1 - dim))
    return factor_of


def scatter_about(rng, extent, scale, limit, shards=(), kind=jnp.bfloat16):
    entries = scale * jax.random.normal(rng, extent, jnp.float32)
    if shards:
        entries = entries * level_of(rng, extent, shards, -0.22, 0.18)
    return jnp.clip(entries, -limit, limit).astype(kind)


def setup_inputs(seed: int = 0) -> dict:
    keys = jax.random.split(jax.random.key(seed), 15)
    return {
        "inputs": scatter_about(keys[0], (TOKENS, D), 1.0, 6.0, ((0, 32),)),
        "cotangent": scatter_about(keys[1], (TOKENS, D), 1.0, 6.0, ((0, 32),)),
        "attn_w": draw_attn_w(jax.random.fold_in(keys[14], 71), 0),
        "out_w": draw_out_w(jax.random.fold_in(keys[14], 71), 0),
        "glu_w": draw_glu_w(jax.random.fold_in(keys[14], 71), 0),
        "down_w": draw_down_w(jax.random.fold_in(keys[14], 71), 0),
        "qv_bias": scatter_about(keys[6], (2, D), 0.5, 3.0, ((1, 32),), jnp.float32),
        "vectors": draw_vectors(jax.random.fold_in(keys[14], 71), 0),
        "attn_mom": draw_attn_mom(jax.random.fold_in(keys[14], 71), 0),
        "out_mom": draw_out_mom(jax.random.fold_in(keys[14], 71), 0),
        "glu_mom": draw_glu_mom(jax.random.fold_in(keys[14], 71), 0),
        "down_mom": draw_down_mom(jax.random.fold_in(keys[14], 71), 0),
        "qv_mom": draw_qv_mom(jax.random.fold_in(keys[14], 71), 0),
        "vector_mom": draw_vector_mom(jax.random.fold_in(keys[14], 71), 0),
    }


@jax.custom_vjp
def low(v):
    return lax.optimization_barrier(v.astype(jnp.bfloat16)).astype(jnp.float32)

@jax.custom_vjp
def low_back(v):
    return v

def low_keep(v):
    return (low(v), None)

def low_pass(kept, grad):
    return (grad,)

def back_keep(v):
    return (v, None)

def back_low(kept, grad):
    return (low(grad),)
low.defvjp(low_keep, low_pass)
low_back.defvjp(back_keep, back_low)
norm_eps = 1e-06
learn_rate = 0.2
decay_rate = 0.01
moment_eps = 1e-06

def alibi_table(head_total):
    power_two = 2 ** int(math.floor(math.log2(head_total)))
    first_set = [2.0 ** (-8.0 * (j + 1) / power_two) for j in range(power_two)]
    extra_set = [2.0 ** (-4.0 * (2 * j + 1) / power_two) for j in range(head_total - power_two)]
    return jnp.array(first_set + extra_set, jnp.float32)

def matmul(left_op, right_op):
    return jnp.dot(left_op, right_op, precision=lax.Precision.HIGHEST)

def layer_norm(tensor_in, gain_row, shift_row):
    center = tensor_in - lax.optimization_barrier(jnp.mean(tensor_in, axis=-1, keepdims=True))
    spread = lax.optimization_barrier(jnp.mean(center * center, axis=-1, keepdims=True))
    return center * lax.rsqrt(spread + norm_eps) * gain_row + shift_row

def head_attend(members):
    queries, key_rows, value_rows, slope = members
    length = key_rows.shape[0]
    block_rows = min(BLOCK, length)
    amount = length // block_rows

    def one_block(pieces):
        query_block, first_row = pieces
        row_pos = first_row + jnp.arange(block_rows, dtype=jnp.int32)
        col_pos = jnp.arange(length, dtype=jnp.int32)
        distance = jnp.abs(row_pos[:, None] - col_pos[None, :]).astype(jnp.float32)
        scores = low_back(matmul(query_block, key_rows.T) * HEAD ** (-0.5) - slope * distance)
        top_val = lax.optimization_barrier(jnp.max(scores, axis=-1, keepdims=True))
        weights = jnp.exp(scores - top_val)
        soft_weights = weights / lax.optimization_barrier(jnp.sum(weights, axis=-1, keepdims=True))
        return matmul(low(soft_weights), value_rows)
    starts = jnp.arange(amount, dtype=jnp.int32) * block_rows
    outputs = lax.map(jax.checkpoint(one_block), (queries.reshape(amount, block_rows, HEAD), starts))
    return outputs.reshape(length, HEAD)

def forward_pass(params, inputs):
    attn_w, out_w, glu_w, down_w, qv_bias, vectors = [low(p) for p in params]
    length = inputs.shape[0]
    queries = low(low_back(matmul(inputs, attn_w[0]) + qv_bias[0]))
    key_rows = low(low_back(matmul(inputs, attn_w[1])))
    value_rows = low(low_back(matmul(inputs, attn_w[2]) + qv_bias[1]))

    def split_heads(tensor_in):
        return tensor_in.reshape(length, HEADS, HEAD).transpose(1, 0, 2)
    head_out = lax.map(head_attend, (split_heads(queries), split_heads(key_rows), split_heads(value_rows), alibi_table(HEADS)))
    attended = low(low_back(head_out.transpose(1, 0, 2).reshape(length, D)))
    branch_one = low_back(matmul(attended, out_w))
    summed_one = inputs + branch_one + vectors[0]
    normed_one = layer_norm(summed_one, vectors[1], vectors[2])
    normed_low = low(normed_one)
    gate_val = low_back(matmul(normed_low, glu_w[0]))
    up_val = low_back(matmul(normed_low, glu_w[1]))
    hidden = low(jax.nn.gelu(gate_val, approximate=False) * up_val)
    branch_two = low_back(matmul(hidden, down_w))
    summed_two = normed_one + branch_two + vectors[3]
    return layer_norm(summed_two, vectors[4], vectors[5])

def lamb_terms(weight, gradient, moments):
    first_moment = 0.5 * moments[0] + 0.5 * gradient
    root_moment = jnp.sqrt(0.5 * moments[1] * moments[1] + 0.5 * gradient * gradient)
    direction = first_moment / (root_moment + moment_eps) + decay_rate * weight
    return (jnp.stack([first_moment, root_moment]), direction)

def piece_sums(tensor_val, stacked):
    squares = tensor_val * tensor_val
    if stacked:
        return lax.optimization_barrier(jnp.sum(squares.reshape(squares.shape[0], -1), axis=1))
    return jnp.sum(squares).reshape(1)

def reference(inputs, cotangent, attn_w, out_w, glu_w, down_w, qv_bias, vectors, attn_mom, out_mom, glu_mom, down_mom, qv_mom, vector_mom):
    params = (attn_w, out_w, glu_w, down_w, qv_bias, vectors)
    seq_inputs = inputs.astype(jnp.float32).reshape(N_DP, LEN, D)
    seq_cot = cotangent.astype(jnp.float32).reshape(N_DP, LEN, D)

    def one_sequence(running, pieces):
        seq_x, seq_g = pieces
        result, pullback = jax.vjp(forward_pass, params, seq_x)
        param_grads, grad_x = pullback(seq_g)
        running = jax.tree.map(jnp.add, running, param_grads)
        return (running, (result.astype(jnp.bfloat16), grad_x))
    start_sums = jax.tree.map(jnp.zeros_like, params)
    gradients, (outputs, grad_inputs) = lax.scan(one_sequence, start_sums, (seq_inputs, seq_cot))
    moments = (attn_mom, out_mom, glu_mom, down_mom, qv_mom, vector_mom)
    stack_flags = (True, False, True, False, True, True)
    new_moments = []
    directions = []
    for weight, gradient, moment in zip(params, gradients, moments):
        pair, direction = lamb_terms(weight, gradient, moment)
        new_moments.append(pair)
        directions.append(direction)
    weight_sums = jnp.concatenate([piece_sums(w, f) for w, f in zip(params, stack_flags)])
    dir_sums = jnp.concatenate([piece_sums(r, f) for r, f in zip(directions, stack_flags)])
    norm_values = jnp.sqrt(jnp.stack([weight_sums, dir_sums]) + 1e-12)
    ratios = norm_values[0] / norm_values[1]
    new_weights = []
    offset = 0
    for weight, direction, stacked in zip(params, directions, stack_flags):
        amount = weight.shape[0] if stacked else 1
        factor = ratios[offset:offset + amount]
        if stacked:
            factor = factor.reshape((amount,) + (1,) * (weight.ndim - 1))
        else:
            factor = factor[0]
        new_weights.append(weight - learn_rate * factor * direction)
        offset = offset + amount
    return (outputs.reshape(TOKENS, D), grad_inputs.reshape(TOKENS, D), gradients[0], gradients[1], gradients[2], gradients[3], gradients[4], gradients[5], new_moments[0], new_moments[1], new_moments[2], new_moments[3], new_moments[4], new_moments[5], new_weights[0], new_weights[1], new_weights[2], new_weights[3], new_weights[4], new_weights[5], norm_values, ratios)
```

```python
import functools
import math

import jax
import jax.numpy as jnp
import numpy as np
from jax import lax
from jax.experimental import pallas as pl
from jax.experimental.pallas import tpu as pltpu
from jax.sharding import PartitionSpec as P

HEADS = 12
HEAD = 64
BLOCK = 256

norm_eps = 1e-06
learn_rate = 0.2
decay_rate = 0.01
moment_eps = 1e-06

bf16 = jnp.bfloat16
f32 = jnp.float32


def dot(a, b, ca, cb):
    return lax.dot_general(a, b, (((ca,), (cb,)), ((), ())), preferred_element_type=f32)


def slope_parts(head_total):
    power_two = 2 ** int(math.floor(math.log2(head_total)))
    slopes = [2.0 ** (-8.0 * (j + 1) / power_two) for j in range(power_two)]
    slopes += [2.0 ** (-4.0 * (2 * j + 1) / power_two) for j in range(head_total - power_two)]
    rest = np.array(slopes, np.float32)
    parts = []
    for _ in range(3):
        part = rest.astype(bf16).astype(np.float32)
        parts.append(part)
        rest = rest - part
    return np.stack(parts, axis=1)


def layer_norm(tensor_in, gain_row, shift_row):
    center = tensor_in - jnp.mean(tensor_in, axis=-1, keepdims=True)
    spread = jnp.mean(center * center, axis=-1, keepdims=True)
    return center * lax.rsqrt(spread + norm_eps) * gain_row + shift_row


def gated(gate_val, up_val):
    return jax.nn.gelu(gate_val, approximate=False) * up_val


def pos_features(length, parts):
    row = lax.broadcasted_iota(jnp.int32, (length, HEAD), 0)
    lane = lax.broadcasted_iota(jnp.int32, (length, HEAD), 1)
    low = (row & 7).astype(f32)
    high = row.astype(f32) - low
    m1, m2, m3 = parts
    slope_q = jnp.where(lane < 2, m1, jnp.where(lane < 4, m2, m3))
    for_q = jnp.where(lane < 6, slope_q, jnp.where(lane < 9, high, jnp.where(lane < 12, low, 0.0)))
    turn = lane - 6
    slope_k = jnp.where(
        (turn == 0) | (turn == 3), m1, jnp.where((turn == 1) | (turn == 4), m2, m3)
    )
    for_k = jnp.where(
        lane < 6, jnp.where((lane & 1) == 0, high, low), jnp.where(lane < 12, -slope_k, 0.0)
    )
    return for_q, for_k


def key_after_query(block):
    late = lax.broadcasted_iota(jnp.int32, (block, block), 0) - lax.broadcasted_iota(
        jnp.int32, (block, block), 1
    )
    return jnp.maximum(late, 0).astype(f32)


def fwd_kernel(
    parts_ref, qkv_ref, out_ref, lse_ref, q_s, k_s, v_s, corr_s, s_s, *, heads, length, unroll
):
    amount = length // BLOCK
    for h in range(heads):
        for_q, for_k = pos_features(length, [parts_ref[h, i] for i in range(3)])
        base = h * 3 * HEAD
        q = qkv_ref[:, base : base + HEAD].astype(f32) * HEAD**-0.5
        k = qkv_ref[:, base + HEAD : base + 2 * HEAD].astype(f32)
        v = qkv_ref[:, base + 2 * HEAD : base + 3 * HEAD].astype(f32)
        q_s[h, 0] = jnp.concatenate([q, for_q], axis=1).astype(bf16)
        q_s[h, 1] = jnp.concatenate([q, -for_q], axis=1).astype(bf16)
        k_s[h] = jnp.concatenate([k, for_k], axis=1).astype(bf16)
        v_s[h] = v.T.astype(bf16)
    late = key_after_query(BLOCK)

    def head(h, _):
        corr_s[...] = 2.0 * (parts_ref[h, 0] + parts_ref[h, 1] + parts_ref[h, 2]) * late

        def group(g, _):
            for u in range(unroll):
                b = g * unroll + u
                rows = pl.ds(pl.multiple_of(b * BLOCK, BLOCK), BLOCK)
                for c in range(amount):
                    after = (c > b).astype(jnp.int32)
                    keys = slice(c * BLOCK, (c + 1) * BLOCK)
                    s_s[u, keys, :] = dot(k_s[h, keys, :], q_s[h, after, rows, :], 1, 1)
                s_s[u, rows, :] = s_s[u, rows, :] - corr_s[...]
            for u in range(unroll):
                b = g * unroll + u
                rows = pl.ds(pl.multiple_of(b * BLOCK, BLOCK), BLOCK)
                s = s_s[u]
                top = jnp.max(s, axis=0, keepdims=True)
                p = jnp.exp(s - top)
                total = jnp.sum(p, axis=0, keepdims=True)
                o = dot(v_s[h], p.astype(bf16), 1, 0)
                out_ref[h, :, rows] = (o / total).astype(bf16)
                lse_ref[h, :, rows] = top + jnp.log(total)
            return 0

        lax.fori_loop(0, amount // unroll, group, 0)
        return 0

    lax.fori_loop(0, heads, head, 0)


def attention_forward(parts, qkv):
    length = qkv.shape[0]
    heads = qkv.shape[1] // (3 * HEAD)
    unroll = 2
    vmem = pl.BlockSpec(memory_space=pltpu.VMEM)
    work = heads * length * length
    return pl.pallas_call(
        functools.partial(fwd_kernel, heads=heads, length=length, unroll=unroll),
        out_shape=(
            jax.ShapeDtypeStruct((heads, HEAD, length), bf16),
            jax.ShapeDtypeStruct((heads, 1, length), f32),
        ),
        in_specs=[pl.BlockSpec(memory_space=pltpu.SMEM), vmem],
        out_specs=(vmem, vmem),
        scratch_shapes=[
            pltpu.VMEM((heads, 2, length, 128), bf16),
            pltpu.VMEM((heads, length, 128), bf16),
            pltpu.VMEM((heads, HEAD, length), bf16),
            pltpu.VMEM((BLOCK, BLOCK), f32),
            pltpu.VMEM((unroll, length, BLOCK), f32),
        ],
        compiler_params=pltpu.CompilerParams(vmem_limit_bytes=40 * 2**20),
        cost_estimate=pl.CostEstimate(
            flops=16 * work * HEAD, bytes_accessed=4 * qkv.size, transcendentals=work
        ),
        name="attention_forward",
    )(parts, qkv)


def bwd_kernel(
    parts_ref,
    qkv_ref,
    dot_ref,
    ot_ref,
    lse_ref,
    out_ref,
    q_s,
    qn_s,
    k_s,
    kt_s,
    v_s,
    do_s,
    centre_s,
    corr_s,
    s_s,
    dq_s,
    dk_s,
    dv_s,
    *,
    heads,
    length,
    unroll,
):
    amount = length // BLOCK
    for h in range(heads):
        for_q, for_k = pos_features(length, [parts_ref[h, i] for i in range(3)])
        base = h * 3 * HEAD
        q = qkv_ref[:, base : base + HEAD].astype(f32) * HEAD**-0.5
        k = qkv_ref[:, base + HEAD : base + 2 * HEAD].astype(f32)
        v = qkv_ref[:, base + 2 * HEAD : base + 3 * HEAD]
        turned = q.T
        turned_pos = for_q.T
        q_s[h, 0] = jnp.concatenate([turned, turned_pos], axis=0).astype(bf16)
        q_s[h, 1] = jnp.concatenate([turned, -turned_pos], axis=0).astype(bf16)
        qn_s[h] = q.astype(bf16)
        k_s[h] = jnp.concatenate([k, for_k], axis=1).astype(bf16)
        kt_s[h] = k.T.astype(bf16)
        v_s[h] = v
        grad = dot_ref[h].astype(f32)
        do_s[h] = grad.T.astype(bf16)
        centre_s[h] = jnp.sum(grad * ot_ref[h].astype(f32), axis=0, keepdims=True)
    late = key_after_query(BLOCK)

    def head(h, _):
        corr_s[...] = 2.0 * (parts_ref[h, 0] + parts_ref[h, 1] + parts_ref[h, 2]) * late
        dq_s[...] = jnp.zeros_like(dq_s)

        def group(g, _):
            for u in range(unroll):
                c = g * unroll + u
                rows = pl.ds(pl.multiple_of(c * BLOCK, BLOCK), BLOCK)
                keys = k_s[h, rows, :]
                for i in range(amount):
                    after = (i < c).astype(jnp.int32)
                    cols = slice(i * BLOCK, (i + 1) * BLOCK)
                    s_s[u, :, cols] = dot(keys, q_s[h, after, :, cols], 1, 0)
                s_s[u, :, rows] = s_s[u, :, rows] - corr_s[...]
            for u in range(unroll):
                c = g * unroll + u
                rows = pl.ds(pl.multiple_of(c * BLOCK, BLOCK), BLOCK)
                p = jnp.exp(s_s[u] - lse_ref[h])
                dp = dot(v_s[h, rows, :], dot_ref[h], 1, 0)
                dv_s[rows, :] = dot(p.astype(bf16), do_s[h], 1, 0)
                ds = (p * (dp - centre_s[h])).astype(bf16)
                dk_s[rows, :] = dot(ds, qn_s[h], 1, 0)
                dq_s[...] += dot(kt_s[h, :, rows], ds, 1, 0)
            return 0

        lax.fori_loop(0, amount // unroll, group, 0)
        out_ref[h, 0] = (dq_s[...] * HEAD**-0.5).astype(bf16)
        out_ref[h, 1] = dk_s[...].T.astype(bf16)
        out_ref[h, 2] = dv_s[...].T.astype(bf16)
        return 0

    lax.fori_loop(0, heads, head, 0)


def attention_backward(parts, qkv, grad_t, out_t, lse):
    length = qkv.shape[0]
    heads = qkv.shape[1] // (3 * HEAD)
    unroll = 2
    vmem = pl.BlockSpec(memory_space=pltpu.VMEM)
    work = heads * length * length
    return pl.pallas_call(
        functools.partial(bwd_kernel, heads=heads, length=length, unroll=unroll),
        out_shape=jax.ShapeDtypeStruct((heads, 3, HEAD, length), bf16),
        in_specs=[pl.BlockSpec(memory_space=pltpu.SMEM)] + [vmem] * 4,
        out_specs=vmem,
        scratch_shapes=[
            pltpu.VMEM((heads, 2, 128, length), bf16),
            pltpu.VMEM((heads, length, HEAD), bf16),
            pltpu.VMEM((heads, length, 128), bf16),
            pltpu.VMEM((heads, HEAD, length), bf16),
            pltpu.VMEM((heads, length, HEAD), bf16),
            pltpu.VMEM((heads, length, HEAD), bf16),
            pltpu.VMEM((heads, 1, length), f32),
            pltpu.VMEM((BLOCK, BLOCK), f32),
            pltpu.VMEM((unroll, BLOCK, length), f32),
            pltpu.VMEM((HEAD, length), f32),
            pltpu.VMEM((length, HEAD), f32),
            pltpu.VMEM((length, HEAD), f32),
        ],
        compiler_params=pltpu.CompilerParams(vmem_limit_bytes=48 * 2**20),
        cost_estimate=pl.CostEstimate(
            flops=40 * work * HEAD, bytes_accessed=8 * qkv.size, transcendentals=work
        ),
        name="attention_backward",
    )(parts, qkv, grad_t, out_t, lse)


def lamb_terms(weight, gradient, moments):
    first_moment = 0.5 * moments[0] + 0.5 * gradient
    root_moment = jnp.sqrt(0.5 * moments[1] * moments[1] + 0.5 * gradient * gradient)
    direction = first_moment / (root_moment + moment_eps) + decay_rate * weight
    return (jnp.stack([first_moment, root_moment]), direction)


def piece_sums(tensor_val, stacked):
    squares = tensor_val * tensor_val
    if stacked:
        return jnp.sum(squares.reshape(squares.shape[0], -1), axis=1)
    return jnp.sum(squares).reshape(1)


def local(
    inputs,
    cotangent,
    attn_w,
    out_w,
    glu_w,
    down_w,
    qv_bias,
    vectors,
    attn_mom,
    out_mom,
    glu_mom,
    down_mom,
    qv_mom,
    vector_mom,
    *,
    n_dp,
    n_tensor,
):
    tensor_pos = lax.axis_index("tensor")
    rows = attn_w.shape[1]
    head_cols = attn_w.shape[2]
    head_count = head_cols // HEAD
    width = rows * n_dp
    hidden_cols = glu_w.shape[2]
    tokens = inputs.shape[0]
    length = tokens * n_tensor
    qv_cols = qv_bias.shape[1]
    parts = lax.dynamic_slice_in_dim(
        jnp.asarray(slope_parts(HEADS)), tensor_pos * head_count, head_count
    )

    attn_rows = (
        attn_w.astype(bf16)
        .reshape(3, rows, head_count, HEAD)
        .transpose(1, 2, 0, 3)
        .reshape(rows, 3 * head_cols)
    )
    out_rows = out_w.astype(bf16).T
    glu_rows = glu_w.astype(bf16).transpose(1, 0, 2).reshape(rows, 2 * hidden_cols)
    down_rows = down_w.astype(bf16).T

    small = jnp.concatenate(
        [
            vectors.astype(bf16).T,
            jnp.pad(qv_bias.astype(bf16).reshape(-1), (0, rows - 2 * qv_cols)).reshape(rows, 1),
            jnp.zeros((rows, 57), bf16),
        ],
        axis=1,
    )
    own = lax.all_gather(jnp.concatenate([attn_rows, small], axis=1), "dp", axis=0, tiled=True)
    attn_own = own[:, : 3 * head_cols]
    vector_rows = own[:, 3 * head_cols : 3 * head_cols + 6].T.astype(f32)
    qv_rows = (
        own[:, 3 * head_cols + 6]
        .reshape(n_dp, rows)[:, : 2 * qv_cols]
        .reshape(n_dp, 2, qv_cols)
        .transpose(1, 0, 2)
        .reshape(2, head_cols)
        .astype(f32)
    )
    qkv_bias = (
        jnp.stack([qv_rows[0], jnp.zeros_like(qv_rows[0]), qv_rows[1]])
        .reshape(3, head_count, HEAD)
        .transpose(1, 0, 2)
        .reshape(3 * head_cols)
    )
    inputs_full = lax.all_gather(inputs, "tensor", axis=0, tiled=True)

    sizes = (head_cols, 2 * hidden_cols, hidden_cols, 3 * head_cols)
    packed = lax.all_gather(
        jnp.concatenate([out_rows, glu_rows, down_rows, attn_rows], axis=1), "tensor"
    )
    gathered = []
    offset = 0
    for size in sizes:
        mine = packed[:, :, offset : offset + size].transpose(1, 0, 2).reshape(rows, -1)
        gathered.append(lax.all_gather(mine, "dp", axis=0, tiled=True))
        offset += size
    out_all, glu_all, down_all, attn_all = gathered

    qkv = (dot(inputs_full, attn_own, 1, 0) + qkv_bias).astype(bf16)
    out_t, lse = attention_forward(parts, qkv)
    attended = lax.all_to_all(
        out_t.reshape(head_cols, length), "tensor", split_axis=1, concat_axis=0, tiled=True
    )
    summed_one = inputs.astype(f32) + dot(attended, out_all, 0, 1) + vector_rows[0]
    normed_one, norm_one_back = jax.vjp(layer_norm, summed_one, vector_rows[1], vector_rows[2])
    normed_low = normed_one.astype(bf16)
    gate_up = dot(normed_low, glu_all, 1, 0).reshape(tokens, n_tensor, 2, hidden_cols)
    hidden_val, gated_back = jax.vjp(gated, gate_up[:, :, 0], gate_up[:, :, 1])
    hidden = hidden_val.astype(bf16).reshape(tokens, n_tensor * hidden_cols)
    summed_two = normed_one + dot(hidden, down_all, 1, 1) + vector_rows[3]
    output, norm_two_back = jax.vjp(layer_norm, summed_two, vector_rows[4], vector_rows[5])
    grad_two, grad_gain_two, grad_shift_two = norm_two_back(cotangent.astype(f32))
    grad_branch = grad_two.astype(bf16)
    down_grad = dot(grad_branch, hidden, 0, 0).astype(bf16)
    down_part = lax.psum_scatter(down_grad, "dp", scatter_dimension=0, tiled=True)
    grad_hidden = dot(grad_branch, down_all, 1, 0).reshape(tokens, n_tensor, hidden_cols)
    grad_gate, grad_up = gated_back(grad_hidden)
    grad_glu = (
        jnp.stack([grad_gate, grad_up], axis=2)
        .astype(bf16)
        .reshape(tokens, 2 * n_tensor * hidden_cols)
    )
    glu_grad = dot(normed_low, grad_glu, 0, 0).astype(bf16)
    glu_part = lax.psum_scatter(glu_grad, "dp", scatter_dimension=0, tiled=True)
    grad_normed = grad_two + dot(grad_glu, glu_all, 1, 1)
    grad_one, grad_gain_one, grad_shift_one = norm_one_back(grad_normed)
    grad_attn = grad_one.astype(bf16)
    out_grad = dot(grad_attn, attended, 0, 1).astype(bf16)
    out_part = lax.psum_scatter(out_grad, "dp", scatter_dimension=0, tiled=True)
    grad_attended = dot(out_all, grad_attn, 0, 1).astype(bf16)
    vector_part = jnp.stack(
        [
            jnp.sum(grad_one, axis=0),
            grad_gain_one,
            grad_shift_one,
            jnp.sum(grad_two, axis=0),
            grad_gain_two,
            grad_shift_two,
        ]
    )
    vector_all = lax.psum(vector_part, ("dp", "tensor"))
    slice_width = vector_mom.shape[2]
    vector_sum = lax.dynamic_slice_in_dim(
        vector_all, (lax.axis_index("dp") * n_tensor + tensor_pos) * slice_width, slice_width, 1
    )
    late_parts = jnp.concatenate(
        [
            out_part.reshape(rows, n_tensor, head_cols),
            glu_part.reshape(rows, n_tensor, 2 * hidden_cols),
            down_part.reshape(rows, n_tensor, hidden_cols),
        ],
        axis=2,
    )
    late_sum = lax.psum_scatter(late_parts, "tensor", scatter_dimension=1, tiled=True)[:, 0].astype(f32)
    out_sum = late_sum[:, :head_cols].T
    glu_sum = (
        late_sum[:, head_cols : head_cols + 2 * hidden_cols]
        .reshape(rows, 2, hidden_cols)
        .transpose(1, 0, 2)
    )
    down_sum = late_sum[:, head_cols + 2 * hidden_cols :].T

    grad_heads = lax.all_to_all(
        grad_attended, "tensor", split_axis=0, concat_axis=1, tiled=True
    ).reshape(head_count, HEAD, length)
    grad_qkv = attention_backward(parts, qkv, grad_heads, out_t, lse).reshape(3 * head_cols, length)
    attn_grad = dot(inputs_full, grad_qkv, 0, 1)
    qv_grad = jnp.sum(grad_qkv.reshape(head_count, 3, HEAD, length).astype(f32), axis=3)
    qv_grad = jnp.stack([qv_grad[:, 0], qv_grad[:, 2]]).reshape(2, n_dp, qv_cols)
    qv_grad = jnp.pad(
        qv_grad.transpose(1, 0, 2).reshape(n_dp, 2 * qv_cols), ((0, 0), (0, rows - 2 * qv_cols))
    ).reshape(width, 1)
    attn_part = jnp.concatenate([attn_grad, qv_grad, jnp.zeros((width, 63), f32)], axis=1)
    attn_part = lax.psum_scatter(attn_part.astype(bf16), "dp", scatter_dimension=0, tiled=True)
    attn_part = attn_part.astype(f32)
    attn_sum = (
        attn_part[:, : 3 * head_cols]
        .reshape(rows, head_count, 3, HEAD)
        .transpose(2, 0, 1, 3)
        .reshape(3, rows, head_cols)
    )
    qv_sum = attn_part[: 2 * qv_cols, 3 * head_cols].reshape(2, qv_cols)

    grad_tokens = lax.all_to_all(grad_qkv, "tensor", split_axis=1, concat_axis=0, tiled=True)
    input_grad = grad_one + dot(grad_tokens, attn_all, 0, 1)

    vector_own = lax.dynamic_slice_in_dim(vectors, tensor_pos * slice_width, slice_width, 1)
    owned_parts = (attn_w, out_w, glu_w, down_w, qv_bias, vector_own)
    gradients = (attn_sum, out_sum, glu_sum, down_sum, qv_sum, vector_sum)
    moments = (attn_mom, out_mom, glu_mom, down_mom, qv_mom, vector_mom)
    stack_flags = (True, False, True, False, True, True)
    new_moments = []
    directions = []
    for weight, gradient, moment in zip(owned_parts, gradients, moments):
        pair, direction = lamb_terms(weight, gradient, moment)
        new_moments.append(pair)
        directions.append(direction)
    weight_sums = jnp.concatenate([piece_sums(w, f) for w, f in zip(owned_parts, stack_flags)])
    dir_sums = jnp.concatenate([piece_sums(r, f) for r, f in zip(directions, stack_flags)])
    totals = lax.psum(jnp.stack([weight_sums, dir_sums]), ("dp", "tensor"))
    norm_values = jnp.sqrt(totals + 1e-12)
    ratios = norm_values[0] / norm_values[1]
    new_weights = []
    offset = 0
    for weight, direction, stacked in zip(owned_parts, directions, stack_flags):
        amount = weight.shape[0] if stacked else 1
        factor = ratios[offset : offset + amount]
        if stacked:
            factor = factor.reshape((amount,) + (1,) * (weight.ndim - 1))
        else:
            factor = factor[0]
        new_weights.append(weight - learn_rate * factor * direction)
        offset = offset + amount
    return (
        output.astype(bf16),
        input_grad,
        *gradients,
        *new_moments,
        *new_weights,
        norm_values,
        ratios,
    )


def solution(mesh):
    tokens = P(("dp", "tensor"), None)
    attn = P(None, "dp", "tensor")
    cols = P("tensor", "dp")
    moments = (
        P(None, None, "dp", "tensor"),
        P(None, "tensor", "dp"),
        P(None, None, "dp", "tensor"),
        P(None, "tensor", "dp"),
        P(None, None, ("tensor", "dp")),
        P(None, None, ("dp", "tensor")),
    )
    weights = (attn, cols, attn, cols, P(None, ("tensor", "dp")))
    split = P(None, ("dp", "tensor"))
    return jax.shard_map(
        functools.partial(local, n_dp=mesh.shape["dp"], n_tensor=mesh.shape["tensor"]),
        mesh=mesh,
        in_specs=(tokens, tokens, *weights, P(None, "dp"), *moments),
        out_specs=(tokens, tokens, *weights, split, *moments, *weights, split, P(), P()),
        check_vma=False,
    )
```

```python
import functools
import math

import jax
import jax.numpy as jnp
import numpy as np
from jax import lax
from jax.experimental import pallas as pl
from jax.experimental.pallas import tpu as pltpu
from jax.sharding import PartitionSpec as P


HEADS = 12
HEAD = 64
BLOCK = 256

norm_eps = 1e-06
learn_rate = 0.2
decay_rate = 0.01
moment_eps = 1e-06


bf16 = jnp.bfloat16
f32 = jnp.float32


def dot(a, b, ca, cb):
    return lax.dot_general(a, b, (((ca,), (cb,)), ((), ())), preferred_element_type=f32)


def slope_parts(head_total):
    power_two = 2 ** int(math.floor(math.log2(head_total)))
    slopes = [2.0 ** (-8.0 * (j + 1) / power_two) for j in range(power_two)]
    slopes += [2.0 ** (-4.0 * (2 * j + 1) / power_two) for j in range(head_total - power_two)]
    rest = np.array(slopes, np.float32)
    parts = []
    for _ in range(3):
        part = rest.astype(bf16).astype(np.float32)
        parts.append(part)
        rest = rest - part
    return np.stack(parts, axis=1)


def pos_features(length, parts):
    row = lax.broadcasted_iota(jnp.int32, (length, HEAD), 0)
    lane = lax.broadcasted_iota(jnp.int32, (length, HEAD), 1)
    low = (row & 7).astype(f32)
    high = row.astype(f32) - low
    m1, m2, m3 = parts
    slope_q = jnp.where(lane < 2, m1, jnp.where(lane < 4, m2, m3))
    for_q = jnp.where(lane < 6, slope_q, jnp.where(lane < 9, high, jnp.where(lane < 12, low, 0.0)))
    turn = lane - 6
    slope_k = jnp.where(
        (turn == 0) | (turn == 3), m1, jnp.where((turn == 1) | (turn == 4), m2, m3)
    )
    for_k = jnp.where(
        lane < 6, jnp.where((lane & 1) == 0, high, low), jnp.where(lane < 12, -slope_k, 0.0)
    )
    return for_q, for_k


def key_after_query(block):
    late = lax.broadcasted_iota(jnp.int32, (block, block), 0) - lax.broadcasted_iota(
        jnp.int32, (block, block), 1
    )
    return jnp.maximum(late, 0).astype(f32)


def fwd_kernel(
    parts_ref, qkv_ref, out_ref, lse_ref, q_s, k_s, v_s, corr_s, s_s, *, heads, length, unroll
):
    amount = length // BLOCK
    for h in range(heads):
        for_q, for_k = pos_features(length, [parts_ref[h, i] for i in range(3)])
        base = h * 3 * HEAD
        q = qkv_ref[:, base : base + HEAD].astype(f32) * HEAD**-0.5
        k = qkv_ref[:, base + HEAD : base + 2 * HEAD].astype(f32)
        v = qkv_ref[:, base + 2 * HEAD : base + 3 * HEAD].astype(f32)
        q_s[h, 0] = jnp.concatenate([q, for_q], axis=1).astype(bf16)
        q_s[h, 1] = jnp.concatenate([q, -for_q], axis=1).astype(bf16)
        k_s[h] = jnp.concatenate([k, for_k], axis=1).astype(bf16)
        v_s[h] = v.T.astype(bf16)
    late = key_after_query(BLOCK)

    def head(h, _):
        corr_s[...] = 2.0 * (parts_ref[h, 0] + parts_ref[h, 1] + parts_ref[h, 2]) * late

        def group(g, _):
            for u in range(unroll):
                b = g * unroll + u
                rows = pl.ds(pl.multiple_of(b * BLOCK, BLOCK), BLOCK)
                for c in range(amount):
                    after = (c > b).astype(jnp.int32)
                    keys = slice(c * BLOCK, (c + 1) * BLOCK)
                    s_s[u, keys, :] = dot(k_s[h, keys, :], q_s[h, after, rows, :], 1, 1)
                s_s[u, rows, :] = s_s[u, rows, :] - corr_s[...]
            for u in range(unroll):
                b = g * unroll + u
                rows = pl.ds(pl.multiple_of(b * BLOCK, BLOCK), BLOCK)
                s = s_s[u]
                top = jnp.max(s, axis=0, keepdims=True)
                p = jnp.exp(s - top)
                total = jnp.sum(p, axis=0, keepdims=True)
                o = dot(v_s[h], p.astype(bf16), 1, 0)
                out_ref[h, :, rows] = (o / total).astype(bf16)
                lse_ref[h, :, rows] = top + jnp.log(total)
            return 0

        lax.fori_loop(0, amount // unroll, group, 0)
        return 0

    lax.fori_loop(0, heads, head, 0)


def attention_forward(parts, qkv):
    length = qkv.shape[0]
    heads = qkv.shape[1] // (3 * HEAD)
    unroll = 2
    vmem = pl.BlockSpec(memory_space=pltpu.VMEM)
    work = heads * length * length
    return pl.pallas_call(
        functools.partial(fwd_kernel, heads=heads, length=length, unroll=unroll),
        out_shape=(
            jax.ShapeDtypeStruct((heads, HEAD, length), bf16),
            jax.ShapeDtypeStruct((heads, 1, length), f32),
        ),
        in_specs=[pl.BlockSpec(memory_space=pltpu.SMEM), vmem],
        out_specs=(vmem, vmem),
        scratch_shapes=[
            pltpu.VMEM((heads, 2, length, 128), bf16),
            pltpu.VMEM((heads, length, 128), bf16),
            pltpu.VMEM((heads, HEAD, length), bf16),
            pltpu.VMEM((BLOCK, BLOCK), f32),
            pltpu.VMEM((unroll, length, BLOCK), f32),
        ],
        compiler_params=pltpu.CompilerParams(vmem_limit_bytes=40 * 2**20),
        cost_estimate=pl.CostEstimate(
            flops=16 * work * HEAD, bytes_accessed=4 * qkv.size, transcendentals=work
        ),
        name="attention_forward",
    )(parts, qkv)


def bwd_kernel(
    parts_ref,
    qkv_ref,
    dot_ref,
    ot_ref,
    lse_ref,
    out_ref,
    q_s,
    qn_s,
    k_s,
    kt_s,
    v_s,
    do_s,
    centre_s,
    corr_s,
    s_s,
    dq_s,
    dk_s,
    dv_s,
    *,
    heads,
    length,
    unroll,
):
    amount = length // BLOCK
    for h in range(heads):
        for_q, for_k = pos_features(length, [parts_ref[h, i] for i in range(3)])
        base = h * 3 * HEAD
        q = qkv_ref[:, base : base + HEAD].astype(f32) * HEAD**-0.5
        k = qkv_ref[:, base + HEAD : base + 2 * HEAD].astype(f32)
        v = qkv_ref[:, base + 2 * HEAD : base + 3 * HEAD]
        turned = q.T
        turned_pos = for_q.T
        q_s[h, 0] = jnp.concatenate([turned, turned_pos], axis=0).astype(bf16)
        q_s[h, 1] = jnp.concatenate([turned, -turned_pos], axis=0).astype(bf16)
        qn_s[h] = q.astype(bf16)
        k_s[h] = jnp.concatenate([k, for_k], axis=1).astype(bf16)
        kt_s[h] = k.T.astype(bf16)
        v_s[h] = v
        grad = dot_ref[h].astype(f32)
        do_s[h] = grad.T.astype(bf16)
        centre_s[h] = jnp.sum(grad * ot_ref[h].astype(f32), axis=0, keepdims=True)
    late = key_after_query(BLOCK)

    def head(h, _):
        corr_s[...] = 2.0 * (parts_ref[h, 0] + parts_ref[h, 1] + parts_ref[h, 2]) * late
        dq_s[...] = jnp.zeros_like(dq_s)

        def group(g, _):
            for u in range(unroll):
                c = g * unroll + u
                rows = pl.ds(pl.multiple_of(c * BLOCK, BLOCK), BLOCK)
                keys = k_s[h, rows, :]
                for i in range(amount):
                    after = (i < c).astype(jnp.int32)
                    cols = slice(i * BLOCK, (i + 1) * BLOCK)
                    s_s[u, :, cols] = dot(keys, q_s[h, after, :, cols], 1, 0)
                s_s[u, :, rows] = s_s[u, :, rows] - corr_s[...]
            for u in range(unroll):
                c = g * unroll + u
                rows = pl.ds(pl.multiple_of(c * BLOCK, BLOCK), BLOCK)
                p = jnp.exp(s_s[u] - lse_ref[h])
                dp = dot(v_s[h, rows, :], dot_ref[h], 1, 0)
                dv_s[rows, :] = dot(p.astype(bf16), do_s[h], 1, 0)
                ds = (p * (dp - centre_s[h])).astype(bf16)
                dk_s[rows, :] = dot(ds, qn_s[h], 1, 0)
                dq_s[...] += dot(kt_s[h, :, rows], ds, 1, 0)
            return 0

        lax.fori_loop(0, amount // unroll, group, 0)
        out_ref[h, 0] = (dq_s[...] * HEAD**-0.5).astype(bf16)
        out_ref[h, 1] = dk_s[...].T.astype(bf16)
        out_ref[h, 2] = dv_s[...].T.astype(bf16)
        return 0

    lax.fori_loop(0, heads, head, 0)


def attention_backward(parts, qkv, grad_t, out_t, lse):
    length = qkv.shape[0]
    heads = qkv.shape[1] // (3 * HEAD)
    unroll = 2
    vmem = pl.BlockSpec(memory_space=pltpu.VMEM)
    work = heads * length * length
    return pl.pallas_call(
        functools.partial(bwd_kernel, heads=heads, length=length, unroll=unroll),
        out_shape=jax.ShapeDtypeStruct((heads, 3, HEAD, length), bf16),
        in_specs=[pl.BlockSpec(memory_space=pltpu.SMEM)] + [vmem] * 4,
        out_specs=vmem,
        scratch_shapes=[
            pltpu.VMEM((heads, 2, 128, length), bf16),
            pltpu.VMEM((heads, length, HEAD), bf16),
            pltpu.VMEM((heads, length, 128), bf16),
            pltpu.VMEM((heads, HEAD, length), bf16),
            pltpu.VMEM((heads, length, HEAD), bf16),
            pltpu.VMEM((heads, length, HEAD), bf16),
            pltpu.VMEM((heads, 1, length), f32),
            pltpu.VMEM((BLOCK, BLOCK), f32),
            pltpu.VMEM((unroll, BLOCK, length), f32),
            pltpu.VMEM((HEAD, length), f32),
            pltpu.VMEM((length, HEAD), f32),
            pltpu.VMEM((length, HEAD), f32),
        ],
        compiler_params=pltpu.CompilerParams(vmem_limit_bytes=48 * 2**20),
        cost_estimate=pl.CostEstimate(
            flops=40 * work * HEAD, bytes_accessed=8 * qkv.size, transcendentals=work
        ),
        name="attention_backward",
    )(parts, qkv, grad_t, out_t, lse)


def normed(z):
    center = z - jnp.mean(z, axis=1, keepdims=True)
    scale = lax.rsqrt(jnp.mean(center * center, axis=1, keepdims=True) + norm_eps)
    return center * scale, scale


def norm_back(grad, unit, scale, gain):
    inner = grad * gain
    mean = jnp.mean(inner, axis=1, keepdims=True)
    return scale * (inner - mean - unit * jnp.mean(inner * unit, axis=1, keepdims=True))


def ff_kernel(
    att_ref,
    x_ref,
    cot_ref,
    vec_ref,
    wall_ref,
    out_ref,
    dz1_ref,
    do_ref,
    dvec_ref,
    gglu_ref,
    grest_ref,
    wgu_s,
    wd_s,
    wo_s,
    act_s,
    der_s,
    hid_s,
    atn_s,
    h1_s,
    x1_s,
    h1r_s,
    h1t_s,
    df_s,
    dft_s,
    acc_s,
    sglu_s,
    sdown_s,
    sout_s,
    load_sem,
    store_sem,
    *,
    head_cols,
    hid_cols,
):
    n_row, n_t, rows = wall_ref.shape[:3]
    width = h1_s.shape[1]
    pad = wo_s.shape[2]
    sizes = (2 * hid_cols, hid_cols, pad)

    def loads(kind, t):
        into = (wgu_s, wd_s, wo_s)[kind]
        low = sum(sizes[:kind])
        return [
            pltpu.make_async_copy(
                wall_ref.at[p, t, :, pl.ds(low, sizes[kind])],
                into.at[t, pl.ds(p * rows, rows), :],
                load_sem.at[kind, t, p],
            )
            for p in range(n_row)
        ]

    def stores(kind, t):
        source = (sglu_s, sdown_s, sout_s)[kind]
        into = (gglu_ref, grest_ref, grest_ref)[kind]
        low = (0, 0, hid_cols)[kind]
        return [
            pltpu.make_async_copy(
                source.at[pl.ds(p * rows, rows), :],
                into.at[p, t, :, pl.ds(low, sizes[kind])],
                store_sem.at[kind, p],
            )
            for p in range(n_row)
        ]

    for kind in (2, 0, 1):
        for t in range(n_t):
            for copy in loads(kind, t):
                copy.start()
    for t in range(n_t):
        atn_s[t] = att_ref[t * head_cols : (t + 1) * head_cols, :].astype(f32).T.astype(bf16)
        for copy in loads(2, t):
            copy.wait()
    branch = jnp.zeros_like(acc_s)
    for t in range(n_t):
        branch = branch + dot(atn_s[t], wo_s[t, :, :head_cols], 1, 1)
    x1, r1 = normed(x_ref[...].astype(f32) + branch + vec_ref[0:1, :])
    x1_s[...] = x1
    h1 = x1 * vec_ref[1:2, :] + vec_ref[2:3, :]
    h1_s[...] = h1
    h1r_s[...] = h1.astype(bf16)
    h1t_s[...] = h1.T.astype(bf16)
    acc_s[...] = jnp.zeros_like(acc_s)
    for kind in (0, 1):
        for t in range(n_t):
            for copy in loads(kind, t):
                copy.wait()

    def forward(t, _):
        g = dot(h1r_s[...], wgu_s[t, :, :hid_cols], 1, 0)
        u = dot(h1r_s[...], wgu_s[t, :, hid_cols:], 1, 0)
        below = 0.5 * (1.0 + lax.erf(g * np.float32(math.sqrt(0.5))))
        dense = jnp.exp(-0.5 * g * g) * np.float32(1.0 / math.sqrt(2.0 * math.pi))
        act = g * below
        act_s[t] = act
        der_s[t] = u * (below + g * dense)
        hidden = (act * u).astype(bf16)
        hid_s[t] = hidden
        acc_s[...] += dot(hidden, wd_s[t], 1, 1)
        return 0

    lax.fori_loop(0, n_t, forward, 0)
    x2, r2 = normed(h1_s[...] + acc_s[...] + vec_ref[3:4, :])
    out_ref[...] = (x2 * vec_ref[4:5, :] + vec_ref[5:6, :]).astype(bf16)
    cot = cot_ref[...].astype(f32)
    dz2 = norm_back(cot, x2, r2, vec_ref[4:5, :])
    dvec_ref[3:4, :] = jnp.sum(dz2, axis=0, keepdims=True)
    dvec_ref[4:5, :] = jnp.sum(cot * x2, axis=0, keepdims=True)
    dvec_ref[5:6, :] = jnp.sum(cot, axis=0, keepdims=True)
    df_s[...] = dz2.astype(bf16)
    dft_s[...] = dz2.T.astype(bf16)
    acc_s[...] = dz2

    def backward(t, _):
        def waits(kind):
            @pl.when(t > 0)
            def _():
                for copy in stores(kind, t - 1):
                    copy.wait()

        waits(1)
        sdown_s[...] = dot(dft_s[...], hid_s[t], 1, 0).astype(bf16)
        for copy in stores(1, t):
            copy.start()
        dh = dot(df_s[...], wd_s[t], 1, 0)
        dg = (dh * der_s[t]).astype(bf16)
        du = (dh * act_s[t]).astype(bf16)
        acc_s[...] += dot(dg, wgu_s[t, :, :hid_cols], 1, 1) + dot(du, wgu_s[t, :, hid_cols:], 1, 1)
        waits(0)
        sglu_s[:, :hid_cols] = dot(h1t_s[...], dg, 1, 0).astype(bf16)
        sglu_s[:, hid_cols:] = dot(h1t_s[...], du, 1, 0).astype(bf16)
        for copy in stores(0, t):
            copy.start()
        return 0

    lax.fori_loop(0, n_t, backward, 0)
    dh1 = acc_s[...]
    x1 = x1_s[...]
    dz1 = norm_back(dh1, x1, r1, vec_ref[1:2, :])
    dvec_ref[0:1, :] = jnp.sum(dz1, axis=0, keepdims=True)
    dvec_ref[1:2, :] = jnp.sum(dh1 * x1, axis=0, keepdims=True)
    dvec_ref[2:3, :] = jnp.sum(dh1, axis=0, keepdims=True)
    dvec_ref[6:8, :] = jnp.zeros((2, width), f32)
    dz1_ref[...] = dz1
    da = dz1.astype(bf16)
    dat = dz1.T.astype(bf16)
    sout_s[...] = jnp.zeros_like(sout_s)
    for t in range(n_t):
        do_ref[t * head_cols : (t + 1) * head_cols, :] = dot(
            da, wo_s[t, :, :head_cols], 1, 0
        ).T.astype(bf16)
        if t > 0:
            for copy in stores(2, t - 1):
                copy.wait()
        sout_s[:, :head_cols] = dot(dat, atn_s[t], 1, 0).astype(bf16)
        for copy in stores(2, t):
            copy.start()
    for kind in range(3):
        for copy in stores(kind, n_t - 1):
            copy.wait()


def feed_forward(attended, inputs, cotangent, vector_rows, wall, head_cols, hid_cols):
    tokens, width = inputs.shape
    n_row, n_t, rows = wall.shape[:3]
    pad = wall.shape[3] - 3 * hid_cols
    vmem = pl.BlockSpec(memory_space=pltpu.VMEM)
    hbm = pl.BlockSpec(memory_space=pl.ANY)
    shape = jax.ShapeDtypeStruct
    size = tokens * width * n_t
    return pl.pallas_call(
        functools.partial(ff_kernel, head_cols=head_cols, hid_cols=hid_cols),
        out_shape=(
            shape((tokens, width), bf16),
            shape((tokens, width), f32),
            shape((n_t * head_cols, tokens), bf16),
            shape((8, width), f32),
            shape((n_row, n_t, rows, 2 * hid_cols), bf16),
            shape((n_row, n_t, rows, hid_cols + pad), bf16),
        ),
        in_specs=[vmem] * 4 + [hbm],
        out_specs=(vmem, vmem, vmem, vmem, hbm, hbm),
        scratch_shapes=[
            pltpu.VMEM((n_t, width, 2 * hid_cols), bf16),
            pltpu.VMEM((n_t, width, hid_cols), bf16),
            pltpu.VMEM((n_t, width, pad), bf16),
            pltpu.VMEM((n_t, tokens, hid_cols), f32),
            pltpu.VMEM((n_t, tokens, hid_cols), f32),
            pltpu.VMEM((n_t, tokens, hid_cols), bf16),
            pltpu.VMEM((n_t, tokens, head_cols), bf16),
            pltpu.VMEM((tokens, width), f32),
            pltpu.VMEM((tokens, width), f32),
            pltpu.VMEM((tokens, width), bf16),
            pltpu.VMEM((width, tokens), bf16),
            pltpu.VMEM((tokens, width), bf16),
            pltpu.VMEM((width, tokens), bf16),
            pltpu.VMEM((tokens, width), f32),
            pltpu.VMEM((width, 2 * hid_cols), bf16),
            pltpu.VMEM((width, hid_cols), bf16),
            pltpu.VMEM((width, pad), bf16),
            pltpu.SemaphoreType.DMA((3, n_t, n_row)),
            pltpu.SemaphoreType.DMA((3, n_row)),
        ],
        compiler_params=pltpu.CompilerParams(vmem_limit_bytes=63 * 2**20),
        cost_estimate=pl.CostEstimate(
            flops=6 * size * (3 * hid_cols + head_cols),
            bytes_accessed=4 * wall.size,
            transcendentals=2 * tokens * n_t * hid_cols,
        ),
        name="feed_forward",
    )(attended, inputs, cotangent, vector_rows, wall)


def on(axis, place):
    return {"device_id": {axis: place}, "device_id_type": pl.DeviceIdType.MESH}


def meet_all(barrier, axis, size):
    place = lax.axis_index(axis)

    def tell(k, _):
        pl.semaphore_signal(barrier, inc=1, **on(axis, lax.rem(place + k, size)))
        return 0

    lax.fori_loop(1, size, tell, 0)


def gather_kernel(*refs, n_chain, n_flat, chain, flat):
    ins, refs = refs[: n_chain + n_flat], refs[n_chain + n_flat :]
    outs, refs = refs[: n_chain + n_flat], refs[n_chain + n_flat :]
    send_sem, recv_sem, local_sem, flat_send, flat_recv = refs
    z = lax.axis_index("tensor")
    p = lax.axis_index("dp")
    barrier = pltpu.get_barrier_semaphore()

    @pl.when(z > 0)
    def _():
        pl.semaphore_signal(barrier, inc=1, **on("tensor", z - 1))

    @pl.when(z < chain - 1)
    def _():
        pl.semaphore_signal(barrier, inc=1, **on("tensor", z + 1))

    met = jnp.where(z > 0, 1, 0) + jnp.where(z < chain - 1, 1, 0)
    if n_flat:
        meet_all(barrier, "dp", flat)
        met = met + flat - 1
    pl.semaphore_wait(barrier, met)

    own = []
    for i in range(n_chain):
        own.append(pltpu.make_async_copy(ins[i], outs[i].at[z], local_sem.at[i]))
    for j in range(n_flat):
        i = n_chain + j
        own.append(pltpu.make_async_copy(ins[i], outs[i].at[p], local_sem.at[i]))

        def push(k, _):
            pltpu.make_async_remote_copy(
                ins[i],
                outs[i].at[p],
                flat_send.at[j, k],
                flat_recv.at[j, p],
                **on("dp", lax.rem(p + k, flat)),
            ).start()
            return 0

        lax.fori_loop(1, flat, push, 0)
    for copy in own:
        copy.start()

    def hop(i, way, step):
        block = z - step if way == 0 else z + step
        target = z + 1 if way == 0 else z - 1
        return pltpu.make_async_remote_copy(
            ins[i] if step == 0 else outs[i].at[block],
            outs[i].at[block],
            send_sem.at[i, way, step],
            recv_sem.at[i, block],
            **on("tensor", target),
        )

    def sends(way, step):
        if way == 0:
            return (z < chain - 1) & (z >= step)
        return (z > 0) & (z + step < chain)

    def arrived(i, block):
        pltpu.make_async_remote_copy(
            outs[i].at[block],
            outs[i].at[block],
            send_sem.at[i, 0, 0],
            recv_sem.at[i, block],
            **on("tensor", lax.rem(z + 1, chain)),
        ).wait_recv()

    for i in range(n_chain):
        for step in range(chain - 1):
            for way in range(2):

                @pl.when(sends(way, step))
                def _():
                    if step > 0:
                        arrived(i, z - step if way == 0 else z + step)
                    hop(i, way, step).start()

    for i in range(n_chain):
        for step in range(1, chain):

            @pl.when((z == chain - 1) & (z >= step))
            def _():
                arrived(i, z - step)

            @pl.when((z == 0) & (z + step < chain))
            def _():
                arrived(i, z + step)

        for step in range(chain - 1):
            for way in range(2):

                @pl.when(sends(way, step))
                def _():
                    hop(i, way, step).wait_send()

    for j in range(n_flat):
        i = n_chain + j

        def finish(k, _):
            q = lax.rem(p + k, flat)
            copy = pltpu.make_async_remote_copy(
                ins[i], outs[i].at[q], flat_send.at[j, k], flat_recv.at[j, q], **on("dp", q)
            )
            copy.wait_send()
            copy.wait_recv()
            return 0

        lax.fori_loop(1, flat, finish, 0)
    for copy in own:
        copy.wait()


def gather_blocks(on_chain, to_all, n_tensor, n_dp, call_id):
    arrays = [*on_chain, *to_all]
    sizes = [n_tensor] * len(on_chain) + [n_dp] * len(to_all)
    vmem = pl.BlockSpec(memory_space=pltpu.VMEM)
    hbm = pl.BlockSpec(memory_space=pl.ANY)
    count = len(arrays)
    dma = pltpu.SemaphoreType.DMA
    return pl.pallas_call(
        functools.partial(
            gather_kernel, n_chain=len(on_chain), n_flat=len(to_all), chain=n_tensor, flat=n_dp
        ),
        out_shape=[jax.ShapeDtypeStruct((n,) + a.shape, a.dtype) for n, a in zip(sizes, arrays)],
        in_specs=[vmem] * count,
        out_specs=[hbm] * count,
        scratch_shapes=[
            dma((count, 2, n_tensor)),
            dma((count, n_tensor)),
            dma((count,)),
            dma((max(len(to_all), 1), n_dp)),
            dma((max(len(to_all), 1), n_dp)),
        ],
        compiler_params=pltpu.CompilerParams(collective_id=call_id, has_side_effects=True),
    )(*arrays)


def collect_kernel(*refs, ops, sizes):
    count = len(ops)
    ins, outs, refs = refs[:count], refs[count : 2 * count], refs[2 * count :]
    sums = [i for i, (kind, _) in enumerate(ops) if kind == "sum"]
    got = dict(zip(sums, refs))
    send_sem, recv_sem, local_sem = refs[len(sums) :]
    barrier = pltpu.get_barrier_semaphore()
    axes = sorted({axis for _, axis in ops})
    for axis in axes:
        meet_all(barrier, axis, sizes[axis])
    pl.semaphore_wait(barrier, sum(sizes[axis] - 1 for axis in axes))

    def cut_lanes(ref, index, size):
        lanes = ref.shape[1] // size
        return ref.at[:, pl.ds(pl.multiple_of(index * lanes, 128), lanes)]

    def cut_rows(ref, index, size):
        rows = ref.shape[0] // size
        return ref.at[pl.ds(pl.multiple_of(index * rows, 16), rows), :]

    def cuts(i, source, target):
        kind, axis = ops[i]
        size = sizes[axis]
        if kind == "rows":
            return cut_lanes(ins[i], source, size), cut_rows(outs[i], target, size)
        if kind == "lanes":
            return cut_rows(ins[i], source, size), cut_lanes(outs[i], target, size)
        return ins[i].at[source], got[i].at[target]

    def copy(i, k, landing):
        axis = ops[i][1]
        d = lax.rem(lax.axis_index(axis) + k, sizes[axis])
        place = d if landing is None else landing
        source, target = cuts(i, d, place)
        return pltpu.make_async_remote_copy(
            source, target, send_sem.at[i, k], recv_sem.at[i, place], **on(axis, d)
        )

    def own(i):
        z = lax.axis_index(ops[i][1])
        return pltpu.make_async_copy(*cuts(i, z, z), local_sem.at[i])

    for i, (kind, axis) in enumerate(ops):

        def push(k, _):
            copy(i, k, lax.axis_index(axis)).start()
            return 0

        lax.fori_loop(1, sizes[axis], push, 0)
        if kind != "sum":
            own(i).start()
    for i, (kind, axis) in enumerate(ops):
        if kind == "sum":
            outs[i][...] = ins[i][lax.axis_index(axis)].astype(f32)

        def take(k, _):
            copy(i, k, None).wait_recv()
            if kind == "sum":
                outs[i][...] += got[i][lax.rem(lax.axis_index(axis) + k, sizes[axis])].astype(f32)
            copy(i, k, None).wait_send()
            return 0

        lax.fori_loop(1, sizes[axis], take, 0)
        if kind != "sum":
            own(i).wait()


def collect(ops, arrays, sizes, call_id):
    def shape_of(op, a):
        kind, axis = op
        n = sizes[axis]
        if kind == "rows":
            return jax.ShapeDtypeStruct((a.shape[0] * n, a.shape[1] // n), a.dtype)
        if kind == "lanes":
            return jax.ShapeDtypeStruct((a.shape[0] // n, a.shape[1] * n), a.dtype)
        return jax.ShapeDtypeStruct(a.shape[1:], f32)

    vmem = pl.BlockSpec(memory_space=pltpu.VMEM)
    dma = pltpu.SemaphoreType.DMA
    most = max(sizes[axis] for _, axis in ops)
    count = len(ops)
    return pl.pallas_call(
        functools.partial(collect_kernel, ops=ops, sizes=sizes),
        out_shape=[shape_of(op, a) for op, a in zip(ops, arrays)],
        in_specs=[vmem] * count,
        out_specs=[vmem] * count,
        scratch_shapes=[
            pltpu.VMEM(a.shape, a.dtype) for op, a in zip(ops, arrays) if op[0] == "sum"
        ]
        + [dma((count, most)), dma((count, most)), dma((count,))],
        compiler_params=pltpu.CompilerParams(
            collective_id=call_id, has_side_effects=True, vmem_limit_bytes=40 * 2**20
        ),
    )(*arrays)


def input_kernel(heads_ref, grad_ref, w_ref, out_ref, w_s, sem):
    n_row, n_t, rows, cols = w_ref.shape
    loads = [
        pltpu.make_async_copy(
            w_ref.at[p, t], w_s.at[t, pl.ds(p * rows, rows), :], sem.at[t, p]
        )
        for t in range(n_t)
        for p in range(n_row)
    ]
    for load in loads:
        load.start()
    for load in loads:
        load.wait()
    out_ref[...] = grad_ref[...]
    for t in range(n_t):
        part = heads_ref[t * cols : (t + 1) * cols, :].astype(f32).T.astype(bf16)
        out_ref[...] += dot(part, w_s[t], 1, 1)


def input_gradient(grad_heads, grad_one, weights):
    n_row, n_t, rows, cols = weights.shape
    vmem = pl.BlockSpec(memory_space=pltpu.VMEM)
    return pl.pallas_call(
        input_kernel,
        out_shape=jax.ShapeDtypeStruct(grad_one.shape, f32),
        in_specs=[vmem, vmem, pl.BlockSpec(memory_space=pl.ANY)],
        out_specs=vmem,
        scratch_shapes=[
            pltpu.VMEM((n_t, n_row * rows, cols), bf16),
            pltpu.SemaphoreType.DMA((n_t, n_row)),
        ],
        compiler_params=pltpu.CompilerParams(vmem_limit_bytes=32 * 2**20),
        cost_estimate=pl.CostEstimate(
            flops=2 * grad_heads.size * grad_one.shape[1],
            bytes_accessed=2 * weights.size + 4 * grad_heads.size,
            transcendentals=0,
        ),
        name="input_gradient",
    )(grad_heads, grad_one, weights)


def sum_kernel(in_ref, out_ref, first, second, part, send_sem, recv_sem, local_sem, *, sizes):
    barrier = pltpu.get_barrier_semaphore()
    for axis, size in sizes:
        meet_all(barrier, axis, size)
    pl.semaphore_wait(barrier, sum(size - 1 for _, size in sizes))
    for stage, (axis, size) in enumerate(sizes):
        source = in_ref if stage == 0 else part
        into = first if stage == 0 else second
        z = lax.axis_index(axis)
        own = pltpu.make_async_copy(source, into.at[z], local_sem.at[stage])
        own.start()

        def push(k, _):
            pltpu.make_async_remote_copy(
                source,
                into.at[z],
                send_sem.at[stage, k],
                recv_sem.at[stage, z],
                **on(axis, lax.rem(z + k, size)),
            ).start()
            return 0

        def take(k, _):
            d = lax.rem(z + k, size)
            copy = pltpu.make_async_remote_copy(
                source, into.at[d], send_sem.at[stage, k], recv_sem.at[stage, d], **on(axis, d)
            )
            copy.wait_recv()
            copy.wait_send()
            return 0

        lax.fori_loop(1, size, push, 0)
        lax.fori_loop(1, size, take, 0)
        own.wait()
        total = into[0]
        for k in range(1, size):
            total = total + into[k]
        if stage == 0:
            part[...] = total
        else:
            out_ref[...] = total


def sum_everywhere(value, n_dp, n_tensor, call_id):
    vmem = pl.BlockSpec(memory_space=pltpu.VMEM)
    dma = pltpu.SemaphoreType.DMA
    most = max(n_dp, n_tensor)
    return pl.pallas_call(
        functools.partial(sum_kernel, sizes=(("dp", n_dp), ("tensor", n_tensor))),
        out_shape=jax.ShapeDtypeStruct(value.shape, f32),
        in_specs=[vmem],
        out_specs=vmem,
        scratch_shapes=[
            pltpu.VMEM((n_dp,) + value.shape, f32),
            pltpu.VMEM((n_tensor,) + value.shape, f32),
            pltpu.VMEM(value.shape, f32),
            dma((2, most)),
            dma((2, most)),
            dma((2,)),
        ],
        compiler_params=pltpu.CompilerParams(collective_id=call_id, has_side_effects=True),
    )(value)


def lamb_terms(weight, gradient, moments):
    first_moment = 0.5 * moments[0] + 0.5 * gradient
    root_moment = jnp.sqrt(0.5 * moments[1] * moments[1] + 0.5 * gradient * gradient)
    direction = first_moment / (root_moment + moment_eps) + decay_rate * weight
    return (jnp.stack([first_moment, root_moment]), direction)


def piece_sums(tensor_val, stacked):
    squares = tensor_val * tensor_val
    if stacked:
        return jnp.sum(squares.reshape(squares.shape[0], -1), axis=1)
    return jnp.sum(squares).reshape(1)


def local(
    inputs,
    cotangent,
    attn_w,
    out_w,
    glu_w,
    down_w,
    qv_bias,
    vectors,
    attn_mom,
    out_mom,
    glu_mom,
    down_mom,
    qv_mom,
    vector_mom,
    *,
    n_dp,
    n_tensor,
):
    tensor_pos = lax.axis_index("tensor")
    rows = attn_w.shape[1]
    head_cols = attn_w.shape[2]
    head_count = head_cols // HEAD
    width = rows * n_dp
    hidden_cols = glu_w.shape[2]
    tokens = inputs.shape[0]
    length = tokens * n_tensor
    qv_cols = qv_bias.shape[1]
    parts = lax.dynamic_slice_in_dim(
        jnp.asarray(slope_parts(HEADS)), tensor_pos * head_count, head_count
    )

    attn_rows = (
        attn_w.astype(bf16)
        .reshape(3, rows, head_count, HEAD)
        .transpose(1, 2, 0, 3)
        .reshape(rows, 3 * head_cols)
    )
    out_rows = out_w.astype(bf16).T
    glu_rows = glu_w.astype(bf16).transpose(1, 0, 2).reshape(rows, 2 * hidden_cols)
    down_rows = down_w.astype(bf16).T

    small = jnp.concatenate(
        [
            vectors.astype(bf16).T,
            jnp.pad(qv_bias.astype(bf16).reshape(-1), (0, rows - 2 * qv_cols)).reshape(rows, 1),
            jnp.zeros((rows, 57), bf16),
        ],
        axis=1,
    )
    wall_rows = jnp.concatenate(
        [glu_rows, down_rows, jnp.pad(out_rows, ((0, 0), (0, -head_cols % 128)))], axis=1
    )
    wall_chain, own = gather_blocks(
        [wall_rows], [jnp.concatenate([attn_rows, small], axis=1)], n_tensor, n_dp, 0
    )
    own = own.reshape(width, -1)
    first_inputs, own = lax.optimization_barrier((inputs, own))
    inputs_full, attn_chain = gather_blocks([first_inputs, attn_rows], [], n_tensor, n_dp, 1)
    inputs_full = inputs_full.reshape(length, width)
    wall = lax.all_gather(wall_chain, "dp")
    attn_all = lax.all_gather(attn_chain, "dp")
    if rows % 16:
        wall, attn_all = [
            w.transpose(1, 0, 2, 3).reshape(1, n_tensor, width, -1) for w in (wall, attn_all)
        ]

    attn_own = own[:, : 3 * head_cols]
    vector_rows = own[:, 3 * head_cols : 3 * head_cols + 6].T.astype(f32)
    qv_rows = (
        own[:, 3 * head_cols + 6]
        .reshape(n_dp, rows)[:, : 2 * qv_cols]
        .reshape(n_dp, 2, qv_cols)
        .transpose(1, 0, 2)
        .reshape(2, head_cols)
        .astype(f32)
    )
    qkv_bias = (
        jnp.stack([qv_rows[0], jnp.zeros_like(qv_rows[0]), qv_rows[1]])
        .reshape(3, head_count, HEAD)
        .transpose(1, 0, 2)
        .reshape(3 * head_cols)
    )

    qkv = (dot(inputs_full, attn_own, 1, 0) + qkv_bias).astype(bf16)
    out_t, lse = attention_forward(parts, qkv)
    sizes = {"dp": n_dp, "tensor": n_tensor}
    (attended,) = collect([("rows", "tensor")], [out_t.reshape(head_cols, length)], sizes, 2)
    output, grad_one, grad_attended, vector_part, grad_glu, grad_rest = feed_forward(
        attended,
        inputs,
        cotangent,
        jnp.pad(vector_rows, ((0, 2), (0, 0))),
        wall,
        head_cols,
        hidden_cols,
    )
    if rows % 16:
        grad_glu, grad_rest = [
            g.reshape(n_tensor, n_dp, rows, -1).transpose(1, 0, 2, 3) for g in (grad_glu, grad_rest)
        ]
    glu_part = lax.psum_scatter(grad_glu, "dp", scatter_dimension=0, tiled=False)
    rest_part = lax.psum_scatter(grad_rest, "dp", scatter_dimension=0, tiled=False)
    vector_all = sum_everywhere(vector_part, n_dp, n_tensor, 5)[:6]
    slice_width = vector_mom.shape[2]
    vector_sum = lax.dynamic_slice_in_dim(
        vector_all, (lax.axis_index("dp") * n_tensor + tensor_pos) * slice_width, slice_width, 1
    )
    (grad_heads,) = collect([("lanes", "tensor")], [grad_attended], sizes, 6)
    grad_heads = grad_heads.reshape(head_count, HEAD, length)
    grad_qkv = attention_backward(parts, qkv, grad_heads, out_t, lse).reshape(3 * head_cols, length)
    attn_grad = dot(inputs_full, grad_qkv, 0, 1)
    qv_grad = jnp.sum(grad_qkv.reshape(head_count, 3, HEAD, length).astype(f32), axis=3)
    qv_grad = jnp.stack([qv_grad[:, 0], qv_grad[:, 2]]).reshape(2, n_dp, qv_cols)
    qv_grad = jnp.pad(
        qv_grad.transpose(1, 0, 2).reshape(n_dp, 2 * qv_cols), ((0, 0), (0, rows - 2 * qv_cols))
    ).reshape(width, 1)
    attn_part = jnp.concatenate([attn_grad, qv_grad, jnp.zeros((width, 63), f32)], axis=1)
    attn_part = attn_part.astype(bf16).reshape(n_dp, rows, -1)
    grad_tokens, attn_part, glu_sum = collect(
        [("rows", "tensor"), ("sum", "dp"), ("sum", "tensor")],
        [grad_qkv, attn_part, glu_part],
        sizes,
        3,
    )
    (rest_sum,) = collect([("sum", "tensor")], [rest_part], sizes, 4)
    glu_sum = glu_sum.reshape(rows, 2, hidden_cols).transpose(1, 0, 2)
    down_sum = rest_sum[:, :hidden_cols].T
    out_sum = rest_sum[:, hidden_cols : hidden_cols + head_cols].T
    attn_sum = (
        attn_part[:, : 3 * head_cols]
        .reshape(rows, head_count, 3, HEAD)
        .transpose(2, 0, 1, 3)
        .reshape(3, rows, head_cols)
    )
    qv_sum = attn_part[: 2 * qv_cols, 3 * head_cols].reshape(2, qv_cols)

    input_grad = input_gradient(grad_tokens, grad_one, attn_all)

    vector_own = lax.dynamic_slice_in_dim(vectors, tensor_pos * slice_width, slice_width, 1)
    owned_parts = (attn_w, out_w, glu_w, down_w, qv_bias, vector_own)
    gradients = (attn_sum, out_sum, glu_sum, down_sum, qv_sum, vector_sum)
    moments = (attn_mom, out_mom, glu_mom, down_mom, qv_mom, vector_mom)
    stack_flags = (True, False, True, False, True, True)
    new_moments = []
    directions = []
    for weight, gradient, moment in zip(owned_parts, gradients, moments):
        pair, direction = lamb_terms(weight, gradient, moment)
        new_moments.append(pair)
        directions.append(direction)
    weight_sums = jnp.concatenate([piece_sums(w, f) for w, f in zip(owned_parts, stack_flags)])
    dir_sums = jnp.concatenate([piece_sums(r, f) for r, f in zip(directions, stack_flags)])
    totals = jnp.pad(jnp.stack([weight_sums, dir_sums]), ((0, 6), (0, 113)))
    totals = sum_everywhere(totals, n_dp, n_tensor, 9)[:2, :15]
    norm_values = jnp.sqrt(totals + 1e-12)
    ratios = norm_values[0] / norm_values[1]
    new_weights = []
    offset = 0
    for weight, direction, stacked in zip(owned_parts, directions, stack_flags):
        amount = weight.shape[0] if stacked else 1
        factor = ratios[offset : offset + amount]
        if stacked:
            factor = factor.reshape((amount,) + (1,) * (weight.ndim - 1))
        else:
            factor = factor[0]
        new_weights.append(weight - learn_rate * factor * direction)
        offset = offset + amount
    return (
        output,
        input_grad,
        *gradients,
        *new_moments,
        *new_weights,
        norm_values,
        ratios,
    )


def solution(mesh):
    tokens = P(("dp", "tensor"), None)
    attn = P(None, "dp", "tensor")
    cols = P("tensor", "dp")
    moments = (
        P(None, None, "dp", "tensor"),
        P(None, "tensor", "dp"),
        P(None, None, "dp", "tensor"),
        P(None, "tensor", "dp"),
        P(None, None, ("tensor", "dp")),
        P(None, None, ("dp", "tensor")),
    )
    weights = (attn, cols, attn, cols, P(None, ("tensor", "dp")))
    split = P(None, ("dp", "tensor"))
    return jax.shard_map(
        functools.partial(local, n_dp=mesh.shape["dp"], n_tensor=mesh.shape["tensor"]),
        mesh=mesh,
        in_specs=(tokens, tokens, *weights, P(None, "dp"), *moments),
        out_specs=(tokens, tokens, *weights, split, *moments, *weights, split, P(), P()),
        check_vma=False,
    )
```

```python
import functools
import math

import jax
import jax.numpy as jnp
import numpy as np
from jax import lax
from jax.experimental import pallas as pl
from jax.experimental.pallas import tpu as pltpu
from jax.sharding import PartitionSpec as P


HEADS = 12
HEAD = 64
BLOCK = 256

norm_eps = 1e-06
learn_rate = 0.2
decay_rate = 0.01
moment_eps = 1e-06


bf16 = jnp.bfloat16
f32 = jnp.float32


def dot(a, b, ca, cb):
    return lax.dot_general(a, b, (((ca,), (cb,)), ((), ())), preferred_element_type=f32)


def slope_parts(head_total):
    power_two = 2 ** int(math.floor(math.log2(head_total)))
    slopes = [2.0 ** (-8.0 * (j + 1) / power_two) for j in range(power_two)]
    slopes += [2.0 ** (-4.0 * (2 * j + 1) / power_two) for j in range(head_total - power_two)]
    rest = np.array(slopes, np.float32)
    parts = []
    for _ in range(3):
        part = rest.astype(bf16).astype(np.float32)
        parts.append(part)
        rest = rest - part
    return np.stack(parts, axis=1)


def pos_features(length, parts):
    row = lax.broadcasted_iota(jnp.int32, (length, HEAD), 0)
    lane = lax.broadcasted_iota(jnp.int32, (length, HEAD), 1)
    low = (row & 7).astype(f32)
    high = row.astype(f32) - low
    m1, m2, m3 = parts
    slope_q = jnp.where(lane < 2, m1, jnp.where(lane < 4, m2, m3))
    for_q = jnp.where(lane < 6, slope_q, jnp.where(lane < 9, high, jnp.where(lane < 12, low, 0.0)))
    turn = lane - 6
    slope_k = jnp.where(
        (turn == 0) | (turn == 3), m1, jnp.where((turn == 1) | (turn == 4), m2, m3)
    )
    for_k = jnp.where(
        lane < 6, jnp.where((lane & 1) == 0, high, low), jnp.where(lane < 12, -slope_k, 0.0)
    )
    return for_q, for_k


def key_after_query(block):
    late = lax.broadcasted_iota(jnp.int32, (block, block), 0) - lax.broadcasted_iota(
        jnp.int32, (block, block), 1
    )
    return jnp.maximum(late, 0).astype(f32)


def fwd_kernel(
    parts_ref, qkv_ref, out_ref, lse_ref, q_s, k_s, v_s, corr_s, s_s, *, heads, length, unroll
):
    amount = length // BLOCK
    for h in range(heads):
        for_q, for_k = pos_features(length, [parts_ref[h, i] for i in range(3)])
        base = h * 3 * HEAD
        q = qkv_ref[:, base : base + HEAD].astype(f32) * HEAD**-0.5
        k = qkv_ref[:, base + HEAD : base + 2 * HEAD].astype(f32)
        v = qkv_ref[:, base + 2 * HEAD : base + 3 * HEAD].astype(f32)
        q_s[h, 0] = jnp.concatenate([q, for_q], axis=1).astype(bf16)
        q_s[h, 1] = jnp.concatenate([q, -for_q], axis=1).astype(bf16)
        k_s[h] = jnp.concatenate([k, for_k], axis=1).astype(bf16)
        v_s[h] = v.T.astype(bf16)
    late = key_after_query(BLOCK)

    def head(h, _):
        corr_s[...] = 2.0 * (parts_ref[h, 0] + parts_ref[h, 1] + parts_ref[h, 2]) * late

        def group(g, _):
            for u in range(unroll):
                b = g * unroll + u
                rows = pl.ds(pl.multiple_of(b * BLOCK, BLOCK), BLOCK)
                for c in range(amount):
                    after = (c > b).astype(jnp.int32)
                    keys = slice(c * BLOCK, (c + 1) * BLOCK)
                    s_s[u, keys, :] = dot(k_s[h, keys, :], q_s[h, after, rows, :], 1, 1)
                s_s[u, rows, :] = s_s[u, rows, :] - corr_s[...]
            for u in range(unroll):
                b = g * unroll + u
                rows = pl.ds(pl.multiple_of(b * BLOCK, BLOCK), BLOCK)
                s = s_s[u]
                top = jnp.max(s, axis=0, keepdims=True)
                p = jnp.exp(s - top)
                total = jnp.sum(p, axis=0, keepdims=True)
                o = dot(v_s[h], p.astype(bf16), 1, 0)
                out_ref[h, :, rows] = (o / total).astype(bf16)
                lse_ref[h, :, rows] = top + jnp.log(total)
            return 0

        lax.fori_loop(0, amount // unroll, group, 0)
        return 0

    lax.fori_loop(0, heads, head, 0)


def attention_forward(parts, qkv):
    length = qkv.shape[0]
    heads = qkv.shape[1] // (3 * HEAD)
    unroll = 2
    vmem = pl.BlockSpec(memory_space=pltpu.VMEM)
    work = heads * length * length
    return pl.pallas_call(
        functools.partial(fwd_kernel, heads=heads, length=length, unroll=unroll),
        out_shape=(
            jax.ShapeDtypeStruct((heads, HEAD, length), bf16),
            jax.ShapeDtypeStruct((heads, 1, length), f32),
        ),
        in_specs=[pl.BlockSpec(memory_space=pltpu.SMEM), vmem],
        out_specs=(vmem, vmem),
        scratch_shapes=[
            pltpu.VMEM((heads, 2, length, 128), bf16),
            pltpu.VMEM((heads, length, 128), bf16),
            pltpu.VMEM((heads, HEAD, length), bf16),
            pltpu.VMEM((BLOCK, BLOCK), f32),
            pltpu.VMEM((unroll, length, BLOCK), f32),
        ],
        compiler_params=pltpu.CompilerParams(vmem_limit_bytes=40 * 2**20),
        cost_estimate=pl.CostEstimate(
            flops=16 * work * HEAD, bytes_accessed=4 * qkv.size, transcendentals=work
        ),
        name="attention_forward",
    )(parts, qkv)


def on(axis, place):
    return {"device_id": {axis: place}, "device_id_type": pl.DeviceIdType.MESH}


def meet_all(barrier, axis, size):
    place = lax.axis_index(axis)

    def tell(k, _):
        pl.semaphore_signal(barrier, inc=1, **on(axis, lax.rem(place + k, size)))
        return 0

    lax.fori_loop(1, size, tell, 0)


def bwd_kernel(
    parts_ref,
    qkv_ref,
    own_ref,
    ot_ref,
    lse_ref,
    x_ref,
    tok_ref,
    dw_ref,
    bias_ref,
    q_s,
    qn_s,
    k_s,
    kt_s,
    v_s,
    do_s,
    dot_s,
    corr_s,
    s_s,
    dq_s,
    dk_s,
    dv_s,
    stage_s,
    dwt_s,
    in_send,
    in_recv,
    in_own,
    out_send,
    out_recv,
    out_own,
    *,
    heads,
    length,
    unroll,
    size,
):
    amount = length // BLOCK
    tokens = length // size
    group = 3 * HEAD
    z = lax.axis_index("tensor")
    barrier = pltpu.get_barrier_semaphore()
    meet_all(barrier, "tensor", size)
    pl.semaphore_wait(barrier, size - 1)

    def taking(h, k, landing):
        d = lax.rem(z + k, size)
        place = d if landing is None else landing
        return pltpu.make_async_remote_copy(
            own_ref.at[pl.ds(pl.multiple_of((d * heads + h) * HEAD, HEAD), HEAD), :],
            dot_s.at[h, :, pl.ds(pl.multiple_of(place * tokens, 128), tokens)],
            in_send.at[h, k],
            in_recv.at[h, place],
            **on("tensor", d),
        )

    def taking_own(h):
        return pltpu.make_async_copy(
            own_ref.at[pl.ds(pl.multiple_of((z * heads + h) * HEAD, HEAD), HEAD), :],
            dot_s.at[h, :, pl.ds(pl.multiple_of(z * tokens, 128), tokens)],
            in_own.at[h],
        )

    def giving(h, k, landing):
        d = lax.rem(z + k, size)
        place = d if landing is None else landing
        return pltpu.make_async_remote_copy(
            stage_s.at[h, :, pl.ds(pl.multiple_of(d * tokens, 128), tokens)],
            tok_ref.at[pl.ds(pl.multiple_of((place * heads + h) * group, HEAD), group), :],
            out_send.at[h, k],
            out_recv.at[h, place],
            **on("tensor", d),
        )

    def giving_own(h):
        return pltpu.make_async_copy(
            stage_s.at[h, :, pl.ds(pl.multiple_of(z * tokens, 128), tokens)],
            tok_ref.at[pl.ds(pl.multiple_of((z * heads + h) * group, HEAD), group), :],
            out_own.at[h],
        )

    for h in range(heads):
        for k in range(1, size):
            taking(h, k, z).start()
        taking_own(h).start()

    for h in range(heads):
        for_q, for_k = pos_features(length, [parts_ref[h, i] for i in range(3)])
        base = h * group
        q = qkv_ref[:, base : base + HEAD].astype(f32) * HEAD**-0.5
        k = qkv_ref[:, base + HEAD : base + 2 * HEAD].astype(f32)
        v = qkv_ref[:, base + 2 * HEAD : base + 3 * HEAD]
        turned = q.T
        turned_pos = for_q.T
        q_s[h, 0] = jnp.concatenate([turned, turned_pos], axis=0).astype(bf16)
        q_s[h, 1] = jnp.concatenate([turned, -turned_pos], axis=0).astype(bf16)
        qn_s[h] = q.astype(bf16)
        k_s[h] = jnp.concatenate([k, for_k], axis=1).astype(bf16)
        kt_s[h] = k.T.astype(bf16)
        v_s[h] = v
    late = key_after_query(BLOCK)

    def head(h, _):
        corr_s[...] = 2.0 * (parts_ref[h, 0] + parts_ref[h, 1] + parts_ref[h, 2]) * late
        dq_s[...] = jnp.zeros_like(dq_s)
        for k in range(1, size):
            taking(h, k, None).wait_recv()
        taking_own(h).wait()
        grad = dot_s[h].astype(f32)
        do_s[...] = grad.T.astype(bf16)
        centre = jnp.sum(grad * ot_ref[h].astype(f32), axis=0, keepdims=True)

        def part(g, _):
            for u in range(unroll):
                c = g * unroll + u
                rows = pl.ds(pl.multiple_of(c * BLOCK, BLOCK), BLOCK)
                keys = k_s[h, rows, :]
                for i in range(amount):
                    after = (i < c).astype(jnp.int32)
                    cols = slice(i * BLOCK, (i + 1) * BLOCK)
                    s_s[u, :, cols] = dot(keys, q_s[h, after, :, cols], 1, 0)
                s_s[u, :, rows] = s_s[u, :, rows] - corr_s[...]
            for u in range(unroll):
                c = g * unroll + u
                rows = pl.ds(pl.multiple_of(c * BLOCK, BLOCK), BLOCK)
                p = jnp.exp(s_s[u] - lse_ref[h])
                dp = dot(v_s[h, rows, :], dot_s[h], 1, 0)
                dv_s[rows, :] = dot(p.astype(bf16), do_s[...], 1, 0)
                ds = (p * (dp - centre)).astype(bf16)
                dk_s[rows, :] = dot(ds, qn_s[h], 1, 0)
                dq_s[...] += dot(kt_s[h, :, rows], ds, 1, 0)
            return 0

        lax.fori_loop(0, amount // unroll, part, 0)
        stage_s[h, :HEAD] = (dq_s[...] * HEAD**-0.5).astype(bf16)
        stage_s[h, HEAD : 2 * HEAD] = dk_s[...].T.astype(bf16)
        stage_s[h, 2 * HEAD :] = dv_s[...].T.astype(bf16)
        dwt_s[h] = dot(stage_s[h], x_ref[...], 1, 0)
        bias_ref[h] = jnp.sum(stage_s[h].astype(f32), axis=1, keepdims=True)
        for k in range(1, size):
            giving(h, k, z).start()
        giving_own(h).start()
        return 0

    lax.fori_loop(0, heads, head, 0)
    for h in range(heads):
        dw_ref[:, h * group : (h + 1) * group] = dwt_s[h].T.astype(bf16)
    for h in range(heads):
        for k in range(1, size):
            taking(h, k, None).wait_send()
            giving(h, k, None).wait_recv()
            giving(h, k, None).wait_send()
        giving_own(h).wait()


def attention_backward(parts, qkv, grad_own, out_t, lse, inputs_full, size, call_id):
    length, width = inputs_full.shape
    heads = qkv.shape[1] // (3 * HEAD)
    unroll = 2
    tokens = length // size
    vmem = pl.BlockSpec(memory_space=pltpu.VMEM)
    shape = jax.ShapeDtypeStruct
    dma = pltpu.SemaphoreType.DMA
    work = heads * length * length
    return pl.pallas_call(
        functools.partial(bwd_kernel, heads=heads, length=length, unroll=unroll, size=size),
        out_shape=(
            shape((size * heads * 3 * HEAD, tokens), bf16),
            shape((width, heads * 3 * HEAD), bf16),
            shape((heads, 3 * HEAD, 1), f32),
        ),
        in_specs=[pl.BlockSpec(memory_space=pltpu.SMEM)] + [vmem] * 5,
        out_specs=(vmem, vmem, vmem),
        scratch_shapes=[
            pltpu.VMEM((heads, 2, 128, length), bf16),
            pltpu.VMEM((heads, length, HEAD), bf16),
            pltpu.VMEM((heads, length, 128), bf16),
            pltpu.VMEM((heads, HEAD, length), bf16),
            pltpu.VMEM((heads, length, HEAD), bf16),
            pltpu.VMEM((length, HEAD), bf16),
            pltpu.VMEM((heads, HEAD, length), bf16),
            pltpu.VMEM((BLOCK, BLOCK), f32),
            pltpu.VMEM((unroll, BLOCK, length), f32),
            pltpu.VMEM((HEAD, length), f32),
            pltpu.VMEM((length, HEAD), f32),
            pltpu.VMEM((length, HEAD), f32),
            pltpu.VMEM((heads, 3 * HEAD, length), bf16),
            pltpu.VMEM((heads, 3 * HEAD, width), f32),
            dma((heads, size)),
            dma((heads, size)),
            dma((heads,)),
            dma((heads, size)),
            dma((heads, size)),
            dma((heads,)),
        ],
        compiler_params=pltpu.CompilerParams(
            collective_id=call_id, has_side_effects=True, vmem_limit_bytes=56 * 2**20
        ),
        cost_estimate=pl.CostEstimate(
            flops=40 * work * HEAD, bytes_accessed=8 * qkv.size, transcendentals=work
        ),
        name="attention_backward",
    )(parts, qkv, grad_own, out_t, lse, inputs_full)


def normed(z):
    center = z - jnp.mean(z, axis=1, keepdims=True)
    scale = lax.rsqrt(jnp.mean(center * center, axis=1, keepdims=True) + norm_eps)
    return center * scale, scale


def norm_back(grad, unit, scale, gain):
    inner = grad * gain
    mean = jnp.mean(inner, axis=1, keepdims=True)
    return scale * (inner - mean - unit * jnp.mean(inner * unit, axis=1, keepdims=True))


def ff_kernel(
    att_ref,
    x_ref,
    cot_ref,
    vec_ref,
    wall_ref,
    out_ref,
    dz1_ref,
    do_ref,
    dvec_ref,
    gglu_ref,
    grest_ref,
    wgu_s,
    wd_s,
    wo_s,
    act_s,
    der_s,
    hid_s,
    atn_s,
    h1_s,
    x1_s,
    h1r_s,
    h1t_s,
    df_s,
    dft_s,
    acc_s,
    sglu_s,
    sdown_s,
    sout_s,
    load_sem,
    store_sem,
    *,
    head_cols,
    hid_cols,
):
    n_row, n_t, rows = wall_ref.shape[:3]
    width = h1_s.shape[1]
    pad = wo_s.shape[2]
    sizes = (2 * hid_cols, hid_cols, pad)

    def loads(kind, t):
        into = (wgu_s, wd_s, wo_s)[kind]
        low = sum(sizes[:kind])
        return [
            pltpu.make_async_copy(
                wall_ref.at[p, t, :, pl.ds(low, sizes[kind])],
                into.at[t, pl.ds(p * rows, rows), :],
                load_sem.at[kind, t, p],
            )
            for p in range(n_row)
        ]

    def stores(kind, t):
        source = (sglu_s, sdown_s, sout_s)[kind]
        into = (gglu_ref, grest_ref, grest_ref)[kind]
        low = (0, 0, hid_cols)[kind]
        return [
            pltpu.make_async_copy(
                source.at[pl.ds(p * rows, rows), :],
                into.at[p, t, :, pl.ds(low, sizes[kind])],
                store_sem.at[kind, p],
            )
            for p in range(n_row)
        ]

    for kind in (2, 0, 1):
        for t in range(n_t):
            for copy in loads(kind, t):
                copy.start()
    for t in range(n_t):
        atn_s[t] = att_ref[t * head_cols : (t + 1) * head_cols, :].astype(f32).T.astype(bf16)
        for copy in loads(2, t):
            copy.wait()
    branch = jnp.zeros_like(acc_s)
    for t in range(n_t):
        branch = branch + dot(atn_s[t], wo_s[t, :, :head_cols], 1, 1)
    x1, r1 = normed(x_ref[...].astype(f32) + branch + vec_ref[0:1, :])
    x1_s[...] = x1
    h1 = x1 * vec_ref[1:2, :] + vec_ref[2:3, :]
    h1_s[...] = h1
    h1r_s[...] = h1.astype(bf16)
    h1t_s[...] = h1.T.astype(bf16)
    acc_s[...] = jnp.zeros_like(acc_s)
    for kind in (0, 1):
        for t in range(n_t):
            for copy in loads(kind, t):
                copy.wait()

    def forward(t, _):
        g = dot(h1r_s[...], wgu_s[t, :, :hid_cols], 1, 0)
        u = dot(h1r_s[...], wgu_s[t, :, hid_cols:], 1, 0)
        below = 0.5 * (1.0 + lax.erf(g * np.float32(math.sqrt(0.5))))
        dense = jnp.exp(-0.5 * g * g) * np.float32(1.0 / math.sqrt(2.0 * math.pi))
        act = g * below
        act_s[t] = act
        der_s[t] = u * (below + g * dense)
        hidden = (act * u).astype(bf16)
        hid_s[t] = hidden
        acc_s[...] += dot(hidden, wd_s[t], 1, 1)
        return 0

    lax.fori_loop(0, n_t, forward, 0)
    x2, r2 = normed(h1_s[...] + acc_s[...] + vec_ref[3:4, :])
    out_ref[...] = (x2 * vec_ref[4:5, :] + vec_ref[5:6, :]).astype(bf16)
    cot = cot_ref[...].astype(f32)
    dz2 = norm_back(cot, x2, r2, vec_ref[4:5, :])
    dvec_ref[3:4, :] = jnp.sum(dz2, axis=0, keepdims=True)
    dvec_ref[4:5, :] = jnp.sum(cot * x2, axis=0, keepdims=True)
    dvec_ref[5:6, :] = jnp.sum(cot, axis=0, keepdims=True)
    df_s[...] = dz2.astype(bf16)
    dft_s[...] = dz2.T.astype(bf16)
    acc_s[...] = dz2

    def backward(t, _):
        def waits(kind):
            @pl.when(t > 0)
            def _():
                for copy in stores(kind, t - 1):
                    copy.wait()

        waits(1)
        sdown_s[...] = dot(dft_s[...], hid_s[t], 1, 0).astype(bf16)
        for copy in stores(1, t):
            copy.start()
        dh = dot(df_s[...], wd_s[t], 1, 0)
        dg = (dh * der_s[t]).astype(bf16)
        du = (dh * act_s[t]).astype(bf16)
        acc_s[...] += dot(dg, wgu_s[t, :, :hid_cols], 1, 1) + dot(du, wgu_s[t, :, hid_cols:], 1, 1)
        waits(0)
        sglu_s[:, :hid_cols] = dot(h1t_s[...], dg, 1, 0).astype(bf16)
        sglu_s[:, hid_cols:] = dot(h1t_s[...], du, 1, 0).astype(bf16)
        for copy in stores(0, t):
            copy.start()
        return 0

    lax.fori_loop(0, n_t, backward, 0)
    dh1 = acc_s[...]
    x1 = x1_s[...]
    dz1 = norm_back(dh1, x1, r1, vec_ref[1:2, :])
    dvec_ref[0:1, :] = jnp.sum(dz1, axis=0, keepdims=True)
    dvec_ref[1:2, :] = jnp.sum(dh1 * x1, axis=0, keepdims=True)
    dvec_ref[2:3, :] = jnp.sum(dh1, axis=0, keepdims=True)
    dvec_ref[6:8, :] = jnp.zeros((2, width), f32)
    dz1_ref[...] = dz1
    da = dz1.astype(bf16)
    dat = dz1.T.astype(bf16)
    sout_s[...] = jnp.zeros_like(sout_s)
    for t in range(n_t):
        do_ref[t * head_cols : (t + 1) * head_cols, :] = dot(
            da, wo_s[t, :, :head_cols], 1, 0
        ).T.astype(bf16)
        if t > 0:
            for copy in stores(2, t - 1):
                copy.wait()
        sout_s[:, :head_cols] = dot(dat, atn_s[t], 1, 0).astype(bf16)
        for copy in stores(2, t):
            copy.start()
    for kind in range(3):
        for copy in stores(kind, n_t - 1):
            copy.wait()


def feed_forward(attended, inputs, cotangent, vector_rows, wall, head_cols, hid_cols):
    tokens, width = inputs.shape
    n_row, n_t, rows = wall.shape[:3]
    pad = wall.shape[3] - 3 * hid_cols
    vmem = pl.BlockSpec(memory_space=pltpu.VMEM)
    hbm = pl.BlockSpec(memory_space=pl.ANY)
    shape = jax.ShapeDtypeStruct
    size = tokens * width * n_t
    return pl.pallas_call(
        functools.partial(ff_kernel, head_cols=head_cols, hid_cols=hid_cols),
        out_shape=(
            shape((tokens, width), bf16),
            shape((tokens, width), f32),
            shape((n_t * head_cols, tokens), bf16),
            shape((8, width), f32),
            shape((n_row, n_t, rows, 2 * hid_cols), bf16),
            shape((n_row, n_t, rows, hid_cols + pad), bf16),
        ),
        in_specs=[vmem] * 4 + [hbm],
        out_specs=(vmem, vmem, vmem, vmem, hbm, hbm),
        scratch_shapes=[
            pltpu.VMEM((n_t, width, 2 * hid_cols), bf16),
            pltpu.VMEM((n_t, width, hid_cols), bf16),
            pltpu.VMEM((n_t, width, pad), bf16),
            pltpu.VMEM((n_t, tokens, hid_cols), f32),
            pltpu.VMEM((n_t, tokens, hid_cols), f32),
            pltpu.VMEM((n_t, tokens, hid_cols), bf16),
            pltpu.VMEM((n_t, tokens, head_cols), bf16),
            pltpu.VMEM((tokens, width), f32),
            pltpu.VMEM((tokens, width), f32),
            pltpu.VMEM((tokens, width), bf16),
            pltpu.VMEM((width, tokens), bf16),
            pltpu.VMEM((tokens, width), bf16),
            pltpu.VMEM((width, tokens), bf16),
            pltpu.VMEM((tokens, width), f32),
            pltpu.VMEM((width, 2 * hid_cols), bf16),
            pltpu.VMEM((width, hid_cols), bf16),
            pltpu.VMEM((width, pad), bf16),
            pltpu.SemaphoreType.DMA((3, n_t, n_row)),
            pltpu.SemaphoreType.DMA((3, n_row)),
        ],
        compiler_params=pltpu.CompilerParams(vmem_limit_bytes=63 * 2**20),
        cost_estimate=pl.CostEstimate(
            flops=6 * size * (3 * hid_cols + head_cols),
            bytes_accessed=4 * wall.size,
            transcendentals=2 * tokens * n_t * hid_cols,
        ),
        name="feed_forward",
    )(attended, inputs, cotangent, vector_rows, wall)


def gather_kernel(*refs, n_chain, n_flat, chain, flat):
    ins, refs = refs[: n_chain + n_flat], refs[n_chain + n_flat :]
    outs, refs = refs[: n_chain + n_flat], refs[n_chain + n_flat :]
    send_sem, recv_sem, local_sem, flat_send, flat_recv = refs
    z = lax.axis_index("tensor")
    p = lax.axis_index("dp")
    barrier = pltpu.get_barrier_semaphore()

    @pl.when(z > 0)
    def _():
        pl.semaphore_signal(barrier, inc=1, **on("tensor", z - 1))

    @pl.when(z < chain - 1)
    def _():
        pl.semaphore_signal(barrier, inc=1, **on("tensor", z + 1))

    met = jnp.where(z > 0, 1, 0) + jnp.where(z < chain - 1, 1, 0)
    if n_flat:
        meet_all(barrier, "dp", flat)
        met = met + flat - 1
    pl.semaphore_wait(barrier, met)

    own = []
    for i in range(n_chain):
        own.append(pltpu.make_async_copy(ins[i], outs[i].at[z], local_sem.at[i]))
    for j in range(n_flat):
        i = n_chain + j
        own.append(pltpu.make_async_copy(ins[i], outs[i].at[p], local_sem.at[i]))

        def push(k, _):
            pltpu.make_async_remote_copy(
                ins[i],
                outs[i].at[p],
                flat_send.at[j, k],
                flat_recv.at[j, p],
                **on("dp", lax.rem(p + k, flat)),
            ).start()
            return 0

        lax.fori_loop(1, flat, push, 0)
    for copy in own:
        copy.start()

    def hop(i, way, step):
        block = z - step if way == 0 else z + step
        target = z + 1 if way == 0 else z - 1
        return pltpu.make_async_remote_copy(
            ins[i] if step == 0 else outs[i].at[block],
            outs[i].at[block],
            send_sem.at[i, way, step],
            recv_sem.at[i, block],
            **on("tensor", target),
        )

    def sends(way, step):
        if way == 0:
            return (z < chain - 1) & (z >= step)
        return (z > 0) & (z + step < chain)

    def arrived(i, block):
        pltpu.make_async_remote_copy(
            outs[i].at[block],
            outs[i].at[block],
            send_sem.at[i, 0, 0],
            recv_sem.at[i, block],
            **on("tensor", lax.rem(z + 1, chain)),
        ).wait_recv()

    for i in range(n_chain):
        for step in range(chain - 1):
            for way in range(2):

                @pl.when(sends(way, step))
                def _():
                    if step > 0:
                        arrived(i, z - step if way == 0 else z + step)
                    hop(i, way, step).start()

    for i in range(n_chain):
        for step in range(1, chain):

            @pl.when((z == chain - 1) & (z >= step))
            def _():
                arrived(i, z - step)

            @pl.when((z == 0) & (z + step < chain))
            def _():
                arrived(i, z + step)

        for step in range(chain - 1):
            for way in range(2):

                @pl.when(sends(way, step))
                def _():
                    hop(i, way, step).wait_send()

    for j in range(n_flat):
        i = n_chain + j

        def finish(k, _):
            q = lax.rem(p + k, flat)
            copy = pltpu.make_async_remote_copy(
                ins[i], outs[i].at[q], flat_send.at[j, k], flat_recv.at[j, q], **on("dp", q)
            )
            copy.wait_send()
            copy.wait_recv()
            return 0

        lax.fori_loop(1, flat, finish, 0)
    for copy in own:
        copy.wait()


def gather_blocks(on_chain, to_all, n_tensor, n_dp, call_id):
    arrays = [*on_chain, *to_all]
    sizes = [n_tensor] * len(on_chain) + [n_dp] * len(to_all)
    vmem = pl.BlockSpec(memory_space=pltpu.VMEM)
    hbm = pl.BlockSpec(memory_space=pl.ANY)
    count = len(arrays)
    dma = pltpu.SemaphoreType.DMA
    return pl.pallas_call(
        functools.partial(
            gather_kernel, n_chain=len(on_chain), n_flat=len(to_all), chain=n_tensor, flat=n_dp
        ),
        out_shape=[jax.ShapeDtypeStruct((n,) + a.shape, a.dtype) for n, a in zip(sizes, arrays)],
        in_specs=[vmem] * count,
        out_specs=[hbm] * count,
        scratch_shapes=[
            dma((count, 2, n_tensor)),
            dma((count, n_tensor)),
            dma((count,)),
            dma((max(len(to_all), 1), n_dp)),
            dma((max(len(to_all), 1), n_dp)),
        ],
        compiler_params=pltpu.CompilerParams(collective_id=call_id, has_side_effects=True),
    )(*arrays)


def collect_kernel(*refs, ops, sizes):
    count = len(ops)
    ins, outs, refs = refs[:count], refs[count : 2 * count], refs[2 * count :]
    sums = [i for i, (kind, _) in enumerate(ops) if kind == "sum"]
    got = dict(zip(sums, refs))
    send_sem, recv_sem, local_sem = refs[len(sums) :]
    barrier = pltpu.get_barrier_semaphore()
    axes = sorted({axis for _, axis in ops})
    for axis in axes:
        meet_all(barrier, axis, sizes[axis])
    pl.semaphore_wait(barrier, sum(sizes[axis] - 1 for axis in axes))

    def cut_lanes(ref, index, size):
        lanes = ref.shape[1] // size
        return ref.at[:, pl.ds(pl.multiple_of(index * lanes, 128), lanes)]

    def cut_rows(ref, index, size):
        rows = ref.shape[0] // size
        return ref.at[pl.ds(pl.multiple_of(index * rows, 16), rows), :]

    def cuts(i, source, target):
        kind, axis = ops[i]
        size = sizes[axis]
        if kind == "rows":
            return cut_lanes(ins[i], source, size), cut_rows(outs[i], target, size)
        if kind == "lanes":
            return cut_rows(ins[i], source, size), cut_lanes(outs[i], target, size)
        return ins[i].at[source], got[i].at[target]

    def copy(i, k, landing):
        axis = ops[i][1]
        d = lax.rem(lax.axis_index(axis) + k, sizes[axis])
        place = d if landing is None else landing
        source, target = cuts(i, d, place)
        return pltpu.make_async_remote_copy(
            source, target, send_sem.at[i, k], recv_sem.at[i, place], **on(axis, d)
        )

    def own(i):
        z = lax.axis_index(ops[i][1])
        return pltpu.make_async_copy(*cuts(i, z, z), local_sem.at[i])

    for i, (kind, axis) in enumerate(ops):

        def push(k, _):
            copy(i, k, lax.axis_index(axis)).start()
            return 0

        lax.fori_loop(1, sizes[axis], push, 0)
        if kind != "sum":
            own(i).start()
    for i, (kind, axis) in enumerate(ops):
        if kind == "sum":
            outs[i][...] = ins[i][lax.axis_index(axis)].astype(f32)

        def take(k, _):
            copy(i, k, None).wait_recv()
            if kind == "sum":
                outs[i][...] += got[i][lax.rem(lax.axis_index(axis) + k, sizes[axis])].astype(f32)
            copy(i, k, None).wait_send()
            return 0

        lax.fori_loop(1, sizes[axis], take, 0)
        if kind != "sum":
            own(i).wait()


def collect(ops, arrays, sizes, call_id):
    def shape_of(op, a):
        kind, axis = op
        n = sizes[axis]
        if kind == "rows":
            return jax.ShapeDtypeStruct((a.shape[0] * n, a.shape[1] // n), a.dtype)
        if kind == "lanes":
            return jax.ShapeDtypeStruct((a.shape[0] // n, a.shape[1] * n), a.dtype)
        return jax.ShapeDtypeStruct(a.shape[1:], f32)

    vmem = pl.BlockSpec(memory_space=pltpu.VMEM)
    dma = pltpu.SemaphoreType.DMA
    most = max(sizes[axis] for _, axis in ops)
    count = len(ops)
    return pl.pallas_call(
        functools.partial(collect_kernel, ops=ops, sizes=sizes),
        out_shape=[shape_of(op, a) for op, a in zip(ops, arrays)],
        in_specs=[vmem] * count,
        out_specs=[vmem] * count,
        scratch_shapes=[
            pltpu.VMEM(a.shape, a.dtype) for op, a in zip(ops, arrays) if op[0] == "sum"
        ]
        + [dma((count, most)), dma((count, most)), dma((count,))],
        compiler_params=pltpu.CompilerParams(
            collective_id=call_id, has_side_effects=True, vmem_limit_bytes=40 * 2**20
        ),
    )(*arrays)


def input_kernel(heads_ref, grad_ref, w_ref, out_ref, w_s, sem):
    n_row, n_t, rows, cols = w_ref.shape
    loads = [
        pltpu.make_async_copy(
            w_ref.at[p, t], w_s.at[t, pl.ds(p * rows, rows), :], sem.at[t, p]
        )
        for t in range(n_t)
        for p in range(n_row)
    ]
    for load in loads:
        load.start()
    for load in loads:
        load.wait()
    out_ref[...] = grad_ref[...]
    for t in range(n_t):
        part = heads_ref[t * cols : (t + 1) * cols, :].astype(f32).T.astype(bf16)
        out_ref[...] += dot(part, w_s[t], 1, 1)


def input_gradient(grad_heads, grad_one, weights):
    n_row, n_t, rows, cols = weights.shape
    vmem = pl.BlockSpec(memory_space=pltpu.VMEM)
    return pl.pallas_call(
        input_kernel,
        out_shape=jax.ShapeDtypeStruct(grad_one.shape, f32),
        in_specs=[vmem, vmem, pl.BlockSpec(memory_space=pl.ANY)],
        out_specs=vmem,
        scratch_shapes=[
            pltpu.VMEM((n_t, n_row * rows, cols), bf16),
            pltpu.SemaphoreType.DMA((n_t, n_row)),
        ],
        compiler_params=pltpu.CompilerParams(vmem_limit_bytes=32 * 2**20),
        cost_estimate=pl.CostEstimate(
            flops=2 * grad_heads.size * grad_one.shape[1],
            bytes_accessed=2 * weights.size + 4 * grad_heads.size,
            transcendentals=0,
        ),
        name="input_gradient",
    )(grad_heads, grad_one, weights)


def sum_kernel(in_ref, out_ref, first, second, part, send_sem, recv_sem, local_sem, *, sizes):
    barrier = pltpu.get_barrier_semaphore()
    for axis, size in sizes:
        meet_all(barrier, axis, size)
    pl.semaphore_wait(barrier, sum(size - 1 for _, size in sizes))
    for stage, (axis, size) in enumerate(sizes):
        source = in_ref if stage == 0 else part
        into = first if stage == 0 else second
        z = lax.axis_index(axis)
        own = pltpu.make_async_copy(source, into.at[z], local_sem.at[stage])
        own.start()

        def push(k, _):
            pltpu.make_async_remote_copy(
                source,
                into.at[z],
                send_sem.at[stage, k],
                recv_sem.at[stage, z],
                **on(axis, lax.rem(z + k, size)),
            ).start()
            return 0

        def take(k, _):
            d = lax.rem(z + k, size)
            copy = pltpu.make_async_remote_copy(
                source, into.at[d], send_sem.at[stage, k], recv_sem.at[stage, d], **on(axis, d)
            )
            copy.wait_recv()
            copy.wait_send()
            return 0

        lax.fori_loop(1, size, push, 0)
        lax.fori_loop(1, size, take, 0)
        own.wait()
        total = into[0]
        for k in range(1, size):
            total = total + into[k]
        if stage == 0:
            part[...] = total
        else:
            out_ref[...] = total


def sum_everywhere(value, n_dp, n_tensor, call_id):
    vmem = pl.BlockSpec(memory_space=pltpu.VMEM)
    dma = pltpu.SemaphoreType.DMA
    most = max(n_dp, n_tensor)
    return pl.pallas_call(
        functools.partial(sum_kernel, sizes=(("dp", n_dp), ("tensor", n_tensor))),
        out_shape=jax.ShapeDtypeStruct(value.shape, f32),
        in_specs=[vmem],
        out_specs=vmem,
        scratch_shapes=[
            pltpu.VMEM((n_dp,) + value.shape, f32),
            pltpu.VMEM((n_tensor,) + value.shape, f32),
            pltpu.VMEM(value.shape, f32),
            dma((2, most)),
            dma((2, most)),
            dma((2,)),
        ],
        compiler_params=pltpu.CompilerParams(collective_id=call_id, has_side_effects=True),
    )(value)


def lamb_terms(weight, gradient, moments):
    first_moment = 0.5 * moments[0] + 0.5 * gradient
    root_moment = jnp.sqrt(0.5 * moments[1] * moments[1] + 0.5 * gradient * gradient)
    direction = first_moment / (root_moment + moment_eps) + decay_rate * weight
    return (jnp.stack([first_moment, root_moment]), direction)


def piece_sums(tensor_val, stacked):
    squares = tensor_val * tensor_val
    if stacked:
        return jnp.sum(squares.reshape(squares.shape[0], -1), axis=1)
    return jnp.sum(squares).reshape(1)


def local(
    inputs,
    cotangent,
    attn_w,
    out_w,
    glu_w,
    down_w,
    qv_bias,
    vectors,
    attn_mom,
    out_mom,
    glu_mom,
    down_mom,
    qv_mom,
    vector_mom,
    *,
    n_dp,
    n_tensor,
):
    tensor_pos = lax.axis_index("tensor")
    rows = attn_w.shape[1]
    head_cols = attn_w.shape[2]
    head_count = head_cols // HEAD
    width = rows * n_dp
    hidden_cols = glu_w.shape[2]
    tokens = inputs.shape[0]
    length = tokens * n_tensor
    qv_cols = qv_bias.shape[1]
    parts = lax.dynamic_slice_in_dim(
        jnp.asarray(slope_parts(HEADS)), tensor_pos * head_count, head_count
    )

    attn_rows = (
        attn_w.astype(bf16)
        .reshape(3, rows, head_count, HEAD)
        .transpose(1, 2, 0, 3)
        .reshape(rows, 3 * head_cols)
    )
    out_rows = out_w.astype(bf16).T
    glu_rows = glu_w.astype(bf16).transpose(1, 0, 2).reshape(rows, 2 * hidden_cols)
    down_rows = down_w.astype(bf16).T

    small = jnp.concatenate(
        [
            vectors.astype(bf16).T,
            jnp.pad(qv_bias.astype(bf16).reshape(-1), (0, rows - 2 * qv_cols)).reshape(rows, 1),
            jnp.zeros((rows, 57), bf16),
        ],
        axis=1,
    )
    wall_rows = jnp.concatenate(
        [glu_rows, down_rows, jnp.pad(out_rows, ((0, 0), (0, -head_cols % 128)))], axis=1
    )
    wall_chain, own = gather_blocks(
        [wall_rows], [jnp.concatenate([attn_rows, small], axis=1)], n_tensor, n_dp, 0
    )
    own = own.reshape(width, -1)
    first_inputs, own = lax.optimization_barrier((inputs, own))
    (inputs_full,) = gather_blocks([first_inputs], [], n_tensor, n_dp, 1)
    inputs_full = inputs_full.reshape(length, width)
    wall = lax.all_gather(wall_chain, "dp")
    attn_all = lax.all_gather(attn_rows, ("dp", "tensor")).reshape(
        n_dp, n_tensor, rows, -1
    )
    if rows % 16:
        wall, attn_all = [
            w.transpose(1, 0, 2, 3).reshape(1, n_tensor, width, -1) for w in (wall, attn_all)
        ]

    attn_own = own[:, : 3 * head_cols]
    vector_rows = own[:, 3 * head_cols : 3 * head_cols + 6].T.astype(f32)
    qv_rows = (
        own[:, 3 * head_cols + 6]
        .reshape(n_dp, rows)[:, : 2 * qv_cols]
        .reshape(n_dp, 2, qv_cols)
        .transpose(1, 0, 2)
        .reshape(2, head_cols)
        .astype(f32)
    )
    qkv_bias = (
        jnp.stack([qv_rows[0], jnp.zeros_like(qv_rows[0]), qv_rows[1]])
        .reshape(3, head_count, HEAD)
        .transpose(1, 0, 2)
        .reshape(3 * head_cols)
    )

    qkv = (dot(inputs_full, attn_own, 1, 0) + qkv_bias).astype(bf16)
    out_t, lse = attention_forward(parts, qkv)
    sizes = {"dp": n_dp, "tensor": n_tensor}
    (attended,) = collect([("rows", "tensor")], [out_t.reshape(head_cols, length)], sizes, 2)
    output, grad_one, grad_attended, vector_part, grad_glu, grad_rest = feed_forward(
        attended,
        inputs,
        cotangent,
        jnp.pad(vector_rows, ((0, 2), (0, 0))),
        wall,
        head_cols,
        hidden_cols,
    )
    if rows % 16:
        grad_glu, grad_rest = [
            g.reshape(n_tensor, n_dp, rows, -1).transpose(1, 0, 2, 3) for g in (grad_glu, grad_rest)
        ]
    glu_part = lax.psum_scatter(grad_glu, "dp", scatter_dimension=0, tiled=False)
    rest_part = lax.psum_scatter(grad_rest, "dp", scatter_dimension=0, tiled=False)
    vector_all = sum_everywhere(vector_part, n_dp, n_tensor, 5)[:6]
    slice_width = vector_mom.shape[2]
    vector_sum = lax.dynamic_slice_in_dim(
        vector_all, (lax.axis_index("dp") * n_tensor + tensor_pos) * slice_width, slice_width, 1
    )
    grad_tokens, attn_grad, qv_grad = attention_backward(
        parts, qkv, grad_attended, out_t, lse, inputs_full, n_tensor, 6
    )
    qv_grad = qv_grad.reshape(head_count, 3, HEAD)
    qv_grad = jnp.stack([qv_grad[:, 0], qv_grad[:, 2]]).reshape(2, n_dp, qv_cols)
    qv_grad = jnp.pad(
        qv_grad.transpose(1, 0, 2).reshape(n_dp, 1, 2 * qv_cols),
        ((0, 0), (0, 7), (0, -2 * qv_cols % 128)),
    )
    qv_sum, attn_part, glu_sum = collect(
        [("sum", "dp"), ("sum", "dp"), ("sum", "tensor")],
        [qv_grad, attn_grad.reshape(n_dp, rows, -1), glu_part],
        sizes,
        3,
    )
    (rest_sum,) = collect([("sum", "tensor")], [rest_part], sizes, 4)
    glu_sum = glu_sum.reshape(rows, 2, hidden_cols).transpose(1, 0, 2)
    down_sum = rest_sum[:, :hidden_cols].T
    out_sum = rest_sum[:, hidden_cols : hidden_cols + head_cols].T
    attn_sum = (
        attn_part.reshape(rows, head_count, 3, HEAD)
        .transpose(2, 0, 1, 3)
        .reshape(3, rows, head_cols)
    )
    qv_sum = qv_sum[0, : 2 * qv_cols].reshape(2, qv_cols)

    input_grad = input_gradient(grad_tokens, grad_one, attn_all)

    vector_own = lax.dynamic_slice_in_dim(vectors, tensor_pos * slice_width, slice_width, 1)
    owned_parts = (attn_w, out_w, glu_w, down_w, qv_bias, vector_own)
    gradients = (attn_sum, out_sum, glu_sum, down_sum, qv_sum, vector_sum)
    moments = (attn_mom, out_mom, glu_mom, down_mom, qv_mom, vector_mom)
    stack_flags = (True, False, True, False, True, True)
    new_moments = []
    directions = []
    for weight, gradient, moment in zip(owned_parts, gradients, moments):
        pair, direction = lamb_terms(weight, gradient, moment)
        new_moments.append(pair)
        directions.append(direction)
    weight_sums = jnp.concatenate([piece_sums(w, f) for w, f in zip(owned_parts, stack_flags)])
    dir_sums = jnp.concatenate([piece_sums(r, f) for r, f in zip(directions, stack_flags)])
    totals = jnp.pad(jnp.stack([weight_sums, dir_sums]), ((0, 6), (0, 113)))
    totals = sum_everywhere(totals, n_dp, n_tensor, 9)[:2, :15]
    norm_values = jnp.sqrt(totals + 1e-12)
    ratios = norm_values[0] / norm_values[1]
    new_weights = []
    offset = 0
    for weight, direction, stacked in zip(owned_parts, directions, stack_flags):
        amount = weight.shape[0] if stacked else 1
        factor = ratios[offset : offset + amount]
        if stacked:
            factor = factor.reshape((amount,) + (1,) * (weight.ndim - 1))
        else:
            factor = factor[0]
        new_weights.append(weight - learn_rate * factor * direction)
        offset = offset + amount
    return (
        output,
        input_grad,
        *gradients,
        *new_moments,
        *new_weights,
        norm_values,
        ratios,
    )


def solution(mesh):
    tokens = P(("dp", "tensor"), None)
    attn = P(None, "dp", "tensor")
    cols = P("tensor", "dp")
    moments = (
        P(None, None, "dp", "tensor"),
        P(None, "tensor", "dp"),
        P(None, None, "dp", "tensor"),
        P(None, "tensor", "dp"),
        P(None, None, ("tensor", "dp")),
        P(None, None, ("dp", "tensor")),
    )
    weights = (attn, cols, attn, cols, P(None, ("tensor", "dp")))
    split = P(None, ("dp", "tensor"))
    return jax.shard_map(
        functools.partial(local, n_dp=mesh.shape["dp"], n_tensor=mesh.shape["tensor"]),
        mesh=mesh,
        in_specs=(tokens, tokens, *weights, P(None, "dp"), *moments),
        out_specs=(tokens, tokens, *weights, split, *moments, *weights, split, P(), P()),
        check_vma=False,
    )
```

```python
import functools
import math

import jax
import jax.numpy as jnp
import numpy as np
from jax import lax
from jax.experimental import pallas as pl
from jax.experimental.pallas import tpu as pltpu
from jax.sharding import PartitionSpec as P


HEADS = 12
HEAD = 64
BLOCK = 256

norm_eps = 1e-06
learn_rate = 0.2
decay_rate = 0.01
moment_eps = 1e-06


bf16 = jnp.bfloat16
f32 = jnp.float32


def dot(a, b, ca, cb):
    return lax.dot_general(a, b, (((ca,), (cb,)), ((), ())), preferred_element_type=f32)


def slope_parts(head_total):
    power_two = 2 ** int(math.floor(math.log2(head_total)))
    slopes = [2.0 ** (-8.0 * (j + 1) / power_two) for j in range(power_two)]
    slopes += [2.0 ** (-4.0 * (2 * j + 1) / power_two) for j in range(head_total - power_two)]
    rest = np.array(slopes, np.float32)
    parts = []
    for _ in range(3):
        part = rest.astype(bf16).astype(np.float32)
        parts.append(part)
        rest = rest - part
    return np.stack(parts, axis=1)


def pos_features(length, parts):
    row = lax.broadcasted_iota(jnp.int32, (length, HEAD), 0)
    lane = lax.broadcasted_iota(jnp.int32, (length, HEAD), 1)
    low = (row & 7).astype(f32)
    high = row.astype(f32) - low
    m1, m2, m3 = parts
    slope_q = jnp.where(lane < 2, m1, jnp.where(lane < 4, m2, m3))
    for_q = jnp.where(lane < 6, slope_q, jnp.where(lane < 9, high, jnp.where(lane < 12, low, 0.0)))
    turn = lane - 6
    slope_k = jnp.where(
        (turn == 0) | (turn == 3), m1, jnp.where((turn == 1) | (turn == 4), m2, m3)
    )
    for_k = jnp.where(
        lane < 6, jnp.where((lane & 1) == 0, high, low), jnp.where(lane < 12, -slope_k, 0.0)
    )
    return for_q, for_k


def key_after_query(block):
    late = lax.broadcasted_iota(jnp.int32, (block, block), 0) - lax.broadcasted_iota(
        jnp.int32, (block, block), 1
    )
    return jnp.maximum(late, 0).astype(f32)


def fwd_kernel(
    parts_ref, qkv_ref, out_ref, lse_ref, q_s, k_s, v_s, corr_s, s_s, *, heads, length, unroll
):
    amount = length // BLOCK
    for h in range(heads):
        for_q, for_k = pos_features(length, [parts_ref[h, i] for i in range(3)])
        base = h * 3 * HEAD
        q = qkv_ref[:, base : base + HEAD].astype(f32) * HEAD**-0.5
        k = qkv_ref[:, base + HEAD : base + 2 * HEAD].astype(f32)
        v = qkv_ref[:, base + 2 * HEAD : base + 3 * HEAD].astype(f32)
        q_s[h, 0] = jnp.concatenate([q, for_q], axis=1).astype(bf16)
        q_s[h, 1] = jnp.concatenate([q, -for_q], axis=1).astype(bf16)
        k_s[h] = jnp.concatenate([k, for_k], axis=1).astype(bf16)
        v_s[h] = v.T.astype(bf16)
    late = key_after_query(BLOCK)

    def head(h, _):
        corr_s[...] = 2.0 * (parts_ref[h, 0] + parts_ref[h, 1] + parts_ref[h, 2]) * late

        def group(g, _):
            for u in range(unroll):
                b = g * unroll + u
                rows = pl.ds(pl.multiple_of(b * BLOCK, BLOCK), BLOCK)
                for c in range(amount):
                    after = (c > b).astype(jnp.int32)
                    keys = slice(c * BLOCK, (c + 1) * BLOCK)
                    s_s[u, keys, :] = dot(k_s[h, keys, :], q_s[h, after, rows, :], 1, 1)
                s_s[u, rows, :] = s_s[u, rows, :] - corr_s[...]
            for u in range(unroll):
                b = g * unroll + u
                rows = pl.ds(pl.multiple_of(b * BLOCK, BLOCK), BLOCK)
                s = s_s[u]
                top = jnp.max(s, axis=0, keepdims=True)
                p = jnp.exp(s - top)
                total = jnp.sum(p, axis=0, keepdims=True)
                o = dot(v_s[h], p.astype(bf16), 1, 0)
                out_ref[h, :, rows] = (o / total).astype(bf16)
                lse_ref[h, :, rows] = top + jnp.log(total)
            return 0

        lax.fori_loop(0, amount // unroll, group, 0)
        return 0

    lax.fori_loop(0, heads, head, 0)


def attention_forward(parts, qkv):
    length = qkv.shape[0]
    heads = qkv.shape[1] // (3 * HEAD)
    unroll = 2
    vmem = pl.BlockSpec(memory_space=pltpu.VMEM)
    work = heads * length * length
    return pl.pallas_call(
        functools.partial(fwd_kernel, heads=heads, length=length, unroll=unroll),
        out_shape=(
            jax.ShapeDtypeStruct((heads, HEAD, length), bf16),
            jax.ShapeDtypeStruct((heads, 1, length), f32),
        ),
        in_specs=[pl.BlockSpec(memory_space=pltpu.SMEM), vmem],
        out_specs=(vmem, vmem),
        scratch_shapes=[
            pltpu.VMEM((heads, 2, length, 128), bf16),
            pltpu.VMEM((heads, length, 128), bf16),
            pltpu.VMEM((heads, HEAD, length), bf16),
            pltpu.VMEM((BLOCK, BLOCK), f32),
            pltpu.VMEM((unroll, length, BLOCK), f32),
        ],
        compiler_params=pltpu.CompilerParams(vmem_limit_bytes=40 * 2**20),
        cost_estimate=pl.CostEstimate(
            flops=16 * work * HEAD, bytes_accessed=4 * qkv.size, transcendentals=work
        ),
        name="attention_forward",
    )(parts, qkv)


def on(axis, place):
    if axis == "all":
        n = lax.axis_size("tensor")
        at = {"dp": lax.div(place, n), "tensor": lax.rem(place, n)}
    else:
        at = {axis: place}
    return {"device_id": at, "device_id_type": pl.DeviceIdType.MESH}


def place_on(axis):
    if axis == "all":
        return lax.axis_index("dp") * lax.axis_size("tensor") + lax.axis_index("tensor")
    return lax.axis_index(axis)


def meet_all(barrier, axis, size):
    place = place_on(axis)

    def tell(k, _):
        pl.semaphore_signal(barrier, inc=1, **on(axis, lax.rem(place + k, size)))
        return 0

    lax.fori_loop(1, size, tell, 0)


def bwd_kernel(
    parts_ref,
    qkv_ref,
    own_ref,
    ot_ref,
    lse_ref,
    x_ref,
    grad_ref,
    vec_ref,
    tok_ref,
    dw_ref,
    bias_ref,
    sum_ref,
    vsum_ref,
    q_s,
    qn_s,
    k_s,
    kt_s,
    v_s,
    do_s,
    dot_s,
    corr_s,
    s_s,
    dq_s,
    dk_s,
    dv_s,
    stage_s,
    dwt_s,
    in_send,
    in_recv,
    in_own,
    kv_send,
    kv_recv,
    q_send,
    q_recv,
    out_own,
    first_own,
    first_got,
    second_got,
    load_sem,
    sum_send,
    sum_recv,
    vec_got,
    vec_send,
    vec_recv,
    *,
    heads,
    length,
    unroll,
    size,
    paired,
):
    amount = length // BLOCK
    tokens = length // size
    group = 3 * HEAD
    z = lax.axis_index("tensor")
    barrier = pltpu.get_barrier_semaphore()
    meet_all(barrier, "tensor", size)
    met = size - 1
    if paired:
        p = lax.axis_index("dp")
        x = lax.rem(lax.div(p, 2), 2)
        y = lax.div(p, 4)
        partners = (p + 2 - 4 * x, p + 4 - 8 * y)
        for partner in partners:
            pl.semaphore_signal(barrier, inc=1, **on("dp", partner))
        met += 2
    pl.semaphore_wait(barrier, met)
    part = size // 2

    def blocks(way, place, other):
        index = 2 * other + place if way == 0 else 2 * place + other
        return grad_ref.at[index, way * part : (way + 1) * part]

    def first(way, other):
        place = (x, y)[way]
        return pltpu.make_async_remote_copy(
            blocks(way, 1 - place, other),
            first_got.at[way, other],
            sum_send.at[0, way, other],
            sum_recv.at[0, way, other],
            **on("dp", partners[way]),
        )

    def first_load(way, other):
        return pltpu.make_async_copy(
            blocks(way, (x, y)[way], other), first_own.at[way, other], load_sem.at[way, other]
        )

    def second(way):
        place = (y, x)[way]
        return pltpu.make_async_remote_copy(
            first_got.at[way, 1 - place],
            second_got.at[way],
            sum_send.at[1, way, 0],
            sum_recv.at[1, way, 0],
            **on("dp", partners[1 - way]),
        )

    def telling(k, landing):
        d = lax.rem(z + k, size)
        place = d if landing is None else landing
        return pltpu.make_async_remote_copy(
            vec_ref, vec_got.at[place], vec_send.at[k], vec_recv.at[place], **on("tensor", d)
        )

    def taking(h, k, landing):
        d = lax.rem(z + k, size)
        place = d if landing is None else landing
        return pltpu.make_async_remote_copy(
            own_ref.at[pl.ds(pl.multiple_of((d * heads + h) * HEAD, HEAD), HEAD), :],
            dot_s.at[h, :, pl.ds(pl.multiple_of(place * tokens, 128), tokens)],
            in_send.at[h, k],
            in_recv.at[h, place],
            **on("tensor", d),
        )

    def taking_own(h):
        return pltpu.make_async_copy(
            own_ref.at[pl.ds(pl.multiple_of((z * heads + h) * HEAD, HEAD), HEAD), :],
            dot_s.at[h, :, pl.ds(pl.multiple_of(z * tokens, 128), tokens)],
            in_own.at[h],
        )

    def giving(h, k, landing, keys):
        d = lax.rem(z + k, size)
        place = d if landing is None else landing
        low, count = (HEAD, 2 * HEAD) if keys else (0, HEAD)
        send, recv = (kv_send, kv_recv) if keys else (q_send, q_recv)
        return pltpu.make_async_remote_copy(
            stage_s.at[h, low : low + count, pl.ds(pl.multiple_of(d * tokens, 128), tokens)],
            tok_ref.at[
                pl.ds(pl.multiple_of((place * heads + h) * group + low, HEAD), count), :
            ],
            send.at[h, k],
            recv.at[h, place],
            **on("tensor", d),
        )

    def giving_own(h):
        return pltpu.make_async_copy(
            stage_s.at[h, :, pl.ds(pl.multiple_of(z * tokens, 128), tokens)],
            tok_ref.at[pl.ds(pl.multiple_of((z * heads + h) * group, HEAD), group), :],
            out_own.at[h],
        )

    for h in range(heads):
        for k in range(1, size):
            taking(h, k, z).start()
        taking_own(h).start()
    for k in range(1, size):
        telling(k, z).start()
    if paired:
        for way in range(2):
            for other in range(2):
                first(way, other).start()
                first_load(way, other).start()

    for h in range(heads):
        for_q, for_k = pos_features(length, [parts_ref[h, i] for i in range(3)])
        base = h * group
        q = qkv_ref[:, base : base + HEAD].astype(f32) * HEAD**-0.5
        k = qkv_ref[:, base + HEAD : base + 2 * HEAD].astype(f32)
        v = qkv_ref[:, base + 2 * HEAD : base + 3 * HEAD]
        turned = q.T
        turned_pos = for_q.T
        q_s[h, 0] = jnp.concatenate([turned, turned_pos], axis=0).astype(bf16)
        q_s[h, 1] = jnp.concatenate([turned, -turned_pos], axis=0).astype(bf16)
        qn_s[h] = q.astype(bf16)
        k_s[h] = jnp.concatenate([k, for_k], axis=1).astype(bf16)
        kt_s[h] = k.T.astype(bf16)
        v_s[h] = v
    late = key_after_query(BLOCK)

    def head(h, _):
        corr_s[...] = 2.0 * (parts_ref[h, 0] + parts_ref[h, 1] + parts_ref[h, 2]) * late
        dq_s[...] = jnp.zeros_like(dq_s)
        for k in range(1, size):
            taking(h, k, None).wait_recv()
        taking_own(h).wait()
        grad = dot_s[h].astype(f32)
        do_s[...] = grad.T.astype(bf16)
        centre = jnp.sum(grad * ot_ref[h].astype(f32), axis=0, keepdims=True)
        if paired:

            @pl.when(h == heads - 1)
            def _():
                for way in range(2):
                    second(way).start()

        def owner(i, _):
            g = lax.rem(z + 1 + i, size)
            for u in range(unroll):
                c = g * unroll + u
                rows = pl.ds(pl.multiple_of(c * BLOCK, BLOCK), BLOCK)
                keys = k_s[h, rows, :]
                for i in range(amount):
                    after = (i < c).astype(jnp.int32)
                    cols = slice(i * BLOCK, (i + 1) * BLOCK)
                    s_s[u, :, cols] = dot(keys, q_s[h, after, :, cols], 1, 0)
                s_s[u, :, rows] = s_s[u, :, rows] - corr_s[...]

            for u in range(unroll):
                c = g * unroll + u
                rows = pl.ds(pl.multiple_of(c * BLOCK, BLOCK), BLOCK)
                here = slice(u * BLOCK, (u + 1) * BLOCK)
                p = jnp.exp(s_s[u] - lse_ref[h])
                dp = dot(v_s[h, rows, :], dot_s[h], 1, 0)
                dv_s[here, :] = dot(p.astype(bf16), do_s[...], 1, 0)
                ds = (p * (dp - centre)).astype(bf16)
                dk_s[here, :] = dot(ds, qn_s[h], 1, 0)
                dq_s[...] += dot(kt_s[h, :, rows], ds, 1, 0)
            lanes = pl.ds(pl.multiple_of(g * tokens, 128), tokens)
            stage_s[h, HEAD : 2 * HEAD, lanes] = dk_s[...].T.astype(bf16)
            stage_s[h, 2 * HEAD :, lanes] = dv_s[...].T.astype(bf16)
            return 0

        lax.fori_loop(0, size, owner, 0)
        stage_s[h, :HEAD] = (dq_s[...] * HEAD**-0.5).astype(bf16)
        dwt_s[h] = dot(stage_s[h], x_ref[...], 1, 0)
        bias_ref[h] = jnp.sum(stage_s[h].astype(f32), axis=1, keepdims=True)
        for k in range(1, size):
            giving(h, k, z, True).start()
            giving(h, k, z, False).start()
        giving_own(h).start()
        if paired:

            @pl.when(h == heads - 2)
            def _():
                for way in range(2):
                    for other in range(2):
                        first(way, other).wait_recv()
                        first(way, other).wait_send()
                        first_load(way, other).wait()
                        for t in range(part):
                            first_got[way, other, t] = (
                                first_got[way, other, t].astype(f32)
                                + first_own[way, other, t].astype(f32)
                            ).astype(bf16)

        return 0

    lax.fori_loop(0, heads, head, 0)
    for h in range(heads):
        dw_ref[:, h * group : (h + 1) * group] = dwt_s[h].T.astype(bf16)
    for h in range(heads):
        for k in range(1, size):
            taking(h, k, None).wait_send()
            for keys in (True, False):
                giving(h, k, None, keys).wait_recv()
                giving(h, k, None, keys).wait_send()
        giving_own(h).wait()
    vsum_ref[...] = vec_ref[...]
    for k in range(1, size):
        telling(k, None).wait_recv()
        telling(k, None).wait_send()
        vsum_ref[...] += vec_got[lax.rem(z + k, size)]
    if paired:
        for way in range(2):
            second(way).wait_recv()
            second(way).wait_send()
            place = (y, x)[way]
            for t in range(part):
                sum_ref[way * part + t] = (
                    first_got[way, place, t].astype(f32) + second_got[way, t].astype(f32)
                ).astype(bf16)
    else:
        sum_ref[...] = jnp.zeros_like(sum_ref)


def attention_backward(
    parts, qkv, grad_own, out_t, lse, inputs_full, grad_sums, vector_part, size, paired, call_id
):
    length, width = inputs_full.shape
    heads = qkv.shape[1] // (3 * HEAD)
    tokens = length // size
    unroll = tokens // BLOCK
    half = (2, 2, size // 2) + (grad_sums.shape[2:] if paired else (16, 128))
    vmem = pl.BlockSpec(memory_space=pltpu.VMEM)
    shape = jax.ShapeDtypeStruct
    dma = pltpu.SemaphoreType.DMA
    work = heads * length * length
    return pl.pallas_call(
        functools.partial(
            bwd_kernel, heads=heads, length=length, unroll=unroll, size=size, paired=paired
        ),
        out_shape=(
            shape((size * heads * 3 * HEAD, tokens), bf16),
            shape((width, heads * 3 * HEAD), bf16),
            shape((heads, 3 * HEAD, 1), f32),
            shape((size,) + half[3:], bf16),
            shape(vector_part.shape, f32),
        ),
        in_specs=[pl.BlockSpec(memory_space=pltpu.SMEM)]
        + [vmem] * 5
        + [pl.BlockSpec(memory_space=pl.ANY), vmem],
        out_specs=(vmem,) * 5,
        scratch_shapes=[
            pltpu.VMEM((heads, 2, 128, length), bf16),
            pltpu.VMEM((heads, length, HEAD), bf16),
            pltpu.VMEM((heads, length, 128), bf16),
            pltpu.VMEM((heads, HEAD, length), bf16),
            pltpu.VMEM((heads, length, HEAD), bf16),
            pltpu.VMEM((length, HEAD), bf16),
            pltpu.VMEM((heads, HEAD, length), bf16),
            pltpu.VMEM((BLOCK, BLOCK), f32),
            pltpu.VMEM((unroll, BLOCK, length), f32),
            pltpu.VMEM((HEAD, length), f32),
            pltpu.VMEM((tokens, HEAD), f32),
            pltpu.VMEM((tokens, HEAD), f32),
            pltpu.VMEM((heads, 3 * HEAD, length), bf16),
            pltpu.VMEM((heads, 3 * HEAD, width), f32),
            dma((heads, size)),
            dma((heads, size)),
            dma((heads,)),
            dma((heads, size)),
            dma((heads, size)),
            dma((heads, size)),
            dma((heads, size)),
            dma((heads,)),
            pltpu.VMEM(half, bf16),
            pltpu.VMEM(half, bf16),
            pltpu.VMEM(half[1:], bf16),
            dma((2, 2)),
            dma((2, 2, 2)),
            dma((2, 2, 2)),
            pltpu.VMEM((size,) + vector_part.shape, f32),
            dma((size,)),
            dma((size,)),
        ],
        compiler_params=pltpu.CompilerParams(
            collective_id=call_id, has_side_effects=True, vmem_limit_bytes=56 * 2**20
        ),
        cost_estimate=pl.CostEstimate(
            flops=40 * work * HEAD, bytes_accessed=8 * qkv.size, transcendentals=work
        ),
        name="attention_backward",
    )(parts, qkv, grad_own, out_t, lse, inputs_full, grad_sums, vector_part)


def normed(z):
    center = z - jnp.mean(z, axis=1, keepdims=True)
    scale = lax.rsqrt(jnp.mean(center * center, axis=1, keepdims=True) + norm_eps)
    return center * scale, scale


def norm_back(grad, unit, scale, gain):
    inner = grad * gain
    mean = jnp.mean(inner, axis=1, keepdims=True)
    return scale * (inner - mean - unit * jnp.mean(inner * unit, axis=1, keepdims=True))


def ff_kernel(
    att_ref,
    x_ref,
    cot_ref,
    vec_ref,
    wall_ref,
    out_ref,
    dz1_ref,
    do_ref,
    dvec_ref,
    gall_ref,
    wgu_s,
    wd_s,
    wo_s,
    act_s,
    der_s,
    hid_s,
    atn_s,
    h1_s,
    x1_s,
    h1r_s,
    h1t_s,
    df_s,
    dft_s,
    acc_s,
    sglu_s,
    sdown_s,
    sout_s,
    rglu_s,
    rdown_s,
    rout_s,
    load_sem,
    store_sem,
    pair_send,
    pair_recv,
    *,
    head_cols,
    hid_cols,
    paired,
):
    n_row, n_t, rows = wall_ref.shape[:3]
    width = h1_s.shape[1]
    pad = wo_s.shape[2]
    sizes = (2 * hid_cols, hid_cols, pad)

    def loads(kind, t):
        into = (wgu_s, wd_s, wo_s)[kind]
        low = sum(sizes[:kind])
        return [
            pltpu.make_async_copy(
                wall_ref.at[p, t, :, pl.ds(low, sizes[kind])],
                into.at[t, pl.ds(p * rows, rows), :],
                load_sem.at[kind, t, p],
            )
            for p in range(n_row)
        ]

    staged = (sglu_s, sdown_s, sout_s)
    received = (rglu_s, rdown_s, rout_s)
    n_out = n_row // 2 if paired else n_row
    if paired:
        p = lax.axis_index("dp")
        core = lax.rem(p, 2)
        partner = p + 1 - 2 * core
        barrier = pltpu.get_barrier_semaphore()
        pl.semaphore_signal(barrier, inc=1, **on("dp", partner))
        pl.semaphore_wait(barrier, 1)

    def mine(kind, q, whose):
        return staged[kind].at[pl.ds(pl.multiple_of((2 * q + whose) * rows, 16), rows), :]

    def stores(kind, t):
        low = sum(sizes[:kind])
        return [
            pltpu.make_async_copy(
                received[kind].at[t, pl.ds(q * rows, rows), :]
                if paired
                else staged[kind].at[pl.ds(q * rows, rows), :],
                gall_ref.at[q, t, :, pl.ds(low, sizes[kind])],
                store_sem.at[kind, t, q],
            )
            for q in range(n_out)
        ]

    def swaps(kind, t):
        return [
            pltpu.make_async_remote_copy(
                mine(kind, q, 1 - core),
                received[kind].at[t, pl.ds(q * rows, rows), :],
                pair_send.at[kind, t, q],
                pair_recv.at[kind, t, q],
                **on("dp", partner),
            )
            for q in range(n_out)
        ]

    def begin(kind, t):
        for copy in swaps(kind, t) if paired else stores(kind, t):
            copy.start()

    def finish(kind, t):
        if not paired:
            for copy in stores(kind, t):
                copy.wait()
            return
        for copy in swaps(kind, t):
            copy.wait_send()
            copy.wait_recv()
        for q in range(n_out):
            here = pl.ds(q * rows, rows)
            received[kind][t, here, :] = (
                received[kind][t, here, :].astype(f32) + mine(kind, q, core)[...].astype(f32)
            ).astype(bf16)
        for copy in stores(kind, t):
            copy.start()

    for kind in (2, 0, 1):
        for t in range(n_t):
            for copy in loads(kind, t):
                copy.start()
    for t in range(n_t):
        atn_s[t] = att_ref[t * head_cols : (t + 1) * head_cols, :].astype(f32).T.astype(bf16)
        for copy in loads(2, t):
            copy.wait()
    branch = jnp.zeros_like(acc_s)
    for t in range(n_t):
        branch = branch + dot(atn_s[t], wo_s[t, :, :head_cols], 1, 1)
    x1, r1 = normed(x_ref[...].astype(f32) + branch + vec_ref[0:1, :])
    x1_s[...] = x1
    h1 = x1 * vec_ref[1:2, :] + vec_ref[2:3, :]
    h1_s[...] = h1
    h1r_s[...] = h1.astype(bf16)
    h1t_s[...] = h1.T.astype(bf16)
    acc_s[...] = jnp.zeros_like(acc_s)
    for kind in (0, 1):
        for t in range(n_t):
            for copy in loads(kind, t):
                copy.wait()

    def forward(t, _):
        g = dot(h1r_s[...], wgu_s[t, :, :hid_cols], 1, 0)
        u = dot(h1r_s[...], wgu_s[t, :, hid_cols:], 1, 0)
        below = 0.5 * (1.0 + lax.erf(g * np.float32(math.sqrt(0.5))))
        dense = jnp.exp(-0.5 * g * g) * np.float32(1.0 / math.sqrt(2.0 * math.pi))
        act = g * below
        act_s[t] = act
        der_s[t] = u * (below + g * dense)
        hidden = (act * u).astype(bf16)
        hid_s[t] = hidden
        acc_s[...] += dot(hidden, wd_s[t], 1, 1)
        return 0

    lax.fori_loop(0, n_t, forward, 0)
    x2, r2 = normed(h1_s[...] + acc_s[...] + vec_ref[3:4, :])
    out_ref[...] = (x2 * vec_ref[4:5, :] + vec_ref[5:6, :]).astype(bf16)
    cot = cot_ref[...].astype(f32)
    dz2 = norm_back(cot, x2, r2, vec_ref[4:5, :])
    dvec_ref[3:4, :] = jnp.sum(dz2, axis=0, keepdims=True)
    dvec_ref[4:5, :] = jnp.sum(cot * x2, axis=0, keepdims=True)
    dvec_ref[5:6, :] = jnp.sum(cot, axis=0, keepdims=True)
    df_s[...] = dz2.astype(bf16)
    dft_s[...] = dz2.T.astype(bf16)
    acc_s[...] = dz2

    def backward(t, _):
        @pl.when(t > 0)
        def _():
            finish(1, t - 1)

        sdown_s[...] = dot(dft_s[...], hid_s[t], 1, 0).astype(bf16)
        dh = dot(df_s[...], wd_s[t], 1, 0)
        dg = (dh * der_s[t]).astype(bf16)
        du = (dh * act_s[t]).astype(bf16)
        begin(1, t)

        @pl.when(t > 0)
        def _():
            finish(0, t - 1)

        sglu_s[:, :hid_cols] = dot(h1t_s[...], dg, 1, 0).astype(bf16)
        sglu_s[:, hid_cols:] = dot(h1t_s[...], du, 1, 0).astype(bf16)
        acc_s[...] += dot(dg, wgu_s[t, :, :hid_cols], 1, 1) + dot(du, wgu_s[t, :, hid_cols:], 1, 1)
        begin(0, t)
        return 0

    lax.fori_loop(0, n_t, backward, 0)
    dh1 = acc_s[...]
    x1 = x1_s[...]
    dz1 = norm_back(dh1, x1, r1, vec_ref[1:2, :])
    dvec_ref[0:1, :] = jnp.sum(dz1, axis=0, keepdims=True)
    dvec_ref[1:2, :] = jnp.sum(dh1 * x1, axis=0, keepdims=True)
    dvec_ref[2:3, :] = jnp.sum(dh1, axis=0, keepdims=True)
    dvec_ref[6:8, :] = jnp.zeros((2, width), f32)
    dz1_ref[...] = dz1
    da = dz1.astype(bf16)
    dat = dz1.T.astype(bf16)
    sout_s[...] = jnp.zeros_like(sout_s)
    for t in range(n_t):
        do_ref[t * head_cols : (t + 1) * head_cols, :] = dot(
            da, wo_s[t, :, :head_cols], 1, 0
        ).T.astype(bf16)
        if t > 0:
            finish(2, t - 1)
        sout_s[:, :head_cols] = dot(dat, atn_s[t], 1, 0).astype(bf16)
        if t == 0:
            for kind in (1, 0):
                finish(kind, n_t - 1)
        begin(2, t)
    finish(2, n_t - 1)
    if paired:
        for kind in range(3):
            for t in range(n_t):
                for copy in stores(kind, t):
                    copy.wait()


def feed_forward(attended, inputs, cotangent, vector_rows, wall, head_cols, hid_cols, paired, call_id):
    tokens, width = inputs.shape
    n_row, n_t, rows = wall.shape[:3]
    pad = wall.shape[3] - 3 * hid_cols
    n_out = n_row // 2 if paired else n_row
    held = n_out * rows if paired else 16
    dma = pltpu.SemaphoreType.DMA
    vmem = pl.BlockSpec(memory_space=pltpu.VMEM)
    hbm = pl.BlockSpec(memory_space=pl.ANY)
    shape = jax.ShapeDtypeStruct
    size = tokens * width * n_t
    return pl.pallas_call(
        functools.partial(ff_kernel, head_cols=head_cols, hid_cols=hid_cols, paired=paired),
        out_shape=(
            shape((tokens, width), bf16),
            shape((tokens, width), f32),
            shape((n_t * head_cols, tokens), bf16),
            shape((8, width), f32),
            shape((n_out, n_t, rows, 3 * hid_cols + pad), bf16),
        ),
        in_specs=[vmem] * 4 + [hbm],
        out_specs=(vmem, vmem, vmem, vmem, hbm),
        scratch_shapes=[
            pltpu.VMEM((n_t, width, 2 * hid_cols), bf16),
            pltpu.VMEM((n_t, width, hid_cols), bf16),
            pltpu.VMEM((n_t, width, pad), bf16),
            pltpu.VMEM((n_t, tokens, hid_cols), f32),
            pltpu.VMEM((n_t, tokens, hid_cols), f32),
            pltpu.VMEM((n_t, tokens, hid_cols), bf16),
            pltpu.VMEM((n_t, tokens, head_cols), bf16),
            pltpu.VMEM((tokens, width), f32),
            pltpu.VMEM((tokens, width), f32),
            pltpu.VMEM((tokens, width), bf16),
            pltpu.VMEM((width, tokens), bf16),
            pltpu.VMEM((tokens, width), bf16),
            pltpu.VMEM((width, tokens), bf16),
            pltpu.VMEM((tokens, width), f32),
            pltpu.VMEM((width, 2 * hid_cols), bf16),
            pltpu.VMEM((width, hid_cols), bf16),
            pltpu.VMEM((width, pad), bf16),
            pltpu.VMEM((n_t, held, 2 * hid_cols), bf16),
            pltpu.VMEM((n_t, held, hid_cols), bf16),
            pltpu.VMEM((n_t, held, pad), bf16),
            dma((3, n_t, n_row)),
            dma((3, n_t, n_out)),
            dma((3, n_t, n_out)),
            dma((3, n_t, n_out)),
        ],
        compiler_params=pltpu.CompilerParams(
            collective_id=call_id if paired else None,
            has_side_effects=True,
            vmem_limit_bytes=63 * 2**20,
        ),
        cost_estimate=pl.CostEstimate(
            flops=6 * size * (3 * hid_cols + head_cols),
            bytes_accessed=4 * wall.size,
            transcendentals=2 * tokens * n_t * hid_cols,
        ),
        name="feed_forward",
    )(attended, inputs, cotangent, vector_rows, wall)


def gather_kernel(*refs, n_chain, n_flat, chain, flat):
    ins, refs = refs[: n_chain + n_flat], refs[n_chain + n_flat :]
    outs, refs = refs[: n_chain + n_flat], refs[n_chain + n_flat :]
    send_sem, recv_sem, local_sem, flat_send, flat_recv = refs
    z = lax.axis_index("tensor")
    p = lax.axis_index("dp")
    barrier = pltpu.get_barrier_semaphore()

    @pl.when(z > 0)
    def _():
        pl.semaphore_signal(barrier, inc=1, **on("tensor", z - 1))

    @pl.when(z < chain - 1)
    def _():
        pl.semaphore_signal(barrier, inc=1, **on("tensor", z + 1))

    met = jnp.where(z > 0, 1, 0) + jnp.where(z < chain - 1, 1, 0)
    if n_flat:
        meet_all(barrier, "dp", flat)
        met = met + flat - 1
    pl.semaphore_wait(barrier, met)

    own = []
    for i in range(n_chain):
        own.append(pltpu.make_async_copy(ins[i], outs[i].at[z], local_sem.at[i]))
    for j in range(n_flat):
        i = n_chain + j
        own.append(pltpu.make_async_copy(ins[i], outs[i].at[p], local_sem.at[i]))

        def push(k, _):
            pltpu.make_async_remote_copy(
                ins[i],
                outs[i].at[p],
                flat_send.at[j, k],
                flat_recv.at[j, p],
                **on("dp", lax.rem(p + k, flat)),
            ).start()
            return 0

        lax.fori_loop(1, flat, push, 0)
    for copy in own:
        copy.start()

    def hop(i, way, step):
        block = z - step if way == 0 else z + step
        target = z + 1 if way == 0 else z - 1
        return pltpu.make_async_remote_copy(
            ins[i] if step == 0 else outs[i].at[block],
            outs[i].at[block],
            send_sem.at[i, way, step],
            recv_sem.at[i, block],
            **on("tensor", target),
        )

    def sends(way, step):
        if way == 0:
            return (z < chain - 1) & (z >= step)
        return (z > 0) & (z + step < chain)

    def arrived(i, block):
        pltpu.make_async_remote_copy(
            outs[i].at[block],
            outs[i].at[block],
            send_sem.at[i, 0, 0],
            recv_sem.at[i, block],
            **on("tensor", lax.rem(z + 1, chain)),
        ).wait_recv()

    for i in range(n_chain):
        for step in range(chain - 1):
            for way in range(2):

                @pl.when(sends(way, step))
                def _():
                    if step > 0:
                        arrived(i, z - step if way == 0 else z + step)
                    hop(i, way, step).start()

    for i in range(n_chain):
        for step in range(1, chain):

            @pl.when((z == chain - 1) & (z >= step))
            def _():
                arrived(i, z - step)

            @pl.when((z == 0) & (z + step < chain))
            def _():
                arrived(i, z + step)

        for step in range(chain - 1):
            for way in range(2):

                @pl.when(sends(way, step))
                def _():
                    hop(i, way, step).wait_send()

    for j in range(n_flat):
        i = n_chain + j

        def finish(k, _):
            q = lax.rem(p + k, flat)
            copy = pltpu.make_async_remote_copy(
                ins[i], outs[i].at[q], flat_send.at[j, k], flat_recv.at[j, q], **on("dp", q)
            )
            copy.wait_send()
            copy.wait_recv()
            return 0

        lax.fori_loop(1, flat, finish, 0)
    for copy in own:
        copy.wait()


def gather_blocks(on_chain, to_all, n_tensor, n_dp, call_id):
    arrays = [*on_chain, *to_all]
    sizes = [n_tensor] * len(on_chain) + [n_dp] * len(to_all)
    vmem = pl.BlockSpec(memory_space=pltpu.VMEM)
    hbm = pl.BlockSpec(memory_space=pl.ANY)
    count = len(arrays)
    dma = pltpu.SemaphoreType.DMA
    return pl.pallas_call(
        functools.partial(
            gather_kernel, n_chain=len(on_chain), n_flat=len(to_all), chain=n_tensor, flat=n_dp
        ),
        out_shape=[jax.ShapeDtypeStruct((n,) + a.shape, a.dtype) for n, a in zip(sizes, arrays)],
        in_specs=[vmem] * count,
        out_specs=[hbm] * count,
        scratch_shapes=[
            dma((count, 2, n_tensor)),
            dma((count, n_tensor)),
            dma((count,)),
            dma((max(len(to_all), 1), n_dp)),
            dma((max(len(to_all), 1), n_dp)),
        ],
        compiler_params=pltpu.CompilerParams(collective_id=call_id, has_side_effects=True),
    )(*arrays)


def input_part(heads_ref, grad_ref, w_ref, out_ref, w_s, sem):
    n_row, n_t, rows, cols = w_ref.shape
    loads = [
        pltpu.make_async_copy(
            w_ref.at[p, t], w_s.at[t, pl.ds(p * rows, rows), :], sem.at[t, p]
        )
        for t in range(n_t)
        for p in range(n_row)
    ]
    for load in loads:
        load.start()
    for load in loads:
        load.wait()
    out_ref[...] = grad_ref[...]
    for t in range(n_t):
        part = heads_ref[t * cols : (t + 1) * cols, :].astype(f32).T.astype(bf16)
        out_ref[...] += dot(part, w_s[t], 1, 1)


def collect_kernel(*refs, ops, sizes, beside):
    count = len(ops)
    ins, refs = refs[:count], refs[count:]
    if beside:
        beside_ins, refs = refs[:3], refs[3:]
    outs, refs = refs[:count], refs[count:]
    if beside:
        beside_out, refs = refs[0], refs[1:]
        beside_scratch, refs = refs[-2:], refs[:-2]
    sums = [i for i, (kind, _) in enumerate(ops) if kind == "sum"]
    got = dict(zip(sums, refs))
    send_sem, recv_sem, local_sem = refs[len(sums) :]
    barrier = pltpu.get_barrier_semaphore()
    axes = sorted({axis for _, axis in ops})
    if "all" in axes:
        axes = ["all"]
    for axis in axes:
        meet_all(barrier, axis, sizes[axis])
    pl.semaphore_wait(barrier, sum(sizes[axis] - 1 for axis in axes))

    def cut_lanes(ref, index, size):
        lanes = ref.shape[1] // size
        return ref.at[:, pl.ds(pl.multiple_of(index * lanes, 128), lanes)]

    def cut_rows(ref, index, size):
        rows = ref.shape[0] // size
        return ref.at[pl.ds(pl.multiple_of(index * rows, 16), rows), :]

    def cuts(i, source, target):
        kind, axis = ops[i]
        size = sizes[axis]
        if kind == "rows":
            return cut_lanes(ins[i], source, size), cut_rows(outs[i], target, size)
        if kind == "lanes":
            return cut_rows(ins[i], source, size), cut_lanes(outs[i], target, size)
        return ins[i].at[source], got[i].at[target]

    def copy(i, k, landing):
        axis = ops[i][1]
        d = lax.rem(place_on(axis) + k, sizes[axis])
        place = d if landing is None else landing
        source, target = cuts(i, d, place)
        return pltpu.make_async_remote_copy(
            source, target, send_sem.at[i, k], recv_sem.at[i, place], **on(axis, d)
        )

    def own(i):
        z = place_on(ops[i][1])
        return pltpu.make_async_copy(*cuts(i, z, z), local_sem.at[i])

    for i, (kind, axis) in enumerate(ops):

        def push(k, _):
            copy(i, k, place_on(axis)).start()
            return 0

        lax.fori_loop(1, sizes[axis], push, 0)
        if kind != "sum":
            own(i).start()
    if beside:
        input_part(*beside_ins, beside_out, *beside_scratch)
    for i, (kind, axis) in enumerate(ops):
        if kind == "sum":
            outs[i][...] = ins[i][place_on(axis)].astype(f32)

        def take(k, _):
            copy(i, k, None).wait_recv()
            if kind == "sum":
                outs[i][...] += got[i][lax.rem(place_on(axis) + k, sizes[axis])].astype(f32)
            copy(i, k, None).wait_send()
            return 0

        lax.fori_loop(1, sizes[axis], take, 0)
        if kind != "sum":
            own(i).wait()


def collect(ops, arrays, sizes, call_id, beside=()):
    def shape_of(op, a):
        kind, axis = op
        n = sizes[axis]
        if kind == "rows":
            return jax.ShapeDtypeStruct((a.shape[0] * n, a.shape[1] // n), a.dtype)
        if kind == "lanes":
            return jax.ShapeDtypeStruct((a.shape[0] // n, a.shape[1] * n), a.dtype)
        return jax.ShapeDtypeStruct(a.shape[1:], f32)

    vmem = pl.BlockSpec(memory_space=pltpu.VMEM)
    dma = pltpu.SemaphoreType.DMA
    most = max(sizes[axis] for _, axis in ops)
    count = len(ops)
    out_shape = [shape_of(op, a) for op, a in zip(ops, arrays)]
    in_specs = [vmem] * count
    scratch = [pltpu.VMEM(a.shape, a.dtype) for op, a in zip(ops, arrays) if op[0] == "sum"]
    scratch += [dma((count, most)), dma((count, most)), dma((count,))]
    if beside:
        n_row, n_t, rows, cols = beside[2].shape
        out_shape.append(jax.ShapeDtypeStruct(beside[1].shape, f32))
        in_specs += [vmem, vmem, pl.BlockSpec(memory_space=pl.ANY)]
        scratch += [pltpu.VMEM((n_t, n_row * rows, cols), bf16), dma((n_t, n_row))]
    return pl.pallas_call(
        functools.partial(collect_kernel, ops=ops, sizes=sizes, beside=bool(beside)),
        out_shape=out_shape,
        in_specs=in_specs,
        out_specs=[vmem] * len(out_shape),
        scratch_shapes=scratch,
        compiler_params=pltpu.CompilerParams(
            collective_id=call_id, has_side_effects=True, vmem_limit_bytes=40 * 2**20
        ),
    )(*arrays, *beside)


def sum_kernel(in_ref, out_ref, first, second, part, send_sem, recv_sem, local_sem, *, sizes):
    barrier = pltpu.get_barrier_semaphore()
    for axis, size in sizes:
        meet_all(barrier, axis, size)
    pl.semaphore_wait(barrier, sum(size - 1 for _, size in sizes))
    for stage, (axis, size) in enumerate(sizes):
        source = in_ref if stage == 0 else part
        into = first if stage == 0 else second
        z = lax.axis_index(axis)
        own = pltpu.make_async_copy(source, into.at[z], local_sem.at[stage])
        own.start()

        def push(k, _):
            pltpu.make_async_remote_copy(
                source,
                into.at[z],
                send_sem.at[stage, k],
                recv_sem.at[stage, z],
                **on(axis, lax.rem(z + k, size)),
            ).start()
            return 0

        def take(k, _):
            d = lax.rem(z + k, size)
            copy = pltpu.make_async_remote_copy(
                source, into.at[d], send_sem.at[stage, k], recv_sem.at[stage, d], **on(axis, d)
            )
            copy.wait_recv()
            copy.wait_send()
            return 0

        lax.fori_loop(1, size, push, 0)
        lax.fori_loop(1, size, take, 0)
        own.wait()
        total = into[0]
        for k in range(1, size):
            total = total + into[k]
        if stage == 0:
            part[...] = total
        else:
            out_ref[...] = total


def lane_of(index):
    return lax.broadcasted_iota(jnp.int32, (8, 128), 1) == index


def pieces(refs, stacked):
    out = []
    for i, (ref, many) in enumerate(zip(refs, stacked)):
        two = len(ref.shape) == 2
        for k in range(ref.shape[0] if many else 1):
            out.append((i, (slice(k, k + 1) if two else k) if many else slice(None)))
    return out


def direction_kernel(*refs, count, stacked):
    ins, outs, refs = refs[: 3 * count], refs[3 * count : 5 * count], refs[5 * count :]
    sums_ref, refs = refs[0], refs[1:]
    held, made, in_sem, out_sem = refs[: 3 * count], refs[3 * count : 5 * count], *refs[5 * count :]
    loads = [pltpu.make_async_copy(ins[i], held[i], in_sem.at[i]) for i in range(3 * count)]
    for load in loads:
        load.start()
    stores = [pltpu.make_async_copy(made[i], outs[i], out_sem.at[i]) for i in range(2 * count)]
    row = lax.broadcasted_iota(jnp.int32, (8, 128), 0)
    sums = jnp.zeros((8, 128), f32)
    done = -1
    for index, (i, at) in enumerate(pieces(ins[:count], stacked)):
        if i != done:
            if done >= 0:
                stores[done].start()
                stores[count + done].start()
            for k in range(3):
                loads[k * count + i].wait()
            done = i
        w, g = held[i][at], held[count + i][at]
        old = held[2 * count + i][1, at]
        first = 0.5 * held[2 * count + i][0, at] + 0.5 * g
        root = jnp.sqrt(0.5 * old * old + 0.5 * g * g)
        r = first / (root + moment_eps) + decay_rate * w
        made[i][0, at] = first
        made[i][1, at] = root
        made[count + i][at] = r
        for place, value in enumerate((w, r)):
            total = jnp.sum(jnp.sum(value * value, axis=1, keepdims=True), axis=0, keepdims=True)
            sums = sums + jnp.where(lane_of(index) & (row == place), total, 0.0)
    stores[done].start()
    stores[count + done].start()
    sums_ref[...] = sums
    for store in stores:
        store.wait()


def lamb_directions(weights, grads, moments, stacked):
    vmem = pl.BlockSpec(memory_space=pltpu.VMEM)
    hbm = pl.BlockSpec(memory_space=pl.ANY)
    shape = jax.ShapeDtypeStruct
    count = len(weights)
    dma = pltpu.SemaphoreType.DMA
    made = [*moments, *weights]
    outs = pl.pallas_call(
        functools.partial(direction_kernel, count=count, stacked=stacked),
        out_shape=[shape(a.shape, f32) for a in made] + [shape((8, 128), f32)],
        in_specs=[hbm] * (3 * count),
        out_specs=[hbm] * (2 * count) + [vmem],
        scratch_shapes=[pltpu.VMEM(a.shape, f32) for a in (*weights, *grads, *moments, *made)]
        + [dma((3 * count,)), dma((2 * count,))],
        compiler_params=pltpu.CompilerParams(vmem_limit_bytes=60 * 2**20),
        name="lamb_directions",
    )(*weights, *grads, *moments)
    return outs[:count], outs[count : 2 * count], outs[2 * count]


def update_kernel(*refs, count, stacked, sizes):
    ins, refs = refs[: 2 * count], refs[2 * count :]
    sums_ref, refs = refs[0], refs[1:]
    outs, refs = refs[:count], refs[count:]
    norms_ref, refs = refs[0], refs[1:]
    held, made = refs[: 2 * count], refs[2 * count : 3 * count]
    in_sem, out_sem, total, *rest = refs[3 * count :]
    loads = [pltpu.make_async_copy(ins[i], held[i], in_sem.at[i]) for i in range(2 * count)]
    for load in loads:
        load.start()
    sum_kernel(sums_ref, total, *rest, sizes=sizes)
    norms = jnp.sqrt(total[...] + 1e-12)
    ratios = norms[0:1] / norms[1:2]
    row = lax.broadcasted_iota(jnp.int32, (8, 128), 0)
    norms_ref[...] = jnp.where(row == 2, ratios, norms)
    for load in loads:
        load.wait()
    for index, (i, at) in enumerate(pieces(outs, stacked)):
        factor = jnp.sum(jnp.where(lane_of(index)[0:1], ratios, 0.0), axis=1, keepdims=True)
        made[i][at] = held[i][at] - learn_rate * factor * held[count + i][at]
    stores = [pltpu.make_async_copy(made[i], outs[i], out_sem.at[i]) for i in range(count)]
    for store in stores:
        store.start()
    for store in stores:
        store.wait()


def lamb_update(weights, directions, sums, stacked, n_dp, n_tensor, call_id):
    vmem = pl.BlockSpec(memory_space=pltpu.VMEM)
    hbm = pl.BlockSpec(memory_space=pl.ANY)
    shape = jax.ShapeDtypeStruct
    count = len(weights)
    dma = pltpu.SemaphoreType.DMA
    most = max(n_dp, n_tensor)
    outs = pl.pallas_call(
        functools.partial(
            update_kernel,
            count=count,
            stacked=stacked,
            sizes=(("dp", n_dp), ("tensor", n_tensor)),
        ),
        out_shape=[shape(w.shape, f32) for w in weights] + [shape((8, 128), f32)],
        in_specs=[hbm] * (2 * count) + [vmem],
        out_specs=[hbm] * count + [vmem],
        scratch_shapes=[pltpu.VMEM(a.shape, f32) for a in (*weights, *directions, *weights)]
        + [
            dma((2 * count,)),
            dma((count,)),
            pltpu.VMEM((8, 128), f32),
            pltpu.VMEM((n_dp, 8, 128), f32),
            pltpu.VMEM((n_tensor, 8, 128), f32),
            pltpu.VMEM((8, 128), f32),
            dma((2, most)),
            dma((2, most)),
            dma((2,)),
        ],
        compiler_params=pltpu.CompilerParams(
            collective_id=call_id, has_side_effects=True, vmem_limit_bytes=40 * 2**20
        ),
        name="lamb_update",
    )(*weights, *directions, sums)
    return outs[:count], outs[count]


def local(
    inputs,
    cotangent,
    attn_w,
    out_w,
    glu_w,
    down_w,
    qv_bias,
    vectors,
    attn_mom,
    out_mom,
    glu_mom,
    down_mom,
    qv_mom,
    vector_mom,
    *,
    n_dp,
    n_tensor,
):
    tensor_pos = lax.axis_index("tensor")
    rows = attn_w.shape[1]
    head_cols = attn_w.shape[2]
    head_count = head_cols // HEAD
    width = rows * n_dp
    hidden_cols = glu_w.shape[2]
    tokens = inputs.shape[0]
    length = tokens * n_tensor
    qv_cols = qv_bias.shape[1]
    parts = lax.dynamic_slice_in_dim(
        jnp.asarray(slope_parts(HEADS)), tensor_pos * head_count, head_count
    )

    attn_rows = (
        attn_w.astype(bf16)
        .reshape(3, rows, head_count, HEAD)
        .transpose(1, 2, 0, 3)
        .reshape(rows, 3 * head_cols)
    )
    out_rows = out_w.astype(bf16).T
    glu_rows = glu_w.astype(bf16).transpose(1, 0, 2).reshape(rows, 2 * hidden_cols)
    down_rows = down_w.astype(bf16).T

    small = jnp.concatenate(
        [
            vectors.astype(bf16).T,
            jnp.pad(qv_bias.astype(bf16).reshape(-1), (0, rows - 2 * qv_cols)).reshape(rows, 1),
            jnp.zeros((rows, 57), bf16),
        ],
        axis=1,
    )
    wall_rows = jnp.concatenate(
        [glu_rows, down_rows, jnp.pad(out_rows, ((0, 0), (0, -head_cols % 128)))], axis=1
    )
    wall_chain, own = gather_blocks(
        [wall_rows], [jnp.concatenate([attn_rows, small], axis=1)], n_tensor, n_dp, 0
    )
    own = own.reshape(width, -1)
    first_inputs, own = lax.optimization_barrier((inputs, own))
    (inputs_full,) = gather_blocks([first_inputs], [], n_tensor, n_dp, 1)
    inputs_full = inputs_full.reshape(length, width)
    wall = lax.all_gather(wall_chain, "dp")
    attn_all = lax.all_gather(attn_rows, ("dp", "tensor")).reshape(
        n_dp, n_tensor, rows, -1
    )
    if rows % 16:
        wall, attn_all = [
            w.transpose(1, 0, 2, 3).reshape(1, n_tensor, width, -1) for w in (wall, attn_all)
        ]

    attn_own = own[:, : 3 * head_cols]
    vector_rows = own[:, 3 * head_cols : 3 * head_cols + 6].T.astype(f32)
    qv_rows = (
        own[:, 3 * head_cols + 6]
        .reshape(n_dp, rows)[:, : 2 * qv_cols]
        .reshape(n_dp, 2, qv_cols)
        .transpose(1, 0, 2)
        .reshape(2, head_cols)
        .astype(f32)
    )
    qkv_bias = (
        jnp.stack([qv_rows[0], jnp.zeros_like(qv_rows[0]), qv_rows[1]])
        .reshape(3, head_count, HEAD)
        .transpose(1, 0, 2)
        .reshape(3 * head_cols)
    )

    qkv = (dot(inputs_full, attn_own, 1, 0) + qkv_bias).astype(bf16)
    out_t, lse = attention_forward(parts, qkv)
    sizes = {"dp": n_dp, "tensor": n_tensor, "all": n_dp * n_tensor}
    (attended,) = collect([("rows", "tensor")], [out_t.reshape(head_cols, length)], sizes, 2)
    paired = n_dp == 8 and rows % 16 == 0 and n_tensor % 2 == 0
    output, grad_one, grad_attended, vector_part, grad_all = feed_forward(
        attended,
        inputs,
        cotangent,
        jnp.pad(vector_rows, ((0, 2), (0, 0))),
        wall,
        head_cols,
        hidden_cols,
        paired,
        8,
    )
    slice_width = vector_mom.shape[2]
    grad_tokens, attn_grad, qv_grad, late_part, vector_part = attention_backward(
        parts, qkv, grad_attended, out_t, lse, inputs_full, grad_all, vector_part, n_tensor, paired, 6
    )
    if not paired:
        if rows % 16:
            grad_all = grad_all.reshape(n_tensor, n_dp, rows, -1).transpose(1, 0, 2, 3)
        late_part = lax.psum_scatter(grad_all, "dp", scatter_dimension=0, tiled=False)
    qv_grad = qv_grad.reshape(head_count, 3, HEAD)
    qv_grad = jnp.stack([qv_grad[:, 0], qv_grad[:, 2]]).reshape(2, n_dp, qv_cols)
    qv_grad = jnp.pad(
        qv_grad.transpose(1, 0, 2).reshape(n_dp, 1, 2 * qv_cols),
        ((0, 0), (0, 7), (0, -2 * qv_cols % 128)),
    )
    vector_blocks = jnp.pad(
        vector_part.reshape(8, n_dp, rows).transpose(1, 0, 2), ((0, 0), (0, 0), (0, -rows % 128))
    )
    late_sum, attn_part, qv_sum, vector_sum, input_grad = collect(
        [("sum", "tensor"), ("sum", "dp"), ("sum", "dp"), ("sum", "dp")],
        [late_part, attn_grad.reshape(n_dp, rows, -1), qv_grad, vector_blocks],
        sizes,
        3,
        (grad_tokens, grad_one, attn_all),
    )
    vector_sum = lax.dynamic_slice_in_dim(
        vector_sum[:6], tensor_pos * slice_width, slice_width, 1
    )
    glu_sum = late_sum[:, : 2 * hidden_cols]
    rest_sum = late_sum[:, 2 * hidden_cols :]
    glu_sum = glu_sum.reshape(rows, 2, hidden_cols).transpose(1, 0, 2)
    down_sum = rest_sum[:, :hidden_cols]
    out_sum = rest_sum[:, hidden_cols : hidden_cols + head_cols].T
    attn_sum = (
        attn_part.reshape(rows, head_count, 3, HEAD)
        .transpose(2, 0, 1, 3)
        .reshape(3, rows, head_cols)
    )
    qv_sum = qv_sum[0, : 2 * qv_cols].reshape(2, qv_cols)

    vector_own = lax.dynamic_slice_in_dim(vectors, tensor_pos * slice_width, slice_width, 1)
    owned_parts = (attn_w, out_w, glu_w, down_w.T, qv_bias, vector_own)
    gradients = (attn_sum, out_sum, glu_sum, down_sum, qv_sum, vector_sum)
    moments = (attn_mom, out_mom, glu_mom, down_mom.swapaxes(1, 2), qv_mom, vector_mom)
    stack_flags = (True, False, True, False, True, True)
    new_moments, directions, sums = lamb_directions(owned_parts, gradients, moments, stack_flags)
    new_weights, norms = lamb_update(
        owned_parts, directions, sums, stack_flags, n_dp, n_tensor, 9
    )
    gradients, new_moments, new_weights = [
        (*group[:3], group[3].swapaxes(-1, -2), *group[4:])
        for group in (gradients, new_moments, new_weights)
    ]
    norm_values = norms[:2, :15]
    ratios = norms[2, :15]
    return (
        output,
        input_grad,
        *gradients,
        *new_moments,
        *new_weights,
        norm_values,
        ratios,
    )


def solution(mesh):
    tokens = P(("dp", "tensor"), None)
    attn = P(None, "dp", "tensor")
    cols = P("tensor", "dp")
    moments = (
        P(None, None, "dp", "tensor"),
        P(None, "tensor", "dp"),
        P(None, None, "dp", "tensor"),
        P(None, "tensor", "dp"),
        P(None, None, ("tensor", "dp")),
        P(None, None, ("dp", "tensor")),
    )
    weights = (attn, cols, attn, cols, P(None, ("tensor", "dp")))
    split = P(None, ("dp", "tensor"))
    return jax.shard_map(
        functools.partial(local, n_dp=mesh.shape["dp"], n_tensor=mesh.shape["tensor"]),
        mesh=mesh,
        in_specs=(tokens, tokens, *weights, P(None, "dp"), *moments),
        out_specs=(tokens, tokens, *weights, split, *moments, *weights, split, P(), P()),
        check_vma=False,
    )
```

```python
import functools
import math

import jax
import jax.numpy as jnp
import numpy as np
from jax import lax
from jax.experimental import pallas as pl
from jax.experimental.pallas import tpu as pltpu
from jax.sharding import PartitionSpec as P


HEADS = 12
HEAD = 64
BLOCK = 256

norm_eps = 1e-06
learn_rate = 0.2
decay_rate = 0.01
moment_eps = 1e-06


bf16 = jnp.bfloat16
f32 = jnp.float32


def dot(a, b, ca, cb):
    return lax.dot_general(a, b, (((ca,), (cb,)), ((), ())), preferred_element_type=f32)


def slope_parts(head_total):
    power_two = 2 ** int(math.floor(math.log2(head_total)))
    slopes = [2.0 ** (-8.0 * (j + 1) / power_two) for j in range(power_two)]
    slopes += [2.0 ** (-4.0 * (2 * j + 1) / power_two) for j in range(head_total - power_two)]
    rest = np.array(slopes, np.float32)
    parts = []
    for _ in range(3):
        part = rest.astype(bf16).astype(np.float32)
        parts.append(part)
        rest = rest - part
    return np.stack(parts, axis=1)


def pos_features(length, parts):
    row = lax.broadcasted_iota(jnp.int32, (length, HEAD), 0)
    lane = lax.broadcasted_iota(jnp.int32, (length, HEAD), 1)
    low = (row & 7).astype(f32)
    high = row.astype(f32) - low
    m1, m2, m3 = parts
    slope_q = jnp.where(lane < 2, m1, jnp.where(lane < 4, m2, m3))
    for_q = jnp.where(lane < 6, slope_q, jnp.where(lane < 9, high, jnp.where(lane < 12, low, 0.0)))
    turn = lane - 6
    slope_k = jnp.where(
        (turn == 0) | (turn == 3), m1, jnp.where((turn == 1) | (turn == 4), m2, m3)
    )
    for_k = jnp.where(
        lane < 6, jnp.where((lane & 1) == 0, high, low), jnp.where(lane < 12, -slope_k, 0.0)
    )
    return for_q, for_k


def key_after_query(block):
    late = lax.broadcasted_iota(jnp.int32, (block, block), 0) - lax.broadcasted_iota(
        jnp.int32, (block, block), 1
    )
    return jnp.maximum(late, 0).astype(f32)


def fwd_kernel(
    parts_ref, qkv_ref, out_ref, lse_ref, q_s, k_s, v_s, corr_s, s_s, *, heads, length, unroll
):
    amount = length // BLOCK
    for h in range(heads):
        for_q, for_k = pos_features(length, [parts_ref[h, i] for i in range(3)])
        base = h * 3 * HEAD
        q = qkv_ref[:, base : base + HEAD].astype(f32) * HEAD**-0.5
        k = qkv_ref[:, base + HEAD : base + 2 * HEAD].astype(f32)
        v = qkv_ref[:, base + 2 * HEAD : base + 3 * HEAD].astype(f32)
        q_s[h, 0] = jnp.concatenate([q, for_q], axis=1).astype(bf16)
        q_s[h, 1] = jnp.concatenate([q, -for_q], axis=1).astype(bf16)
        k_s[h] = jnp.concatenate([k, for_k], axis=1).astype(bf16)
        v_s[h] = v.T.astype(bf16)
    late = key_after_query(BLOCK)

    def head(h, _):
        corr_s[...] = 2.0 * (parts_ref[h, 0] + parts_ref[h, 1] + parts_ref[h, 2]) * late

        def group(g, _):
            for u in range(unroll):
                b = g * unroll + u
                rows = pl.ds(pl.multiple_of(b * BLOCK, BLOCK), BLOCK)
                for c in range(amount):
                    after = (c > b).astype(jnp.int32)
                    keys = slice(c * BLOCK, (c + 1) * BLOCK)
                    s_s[u, keys, :] = dot(k_s[h, keys, :], q_s[h, after, rows, :], 1, 1)
                s_s[u, rows, :] = s_s[u, rows, :] - corr_s[...]
            for u in range(unroll):
                b = g * unroll + u
                rows = pl.ds(pl.multiple_of(b * BLOCK, BLOCK), BLOCK)
                s = s_s[u]
                top = jnp.max(s, axis=0, keepdims=True)
                p = jnp.exp(s - top)
                total = jnp.sum(p, axis=0, keepdims=True)
                o = dot(v_s[h], p.astype(bf16), 1, 0)
                out_ref[h, :, rows] = (o / total).astype(bf16)
                lse_ref[h, :, rows] = top + jnp.log(total)
            return 0

        lax.fori_loop(0, amount // unroll, group, 0)
        return 0

    lax.fori_loop(0, heads, head, 0)


def attention_forward(parts, qkv):
    length = qkv.shape[0]
    heads = qkv.shape[1] // (3 * HEAD)
    unroll = 4
    vmem = pl.BlockSpec(memory_space=pltpu.VMEM)
    work = heads * length * length
    return pl.pallas_call(
        functools.partial(fwd_kernel, heads=heads, length=length, unroll=unroll),
        out_shape=(
            jax.ShapeDtypeStruct((heads, HEAD, length), bf16),
            jax.ShapeDtypeStruct((heads, 1, length), f32),
        ),
        in_specs=[pl.BlockSpec(memory_space=pltpu.SMEM), vmem],
        out_specs=(vmem, vmem),
        scratch_shapes=[
            pltpu.VMEM((heads, 2, length, 128), bf16),
            pltpu.VMEM((heads, length, 128), bf16),
            pltpu.VMEM((heads, HEAD, length), bf16),
            pltpu.VMEM((BLOCK, BLOCK), f32),
            pltpu.VMEM((unroll, length, BLOCK), f32),
        ],
        compiler_params=pltpu.CompilerParams(vmem_limit_bytes=40 * 2**20),
        cost_estimate=pl.CostEstimate(
            flops=16 * work * HEAD, bytes_accessed=4 * qkv.size, transcendentals=work
        ),
        name="attention_forward",
    )(parts, qkv)


def on(axis, place):
    if axis == "all":
        n = lax.axis_size("tensor")
        at = {"dp": lax.div(place, n), "tensor": lax.rem(place, n)}
    else:
        at = {axis: place}
    return {"device_id": at, "device_id_type": pl.DeviceIdType.MESH}


def place_on(axis):
    if axis == "all":
        return lax.axis_index("dp") * lax.axis_size("tensor") + lax.axis_index("tensor")
    return lax.axis_index(axis)


def meet_all(barrier, axis, size):
    place = place_on(axis)

    def tell(k, _):
        pl.semaphore_signal(barrier, inc=1, **on(axis, lax.rem(place + k, size)))
        return 0

    lax.fori_loop(1, size, tell, 0)


def bwd_kernel(
    parts_ref,
    qkv_ref,
    own_ref,
    ot_ref,
    lse_ref,
    x_ref,
    grad_ref,
    vec_ref,
    tok_ref,
    dw_ref,
    bias_ref,
    sum_ref,
    vsum_ref,
    q_s,
    qn_s,
    k_s,
    kt_s,
    v_s,
    do_s,
    dot_s,
    corr_s,
    s_s,
    dq_s,
    dk_s,
    dv_s,
    stage_s,
    dwt_s,
    in_send,
    in_recv,
    in_own,
    kv_send,
    kv_recv,
    q_send,
    q_recv,
    out_own,
    first_own,
    first_got,
    second_got,
    load_sem,
    sum_send,
    sum_recv,
    vec_got,
    vec_send,
    vec_recv,
    *,
    heads,
    length,
    unroll,
    size,
    paired,
):
    amount = length // BLOCK
    tokens = length // size
    group = 3 * HEAD
    z = lax.axis_index("tensor")
    barrier = pltpu.get_barrier_semaphore()
    meet_all(barrier, "tensor", size)
    met = size - 1
    if paired:
        p = lax.axis_index("dp")
        x = lax.rem(lax.div(p, 2), 2)
        y = lax.div(p, 4)
        partners = (p + 2 - 4 * x, p + 4 - 8 * y)
        for partner in partners:
            pl.semaphore_signal(barrier, inc=1, **on("dp", partner))
        met += 2
    pl.semaphore_wait(barrier, met)
    part = size // 2

    def blocks(way, place, other):
        index = 2 * other + place if way == 0 else 2 * place + other
        return grad_ref.at[index, way * part : (way + 1) * part]

    def first(way, other):
        place = (x, y)[way]
        return pltpu.make_async_remote_copy(
            blocks(way, 1 - place, other),
            first_got.at[way, other],
            sum_send.at[0, way, other],
            sum_recv.at[0, way, other],
            **on("dp", partners[way]),
        )

    def first_load(way, other):
        return pltpu.make_async_copy(
            blocks(way, (x, y)[way], other), first_own.at[way, other], load_sem.at[way, other]
        )

    def second(way):
        place = (y, x)[way]
        return pltpu.make_async_remote_copy(
            first_got.at[way, 1 - place],
            second_got.at[way],
            sum_send.at[1, way, 0],
            sum_recv.at[1, way, 0],
            **on("dp", partners[1 - way]),
        )

    def telling(k, landing):
        d = lax.rem(z + k, size)
        place = d if landing is None else landing
        return pltpu.make_async_remote_copy(
            vec_ref, vec_got.at[place], vec_send.at[k], vec_recv.at[place], **on("tensor", d)
        )

    def taking(h, k, landing):
        d = lax.rem(z + k, size)
        place = d if landing is None else landing
        return pltpu.make_async_remote_copy(
            own_ref.at[pl.ds(pl.multiple_of((d * heads + h) * HEAD, HEAD), HEAD), :],
            dot_s.at[h, :, pl.ds(pl.multiple_of(place * tokens, 128), tokens)],
            in_send.at[h, k],
            in_recv.at[h, place],
            **on("tensor", d),
        )

    def taking_own(h):
        return pltpu.make_async_copy(
            own_ref.at[pl.ds(pl.multiple_of((z * heads + h) * HEAD, HEAD), HEAD), :],
            dot_s.at[h, :, pl.ds(pl.multiple_of(z * tokens, 128), tokens)],
            in_own.at[h],
        )

    def giving(h, k, landing, keys):
        d = lax.rem(z + k, size)
        place = d if landing is None else landing
        low, count = (HEAD, 2 * HEAD) if keys else (0, HEAD)
        send, recv = (kv_send, kv_recv) if keys else (q_send, q_recv)
        return pltpu.make_async_remote_copy(
            stage_s.at[h, low : low + count, pl.ds(pl.multiple_of(d * tokens, 128), tokens)],
            tok_ref.at[
                pl.ds(pl.multiple_of((place * heads + h) * group + low, HEAD), count), :
            ],
            send.at[h, k],
            recv.at[h, place],
            **on("tensor", d),
        )

    def giving_own(h):
        return pltpu.make_async_copy(
            stage_s.at[h, :, pl.ds(pl.multiple_of(z * tokens, 128), tokens)],
            tok_ref.at[pl.ds(pl.multiple_of((z * heads + h) * group, HEAD), group), :],
            out_own.at[h],
        )

    for h in range(heads):
        for k in range(1, size):
            taking(h, k, z).start()
        taking_own(h).start()
    for k in range(1, size):
        telling(k, z).start()
    if paired:
        for way in range(2):
            for other in range(2):
                first(way, other).start()
                first_load(way, other).start()

    for h in range(heads):
        for_q, for_k = pos_features(length, [parts_ref[h, i] for i in range(3)])
        base = h * group
        q = qkv_ref[:, base : base + HEAD].astype(f32) * HEAD**-0.5
        k = qkv_ref[:, base + HEAD : base + 2 * HEAD].astype(f32)
        v = qkv_ref[:, base + 2 * HEAD : base + 3 * HEAD]
        turned = q.T
        turned_pos = for_q.T
        q_s[h, 0] = jnp.concatenate([turned, turned_pos], axis=0).astype(bf16)
        q_s[h, 1] = jnp.concatenate([turned, -turned_pos], axis=0).astype(bf16)
        qn_s[h] = q.astype(bf16)
        k_s[h] = jnp.concatenate([k, for_k], axis=1).astype(bf16)
        kt_s[h] = k.T.astype(bf16)
        v_s[h] = v
    late = key_after_query(BLOCK)

    def head(h, _):
        corr_s[...] = 2.0 * (parts_ref[h, 0] + parts_ref[h, 1] + parts_ref[h, 2]) * late
        dq_s[...] = jnp.zeros_like(dq_s)
        for k in range(1, size):
            taking(h, k, None).wait_recv()
        taking_own(h).wait()
        grad = dot_s[h].astype(f32)
        do_s[...] = grad.T.astype(bf16)
        centre = jnp.sum(grad * ot_ref[h].astype(f32), axis=0, keepdims=True)
        if paired:

            @pl.when(h == heads - 1)
            def _():
                for way in range(2):
                    second(way).start()

        def owner(i, _):
            g = lax.rem(z + 1 + i, size)
            for u in range(unroll):
                c = g * unroll + u
                rows = pl.ds(pl.multiple_of(c * BLOCK, BLOCK), BLOCK)
                keys = k_s[h, rows, :]
                for i in range(amount):
                    after = (i < c).astype(jnp.int32)
                    cols = slice(i * BLOCK, (i + 1) * BLOCK)
                    s_s[u, :, cols] = dot(keys, q_s[h, after, :, cols], 1, 0)
                s_s[u, :, rows] = s_s[u, :, rows] - corr_s[...]

            for u in range(unroll):
                c = g * unroll + u
                rows = pl.ds(pl.multiple_of(c * BLOCK, BLOCK), BLOCK)
                here = slice(u * BLOCK, (u + 1) * BLOCK)
                p = jnp.exp(s_s[u] - lse_ref[h])
                dp = dot(v_s[h, rows, :], dot_s[h], 1, 0)
                dv_s[here, :] = dot(p.astype(bf16), do_s[...], 1, 0)
                ds = (p * (dp - centre)).astype(bf16)
                dk_s[here, :] = dot(ds, qn_s[h], 1, 0)
                dq_s[...] += dot(kt_s[h, :, rows], ds, 1, 0)
            lanes = pl.ds(pl.multiple_of(g * tokens, 128), tokens)
            stage_s[h, HEAD : 2 * HEAD, lanes] = dk_s[...].T.astype(bf16)
            stage_s[h, 2 * HEAD :, lanes] = dv_s[...].T.astype(bf16)
            return 0

        lax.fori_loop(0, size, owner, 0)
        stage_s[h, :HEAD] = (dq_s[...] * HEAD**-0.5).astype(bf16)
        dwt_s[h] = dot(stage_s[h], x_ref[...], 1, 0)
        bias_ref[h] = jnp.sum(stage_s[h].astype(f32), axis=1, keepdims=True)
        for k in range(1, size):
            giving(h, k, z, True).start()
            giving(h, k, z, False).start()
        giving_own(h).start()
        if paired:

            @pl.when(h == heads - 2)
            def _():
                for way in range(2):
                    for other in range(2):
                        first(way, other).wait_recv()
                        first(way, other).wait_send()
                        first_load(way, other).wait()
                        for t in range(part):
                            first_got[way, other, t] = (
                                first_got[way, other, t].astype(f32)
                                + first_own[way, other, t].astype(f32)
                            ).astype(bf16)

        return 0

    lax.fori_loop(0, heads, head, 0)
    for h in range(heads):
        dw_ref[:, h * group : (h + 1) * group] = dwt_s[h].T.astype(bf16)
    for h in range(heads):
        for k in range(1, size):
            taking(h, k, None).wait_send()
            for keys in (True, False):
                giving(h, k, None, keys).wait_recv()
                giving(h, k, None, keys).wait_send()
        giving_own(h).wait()
    vsum_ref[...] = vec_ref[...]
    for k in range(1, size):
        telling(k, None).wait_recv()
        telling(k, None).wait_send()
        vsum_ref[...] += vec_got[lax.rem(z + k, size)]
    if paired:
        for way in range(2):
            second(way).wait_recv()
            second(way).wait_send()
            place = (y, x)[way]
            for t in range(part):
                sum_ref[way * part + t] = (
                    first_got[way, place, t].astype(f32) + second_got[way, t].astype(f32)
                ).astype(bf16)
    else:
        sum_ref[...] = jnp.zeros_like(sum_ref)


def attention_backward(
    parts, qkv, grad_own, out_t, lse, inputs_full, grad_sums, vector_part, size, paired, call_id
):
    length, width = inputs_full.shape
    heads = qkv.shape[1] // (3 * HEAD)
    tokens = length // size
    unroll = tokens // BLOCK
    half = (2, 2, size // 2) + (grad_sums.shape[2:] if paired else (16, 128))
    vmem = pl.BlockSpec(memory_space=pltpu.VMEM)
    shape = jax.ShapeDtypeStruct
    dma = pltpu.SemaphoreType.DMA
    work = heads * length * length
    return pl.pallas_call(
        functools.partial(
            bwd_kernel, heads=heads, length=length, unroll=unroll, size=size, paired=paired
        ),
        out_shape=(
            shape((size * heads * 3 * HEAD, tokens), bf16),
            shape((width, heads * 3 * HEAD), bf16),
            shape((heads, 3 * HEAD, 1), f32),
            shape((size,) + half[3:], bf16),
            shape(vector_part.shape, f32),
        ),
        in_specs=[pl.BlockSpec(memory_space=pltpu.SMEM)]
        + [vmem] * 5
        + [pl.BlockSpec(memory_space=pl.ANY), vmem],
        out_specs=(vmem,) * 5,
        scratch_shapes=[
            pltpu.VMEM((heads, 2, 128, length), bf16),
            pltpu.VMEM((heads, length, HEAD), bf16),
            pltpu.VMEM((heads, length, 128), bf16),
            pltpu.VMEM((heads, HEAD, length), bf16),
            pltpu.VMEM((heads, length, HEAD), bf16),
            pltpu.VMEM((length, HEAD), bf16),
            pltpu.VMEM((heads, HEAD, length), bf16),
            pltpu.VMEM((BLOCK, BLOCK), f32),
            pltpu.VMEM((unroll, BLOCK, length), f32),
            pltpu.VMEM((HEAD, length), f32),
            pltpu.VMEM((tokens, HEAD), f32),
            pltpu.VMEM((tokens, HEAD), f32),
            pltpu.VMEM((heads, 3 * HEAD, length), bf16),
            pltpu.VMEM((heads, 3 * HEAD, width), f32),
            dma((heads, size)),
            dma((heads, size)),
            dma((heads,)),
            dma((heads, size)),
            dma((heads, size)),
            dma((heads, size)),
            dma((heads, size)),
            dma((heads,)),
            pltpu.VMEM(half, bf16),
            pltpu.VMEM(half, bf16),
            pltpu.VMEM(half[1:], bf16),
            dma((2, 2)),
            dma((2, 2, 2)),
            dma((2, 2, 2)),
            pltpu.VMEM((size,) + vector_part.shape, f32),
            dma((size,)),
            dma((size,)),
        ],
        compiler_params=pltpu.CompilerParams(
            collective_id=call_id, has_side_effects=True, vmem_limit_bytes=56 * 2**20
        ),
        cost_estimate=pl.CostEstimate(
            flops=40 * work * HEAD, bytes_accessed=8 * qkv.size, transcendentals=work
        ),
        name="attention_backward",
    )(parts, qkv, grad_own, out_t, lse, inputs_full, grad_sums, vector_part)


def normed(z):
    center = z - jnp.mean(z, axis=1, keepdims=True)
    scale = lax.rsqrt(jnp.mean(center * center, axis=1, keepdims=True) + norm_eps)
    return center * scale, scale


def norm_back(grad, unit, scale, gain):
    inner = grad * gain
    mean = jnp.mean(inner, axis=1, keepdims=True)
    return scale * (inner - mean - unit * jnp.mean(inner * unit, axis=1, keepdims=True))


def ff_kernel(
    att_ref,
    x_ref,
    cot_ref,
    vec_ref,
    wall_ref,
    out_ref,
    dz1_ref,
    do_ref,
    dvec_ref,
    gall_ref,
    wgu_s,
    wd_s,
    wo_s,
    act_s,
    der_s,
    hid_s,
    atn_s,
    h1_s,
    x1_s,
    h1r_s,
    h1t_s,
    df_s,
    dft_s,
    acc_s,
    sglu_s,
    sdown_s,
    sout_s,
    rglu_s,
    rdown_s,
    rout_s,
    load_sem,
    store_sem,
    pair_send,
    pair_recv,
    *,
    head_cols,
    hid_cols,
    paired,
):
    n_row, n_t, rows = wall_ref.shape[:3]
    width = h1_s.shape[1]
    pad = wo_s.shape[2]
    sizes = (2 * hid_cols, hid_cols, pad)

    def loads(kind, t):
        into = (wgu_s, wd_s, wo_s)[kind]
        low = sum(sizes[:kind])
        return [
            pltpu.make_async_copy(
                wall_ref.at[p, t, :, pl.ds(low, sizes[kind])],
                into.at[t, pl.ds(p * rows, rows), :],
                load_sem.at[kind, t, p],
            )
            for p in range(n_row)
        ]

    staged = (sglu_s, sdown_s, sout_s)
    received = (rglu_s, rdown_s, rout_s)
    n_out = n_row // 2 if paired else n_row
    if paired:
        p = lax.axis_index("dp")
        core = lax.rem(p, 2)
        partner = p + 1 - 2 * core
        barrier = pltpu.get_barrier_semaphore()
        pl.semaphore_signal(barrier, inc=1, **on("dp", partner))
        pl.semaphore_wait(barrier, 1)

    def mine(kind, q, whose):
        return staged[kind].at[pl.ds(pl.multiple_of((2 * q + whose) * rows, 16), rows), :]

    def stores(kind, t):
        low = sum(sizes[:kind])
        return [
            pltpu.make_async_copy(
                received[kind].at[t, pl.ds(q * rows, rows), :]
                if paired
                else staged[kind].at[pl.ds(q * rows, rows), :],
                gall_ref.at[q, t, :, pl.ds(low, sizes[kind])],
                store_sem.at[kind, t, q],
            )
            for q in range(n_out)
        ]

    def swaps(kind, t):
        return [
            pltpu.make_async_remote_copy(
                mine(kind, q, 1 - core),
                received[kind].at[t, pl.ds(q * rows, rows), :],
                pair_send.at[kind, t, q],
                pair_recv.at[kind, t, q],
                **on("dp", partner),
            )
            for q in range(n_out)
        ]

    def begin(kind, t):
        for copy in swaps(kind, t) if paired else stores(kind, t):
            copy.start()

    def finish(kind, t):
        if not paired:
            for copy in stores(kind, t):
                copy.wait()
            return
        for copy in swaps(kind, t):
            copy.wait_send()
            copy.wait_recv()
        for q in range(n_out):
            here = pl.ds(q * rows, rows)
            received[kind][t, here, :] = (
                received[kind][t, here, :].astype(f32) + mine(kind, q, core)[...].astype(f32)
            ).astype(bf16)
        for copy in stores(kind, t):
            copy.start()

    for kind in (2, 0, 1):
        for t in range(n_t):
            for copy in loads(kind, t):
                copy.start()
    for t in range(n_t):
        atn_s[t] = att_ref[t * head_cols : (t + 1) * head_cols, :].astype(f32).T.astype(bf16)
        for copy in loads(2, t):
            copy.wait()
    branch = jnp.zeros_like(acc_s)
    for t in range(n_t):
        branch = branch + dot(atn_s[t], wo_s[t, :, :head_cols], 1, 1)
    x1, r1 = normed(x_ref[...].astype(f32) + branch + vec_ref[0:1, :])
    x1_s[...] = x1
    h1 = x1 * vec_ref[1:2, :] + vec_ref[2:3, :]
    h1_s[...] = h1
    h1r_s[...] = h1.astype(bf16)
    h1t_s[...] = h1.T.astype(bf16)
    acc_s[...] = jnp.zeros_like(acc_s)
    for kind in (0, 1):
        for t in range(n_t):
            for copy in loads(kind, t):
                copy.wait()

    def forward(t, _):
        g = dot(h1r_s[...], wgu_s[t, :, :hid_cols], 1, 0)
        u = dot(h1r_s[...], wgu_s[t, :, hid_cols:], 1, 0)
        below = 0.5 * (1.0 + lax.erf(g * np.float32(math.sqrt(0.5))))
        dense = jnp.exp(-0.5 * g * g) * np.float32(1.0 / math.sqrt(2.0 * math.pi))
        act = g * below
        act_s[t] = act
        der_s[t] = u * (below + g * dense)
        hidden = (act * u).astype(bf16)
        hid_s[t] = hidden
        acc_s[...] += dot(hidden, wd_s[t], 1, 1)
        return 0

    lax.fori_loop(0, n_t, forward, 0)
    x2, r2 = normed(h1_s[...] + acc_s[...] + vec_ref[3:4, :])
    out_ref[...] = (x2 * vec_ref[4:5, :] + vec_ref[5:6, :]).astype(bf16)
    cot = cot_ref[...].astype(f32)
    dz2 = norm_back(cot, x2, r2, vec_ref[4:5, :])
    dvec_ref[3:4, :] = jnp.sum(dz2, axis=0, keepdims=True)
    dvec_ref[4:5, :] = jnp.sum(cot * x2, axis=0, keepdims=True)
    dvec_ref[5:6, :] = jnp.sum(cot, axis=0, keepdims=True)
    df_s[...] = dz2.astype(bf16)
    dft_s[...] = dz2.T.astype(bf16)
    acc_s[...] = dz2

    def backward(t, _):
        @pl.when(t > 0)
        def _():
            finish(1, t - 1)

        sdown_s[...] = dot(dft_s[...], hid_s[t], 1, 0).astype(bf16)
        dh = dot(df_s[...], wd_s[t], 1, 0)
        dg = (dh * der_s[t]).astype(bf16)
        du = (dh * act_s[t]).astype(bf16)
        begin(1, t)

        @pl.when(t > 0)
        def _():
            finish(0, t - 1)

        sglu_s[:, :hid_cols] = dot(h1t_s[...], dg, 1, 0).astype(bf16)
        sglu_s[:, hid_cols:] = dot(h1t_s[...], du, 1, 0).astype(bf16)
        acc_s[...] += dot(dg, wgu_s[t, :, :hid_cols], 1, 1) + dot(du, wgu_s[t, :, hid_cols:], 1, 1)
        begin(0, t)
        return 0

    lax.fori_loop(0, n_t, backward, 0)
    dh1 = acc_s[...]
    x1 = x1_s[...]
    dz1 = norm_back(dh1, x1, r1, vec_ref[1:2, :])
    dvec_ref[0:1, :] = jnp.sum(dz1, axis=0, keepdims=True)
    dvec_ref[1:2, :] = jnp.sum(dh1 * x1, axis=0, keepdims=True)
    dvec_ref[2:3, :] = jnp.sum(dh1, axis=0, keepdims=True)
    dvec_ref[6:8, :] = jnp.zeros((2, width), f32)
    dz1_ref[...] = dz1
    da = dz1.astype(bf16)
    dat = dz1.T.astype(bf16)
    sout_s[...] = jnp.zeros_like(sout_s)
    for t in range(n_t):
        do_ref[t * head_cols : (t + 1) * head_cols, :] = dot(
            da, wo_s[t, :, :head_cols], 1, 0
        ).T.astype(bf16)
        if t > 0:
            finish(2, t - 1)
        sout_s[:, :head_cols] = dot(dat, atn_s[t], 1, 0).astype(bf16)
        if t == 0:
            for kind in (1, 0):
                finish(kind, n_t - 1)
        begin(2, t)
    finish(2, n_t - 1)
    if paired:
        for kind in range(3):
            for t in range(n_t):
                for copy in stores(kind, t):
                    copy.wait()


def feed_forward(attended, inputs, cotangent, vector_rows, wall, head_cols, hid_cols, paired, call_id):
    tokens, width = inputs.shape
    n_row, n_t, rows = wall.shape[:3]
    pad = wall.shape[3] - 3 * hid_cols
    n_out = n_row // 2 if paired else n_row
    held = n_out * rows if paired else 16
    dma = pltpu.SemaphoreType.DMA
    vmem = pl.BlockSpec(memory_space=pltpu.VMEM)
    hbm = pl.BlockSpec(memory_space=pl.ANY)
    shape = jax.ShapeDtypeStruct
    size = tokens * width * n_t
    return pl.pallas_call(
        functools.partial(ff_kernel, head_cols=head_cols, hid_cols=hid_cols, paired=paired),
        out_shape=(
            shape((tokens, width), bf16),
            shape((tokens, width), f32),
            shape((n_t * head_cols, tokens), bf16),
            shape((8, width), f32),
            shape((n_out, n_t, rows, 3 * hid_cols + pad), bf16),
        ),
        in_specs=[vmem] * 4 + [hbm],
        out_specs=(vmem, vmem, vmem, vmem, hbm),
        scratch_shapes=[
            pltpu.VMEM((n_t, width, 2 * hid_cols), bf16),
            pltpu.VMEM((n_t, width, hid_cols), bf16),
            pltpu.VMEM((n_t, width, pad), bf16),
            pltpu.VMEM((n_t, tokens, hid_cols), f32),
            pltpu.VMEM((n_t, tokens, hid_cols), f32),
            pltpu.VMEM((n_t, tokens, hid_cols), bf16),
            pltpu.VMEM((n_t, tokens, head_cols), bf16),
            pltpu.VMEM((tokens, width), f32),
            pltpu.VMEM((tokens, width), f32),
            pltpu.VMEM((tokens, width), bf16),
            pltpu.VMEM((width, tokens), bf16),
            pltpu.VMEM((tokens, width), bf16),
            pltpu.VMEM((width, tokens), bf16),
            pltpu.VMEM((tokens, width), f32),
            pltpu.VMEM((width, 2 * hid_cols), bf16),
            pltpu.VMEM((width, hid_cols), bf16),
            pltpu.VMEM((width, pad), bf16),
            pltpu.VMEM((n_t, held, 2 * hid_cols), bf16),
            pltpu.VMEM((n_t, held, hid_cols), bf16),
            pltpu.VMEM((n_t, held, pad), bf16),
            dma((3, n_t, n_row)),
            dma((3, n_t, n_out)),
            dma((3, n_t, n_out)),
            dma((3, n_t, n_out)),
        ],
        compiler_params=pltpu.CompilerParams(
            collective_id=call_id if paired else None,
            has_side_effects=True,
            vmem_limit_bytes=63 * 2**20,
        ),
        cost_estimate=pl.CostEstimate(
            flops=6 * size * (3 * hid_cols + head_cols),
            bytes_accessed=4 * wall.size,
            transcendentals=2 * tokens * n_t * hid_cols,
        ),
        name="feed_forward",
    )(attended, inputs, cotangent, vector_rows, wall)


def gather_kernel(*refs, n_chain, n_flat, chain, flat):
    ins, refs = refs[: n_chain + n_flat], refs[n_chain + n_flat :]
    outs, refs = refs[: n_chain + n_flat], refs[n_chain + n_flat :]
    send_sem, recv_sem, local_sem, flat_send, flat_recv = refs
    z = lax.axis_index("tensor")
    p = lax.axis_index("dp")
    barrier = pltpu.get_barrier_semaphore()

    @pl.when(z > 0)
    def _():
        pl.semaphore_signal(barrier, inc=1, **on("tensor", z - 1))

    @pl.when(z < chain - 1)
    def _():
        pl.semaphore_signal(barrier, inc=1, **on("tensor", z + 1))

    met = jnp.where(z > 0, 1, 0) + jnp.where(z < chain - 1, 1, 0)
    if n_flat:
        meet_all(barrier, "dp", flat)
        met = met + flat - 1
    pl.semaphore_wait(barrier, met)

    own = []
    for i in range(n_chain):
        own.append(pltpu.make_async_copy(ins[i], outs[i].at[z], local_sem.at[i]))
    for j in range(n_flat):
        i = n_chain + j
        own.append(pltpu.make_async_copy(ins[i], outs[i].at[p], local_sem.at[i]))

        def push(k, _):
            pltpu.make_async_remote_copy(
                ins[i],
                outs[i].at[p],
                flat_send.at[j, k],
                flat_recv.at[j, p],
                **on("dp", lax.rem(p + k, flat)),
            ).start()
            return 0

        lax.fori_loop(1, flat, push, 0)
    for copy in own:
        copy.start()

    def hop(i, way, step):
        block = z - step if way == 0 else z + step
        target = z + 1 if way == 0 else z - 1
        return pltpu.make_async_remote_copy(
            ins[i] if step == 0 else outs[i].at[block],
            outs[i].at[block],
            send_sem.at[i, way, step],
            recv_sem.at[i, block],
            **on("tensor", target),
        )

    def sends(way, step):
        if way == 0:
            return (z < chain - 1) & (z >= step)
        return (z > 0) & (z + step < chain)

    def arrived(i, block):
        pltpu.make_async_remote_copy(
            outs[i].at[block],
            outs[i].at[block],
            send_sem.at[i, 0, 0],
            recv_sem.at[i, block],
            **on("tensor", lax.rem(z + 1, chain)),
        ).wait_recv()

    for i in range(n_chain):
        for step in range(chain - 1):
            for way in range(2):

                @pl.when(sends(way, step))
                def _():
                    if step > 0:
                        arrived(i, z - step if way == 0 else z + step)
                    hop(i, way, step).start()

    for i in range(n_chain):
        for step in range(1, chain):

            @pl.when((z == chain - 1) & (z >= step))
            def _():
                arrived(i, z - step)

            @pl.when((z == 0) & (z + step < chain))
            def _():
                arrived(i, z + step)

        for step in range(chain - 1):
            for way in range(2):

                @pl.when(sends(way, step))
                def _():
                    hop(i, way, step).wait_send()

    for j in range(n_flat):
        i = n_chain + j

        def finish(k, _):
            q = lax.rem(p + k, flat)
            copy = pltpu.make_async_remote_copy(
                ins[i], outs[i].at[q], flat_send.at[j, k], flat_recv.at[j, q], **on("dp", q)
            )
            copy.wait_send()
            copy.wait_recv()
            return 0

        lax.fori_loop(1, flat, finish, 0)
    for copy in own:
        copy.wait()


def gather_blocks(on_chain, to_all, n_tensor, n_dp, call_id):
    arrays = [*on_chain, *to_all]
    sizes = [n_tensor] * len(on_chain) + [n_dp] * len(to_all)
    vmem = pl.BlockSpec(memory_space=pltpu.VMEM)
    hbm = pl.BlockSpec(memory_space=pl.ANY)
    count = len(arrays)
    dma = pltpu.SemaphoreType.DMA
    return pl.pallas_call(
        functools.partial(
            gather_kernel, n_chain=len(on_chain), n_flat=len(to_all), chain=n_tensor, flat=n_dp
        ),
        out_shape=[jax.ShapeDtypeStruct((n,) + a.shape, a.dtype) for n, a in zip(sizes, arrays)],
        in_specs=[vmem] * count,
        out_specs=[hbm] * count,
        scratch_shapes=[
            dma((count, 2, n_tensor)),
            dma((count, n_tensor)),
            dma((count,)),
            dma((max(len(to_all), 1), n_dp)),
            dma((max(len(to_all), 1), n_dp)),
        ],
        compiler_params=pltpu.CompilerParams(collective_id=call_id, has_side_effects=True),
    )(*arrays)


def input_part(heads_ref, grad_ref, w_ref, out_ref, w_s, sem):
    n_row, n_t, rows, cols = w_ref.shape
    loads = [
        pltpu.make_async_copy(
            w_ref.at[p, t], w_s.at[t, pl.ds(p * rows, rows), :], sem.at[t, p]
        )
        for t in range(n_t)
        for p in range(n_row)
    ]
    for load in loads:
        load.start()
    for load in loads:
        load.wait()
    out_ref[...] = grad_ref[...]
    for t in range(n_t):
        part = heads_ref[t * cols : (t + 1) * cols, :].astype(f32).T.astype(bf16)
        out_ref[...] += dot(part, w_s[t], 1, 1)


def collect_kernel(*refs, ops, sizes, beside):
    count = len(ops)
    ins, refs = refs[:count], refs[count:]
    if beside:
        beside_ins, refs = refs[:3], refs[3:]
    outs, refs = refs[:count], refs[count:]
    if beside:
        beside_out, refs = refs[0], refs[1:]
        beside_scratch, refs = refs[-2:], refs[:-2]
    sums = [i for i, (kind, _) in enumerate(ops) if kind == "sum"]
    got = dict(zip(sums, refs))
    send_sem, recv_sem, local_sem = refs[len(sums) :]
    barrier = pltpu.get_barrier_semaphore()
    axes = sorted({axis for _, axis in ops})
    if "all" in axes:
        axes = ["all"]
    for axis in axes:
        meet_all(barrier, axis, sizes[axis])
    pl.semaphore_wait(barrier, sum(sizes[axis] - 1 for axis in axes))

    def cut_lanes(ref, index, size):
        lanes = ref.shape[1] // size
        return ref.at[:, pl.ds(pl.multiple_of(index * lanes, 128), lanes)]

    def cut_rows(ref, index, size):
        rows = ref.shape[0] // size
        return ref.at[pl.ds(pl.multiple_of(index * rows, 16), rows), :]

    def cuts(i, source, target):
        kind, axis = ops[i]
        size = sizes[axis]
        if kind == "rows":
            return cut_lanes(ins[i], source, size), cut_rows(outs[i], target, size)
        if kind == "lanes":
            return cut_rows(ins[i], source, size), cut_lanes(outs[i], target, size)
        return ins[i].at[source], got[i].at[target]

    def copy(i, k, landing):
        axis = ops[i][1]
        d = lax.rem(place_on(axis) + k, sizes[axis])
        place = d if landing is None else landing
        source, target = cuts(i, d, place)
        return pltpu.make_async_remote_copy(
            source, target, send_sem.at[i, k], recv_sem.at[i, place], **on(axis, d)
        )

    def own(i):
        z = place_on(ops[i][1])
        return pltpu.make_async_copy(*cuts(i, z, z), local_sem.at[i])

    for i, (kind, axis) in enumerate(ops):

        def push(k, _):
            copy(i, k, place_on(axis)).start()
            return 0

        lax.fori_loop(1, sizes[axis], push, 0)
        if kind != "sum":
            own(i).start()
    if beside:
        input_part(*beside_ins, beside_out, *beside_scratch)
    for i, (kind, axis) in enumerate(ops):
        if kind == "sum":
            outs[i][...] = ins[i][place_on(axis)].astype(f32)

        def take(k, _):
            copy(i, k, None).wait_recv()
            if kind == "sum":
                outs[i][...] += got[i][lax.rem(place_on(axis) + k, sizes[axis])].astype(f32)
            copy(i, k, None).wait_send()
            return 0

        lax.fori_loop(1, sizes[axis], take, 0)
        if kind != "sum":
            own(i).wait()


def collect(ops, arrays, sizes, call_id, beside=()):
    def shape_of(op, a):
        kind, axis = op
        n = sizes[axis]
        if kind == "rows":
            return jax.ShapeDtypeStruct((a.shape[0] * n, a.shape[1] // n), a.dtype)
        if kind == "lanes":
            return jax.ShapeDtypeStruct((a.shape[0] // n, a.shape[1] * n), a.dtype)
        return jax.ShapeDtypeStruct(a.shape[1:], f32)

    vmem = pl.BlockSpec(memory_space=pltpu.VMEM)
    dma = pltpu.SemaphoreType.DMA
    most = max(sizes[axis] for _, axis in ops)
    count = len(ops)
    out_shape = [shape_of(op, a) for op, a in zip(ops, arrays)]
    in_specs = [vmem] * count
    scratch = [pltpu.VMEM(a.shape, a.dtype) for op, a in zip(ops, arrays) if op[0] == "sum"]
    scratch += [dma((count, most)), dma((count, most)), dma((count,))]
    if beside:
        n_row, n_t, rows, cols = beside[2].shape
        out_shape.append(jax.ShapeDtypeStruct(beside[1].shape, f32))
        in_specs += [vmem, vmem, pl.BlockSpec(memory_space=pl.ANY)]
        scratch += [pltpu.VMEM((n_t, n_row * rows, cols), bf16), dma((n_t, n_row))]
    return pl.pallas_call(
        functools.partial(collect_kernel, ops=ops, sizes=sizes, beside=bool(beside)),
        out_shape=out_shape,
        in_specs=in_specs,
        out_specs=[vmem] * len(out_shape),
        scratch_shapes=scratch,
        compiler_params=pltpu.CompilerParams(
            collective_id=call_id, has_side_effects=True, vmem_limit_bytes=40 * 2**20
        ),
    )(*arrays, *beside)


def sum_kernel(in_ref, out_ref, first, second, part, send_sem, recv_sem, local_sem, *, sizes):
    barrier = pltpu.get_barrier_semaphore()
    for axis, size in sizes:
        meet_all(barrier, axis, size)
    pl.semaphore_wait(barrier, sum(size - 1 for _, size in sizes))
    for stage, (axis, size) in enumerate(sizes):
        source = in_ref if stage == 0 else part
        into = first if stage == 0 else second
        z = lax.axis_index(axis)
        own = pltpu.make_async_copy(source, into.at[z], local_sem.at[stage])
        own.start()

        def push(k, _):
            pltpu.make_async_remote_copy(
                source,
                into.at[z],
                send_sem.at[stage, k],
                recv_sem.at[stage, z],
                **on(axis, lax.rem(z + k, size)),
            ).start()
            return 0

        def take(k, _):
            d = lax.rem(z + k, size)
            copy = pltpu.make_async_remote_copy(
                source, into.at[d], send_sem.at[stage, k], recv_sem.at[stage, d], **on(axis, d)
            )
            copy.wait_recv()
            copy.wait_send()
            return 0

        lax.fori_loop(1, size, push, 0)
        lax.fori_loop(1, size, take, 0)
        own.wait()
        total = into[0]
        for k in range(1, size):
            total = total + into[k]
        if stage == 0:
            part[...] = total
        else:
            out_ref[...] = total


def lane_of(index):
    return lax.broadcasted_iota(jnp.int32, (8, 128), 1) == index


def pieces(refs, stacked):
    out = []
    for i, (ref, many) in enumerate(zip(refs, stacked)):
        two = len(ref.shape) == 2
        for k in range(ref.shape[0] if many else 1):
            out.append((i, (slice(k, k + 1) if two else k) if many else slice(None)))
    return out


def direction_kernel(*refs, count, stacked):
    ins, outs, refs = refs[: 3 * count], refs[3 * count : 5 * count], refs[5 * count :]
    sums_ref, refs = refs[0], refs[1:]
    held, made, in_sem, out_sem = refs[: 3 * count], refs[3 * count : 5 * count], *refs[5 * count :]
    loads = [pltpu.make_async_copy(ins[i], held[i], in_sem.at[i]) for i in range(3 * count)]
    for load in loads:
        load.start()
    stores = [pltpu.make_async_copy(made[i], outs[i], out_sem.at[i]) for i in range(2 * count)]
    row = lax.broadcasted_iota(jnp.int32, (8, 128), 0)
    sums = jnp.zeros((8, 128), f32)
    done = -1
    for index, (i, at) in enumerate(pieces(ins[:count], stacked)):
        if i != done:
            if done >= 0:
                stores[done].start()
                stores[count + done].start()
            for k in range(3):
                loads[k * count + i].wait()
            done = i
        w, g = held[i][at], held[count + i][at]
        old = held[2 * count + i][1, at]
        first = 0.5 * held[2 * count + i][0, at] + 0.5 * g
        root = jnp.sqrt(0.5 * old * old + 0.5 * g * g)
        r = first / (root + moment_eps) + decay_rate * w
        made[i][0, at] = first
        made[i][1, at] = root
        made[count + i][at] = r
        for place, value in enumerate((w, r)):
            total = jnp.sum(jnp.sum(value * value, axis=1, keepdims=True), axis=0, keepdims=True)
            sums = sums + jnp.where(lane_of(index) & (row == place), total, 0.0)
    stores[done].start()
    stores[count + done].start()
    sums_ref[...] = sums
    for store in stores:
        store.wait()


def lamb_directions(weights, grads, moments, stacked):
    vmem = pl.BlockSpec(memory_space=pltpu.VMEM)
    hbm = pl.BlockSpec(memory_space=pl.ANY)
    shape = jax.ShapeDtypeStruct
    count = len(weights)
    dma = pltpu.SemaphoreType.DMA
    made = [*moments, *weights]
    outs = pl.pallas_call(
        functools.partial(direction_kernel, count=count, stacked=stacked),
        out_shape=[shape(a.shape, f32) for a in made] + [shape((8, 128), f32)],
        in_specs=[hbm] * (3 * count),
        out_specs=[hbm] * (2 * count) + [vmem],
        scratch_shapes=[pltpu.VMEM(a.shape, f32) for a in (*weights, *grads, *moments, *made)]
        + [dma((3 * count,)), dma((2 * count,))],
        compiler_params=pltpu.CompilerParams(vmem_limit_bytes=60 * 2**20),
        name="lamb_directions",
    )(*weights, *grads, *moments)
    return outs[:count], outs[count : 2 * count], outs[2 * count]


def update_kernel(*refs, count, stacked, sizes):
    ins, refs = refs[: 2 * count], refs[2 * count :]
    sums_ref, refs = refs[0], refs[1:]
    outs, refs = refs[:count], refs[count:]
    norms_ref, refs = refs[0], refs[1:]
    held, made = refs[: 2 * count], refs[2 * count : 3 * count]
    in_sem, out_sem, total, *rest = refs[3 * count :]
    loads = [pltpu.make_async_copy(ins[i], held[i], in_sem.at[i]) for i in range(2 * count)]
    for load in loads:
        load.start()
    sum_kernel(sums_ref, total, *rest, sizes=sizes)
    norms = jnp.sqrt(total[...] + 1e-12)
    ratios = norms[0:1] / norms[1:2]
    row = lax.broadcasted_iota(jnp.int32, (8, 128), 0)
    norms_ref[...] = jnp.where(row == 2, ratios, norms)
    for load in loads:
        load.wait()
    for index, (i, at) in enumerate(pieces(outs, stacked)):
        factor = jnp.sum(jnp.where(lane_of(index)[0:1], ratios, 0.0), axis=1, keepdims=True)
        made[i][at] = held[i][at] - learn_rate * factor * held[count + i][at]
    stores = [pltpu.make_async_copy(made[i], outs[i], out_sem.at[i]) for i in range(count)]
    for store in stores:
        store.start()
    for store in stores:
        store.wait()


def lamb_update(weights, directions, sums, stacked, n_dp, n_tensor, call_id):
    vmem = pl.BlockSpec(memory_space=pltpu.VMEM)
    hbm = pl.BlockSpec(memory_space=pl.ANY)
    shape = jax.ShapeDtypeStruct
    count = len(weights)
    dma = pltpu.SemaphoreType.DMA
    most = max(n_dp, n_tensor)
    outs = pl.pallas_call(
        functools.partial(
            update_kernel,
            count=count,
            stacked=stacked,
            sizes=(("dp", n_dp), ("tensor", n_tensor)),
        ),
        out_shape=[shape(w.shape, f32) for w in weights] + [shape((8, 128), f32)],
        in_specs=[hbm] * (2 * count) + [vmem],
        out_specs=[hbm] * count + [vmem],
        scratch_shapes=[pltpu.VMEM(a.shape, f32) for a in (*weights, *directions, *weights)]
        + [
            dma((2 * count,)),
            dma((count,)),
            pltpu.VMEM((8, 128), f32),
            pltpu.VMEM((n_dp, 8, 128), f32),
            pltpu.VMEM((n_tensor, 8, 128), f32),
            pltpu.VMEM((8, 128), f32),
            dma((2, most)),
            dma((2, most)),
            dma((2,)),
        ],
        compiler_params=pltpu.CompilerParams(
            collective_id=call_id, has_side_effects=True, vmem_limit_bytes=40 * 2**20
        ),
        name="lamb_update",
    )(*weights, *directions, sums)
    return outs[:count], outs[count]


def local(
    inputs,
    cotangent,
    attn_w,
    out_w,
    glu_w,
    down_w,
    qv_bias,
    vectors,
    attn_mom,
    out_mom,
    glu_mom,
    down_mom,
    qv_mom,
    vector_mom,
    *,
    n_dp,
    n_tensor,
):
    tensor_pos = lax.axis_index("tensor")
    rows = attn_w.shape[1]
    head_cols = attn_w.shape[2]
    head_count = head_cols // HEAD
    width = rows * n_dp
    hidden_cols = glu_w.shape[2]
    tokens = inputs.shape[0]
    length = tokens * n_tensor
    qv_cols = qv_bias.shape[1]
    parts = lax.dynamic_slice_in_dim(
        jnp.asarray(slope_parts(HEADS)), tensor_pos * head_count, head_count
    )

    attn_rows = (
        attn_w.astype(bf16)
        .reshape(3, rows, head_count, HEAD)
        .transpose(1, 2, 0, 3)
        .reshape(rows, 3 * head_cols)
    )
    out_rows = out_w.astype(bf16).T
    glu_rows = glu_w.astype(bf16).transpose(1, 0, 2).reshape(rows, 2 * hidden_cols)
    down_rows = down_w.astype(bf16).T

    small = jnp.concatenate(
        [
            vectors.astype(bf16).T,
            jnp.pad(qv_bias.astype(bf16).reshape(-1), (0, rows - 2 * qv_cols)).reshape(rows, 1),
            jnp.zeros((rows, 57), bf16),
        ],
        axis=1,
    )
    wall_rows = jnp.concatenate(
        [glu_rows, down_rows, jnp.pad(out_rows, ((0, 0), (0, -head_cols % 128)))], axis=1
    )
    wall_chain, own = gather_blocks(
        [wall_rows], [jnp.concatenate([attn_rows, small], axis=1)], n_tensor, n_dp, 0
    )
    own = own.reshape(width, -1)
    first_inputs, own = lax.optimization_barrier((inputs, own))
    (inputs_full,) = gather_blocks([first_inputs], [], n_tensor, n_dp, 1)
    inputs_full = inputs_full.reshape(length, width)
    wall = lax.all_gather(wall_chain, "dp")
    if rows % 16:
        wall = wall.transpose(1, 0, 2, 3).reshape(1, n_tensor, width, -1)

    attn_own = own[:, : 3 * head_cols]
    vector_rows = own[:, 3 * head_cols : 3 * head_cols + 6].T.astype(f32)
    qv_rows = (
        own[:, 3 * head_cols + 6]
        .reshape(n_dp, rows)[:, : 2 * qv_cols]
        .reshape(n_dp, 2, qv_cols)
        .transpose(1, 0, 2)
        .reshape(2, head_cols)
        .astype(f32)
    )
    qkv_bias = (
        jnp.stack([qv_rows[0], jnp.zeros_like(qv_rows[0]), qv_rows[1]])
        .reshape(3, head_count, HEAD)
        .transpose(1, 0, 2)
        .reshape(3 * head_cols)
    )

    qkv = (dot(inputs_full, attn_own, 1, 0) + qkv_bias).astype(bf16)
    out_t, lse = attention_forward(parts, qkv)
    sizes = {"dp": n_dp, "tensor": n_tensor, "all": n_dp * n_tensor}
    (attended,) = collect([("rows", "tensor")], [out_t.reshape(head_cols, length)], sizes, 2)
    attended, attn_rows = lax.optimization_barrier((attended, attn_rows))
    attn_all = lax.all_gather(attn_rows, ("dp", "tensor")).reshape(
        n_dp, n_tensor, rows, -1
    )
    if rows % 16:
        attn_all = attn_all.transpose(1, 0, 2, 3).reshape(1, n_tensor, width, -1)
    paired = n_dp == 8 and rows % 16 == 0 and n_tensor % 2 == 0
    output, grad_one, grad_attended, vector_part, grad_all = feed_forward(
        attended,
        inputs,
        cotangent,
        jnp.pad(vector_rows, ((0, 2), (0, 0))),
        wall,
        head_cols,
        hidden_cols,
        paired,
        8,
    )
    slice_width = vector_mom.shape[2]
    grad_tokens, attn_grad, qv_grad, late_part, vector_part = attention_backward(
        parts, qkv, grad_attended, out_t, lse, inputs_full, grad_all, vector_part, n_tensor, paired, 6
    )
    if not paired:
        if rows % 16:
            grad_all = grad_all.reshape(n_tensor, n_dp, rows, -1).transpose(1, 0, 2, 3)
        late_part = lax.psum_scatter(grad_all, "dp", scatter_dimension=0, tiled=False)
    qv_grad = qv_grad.reshape(head_count, 3, HEAD)
    qv_grad = jnp.stack([qv_grad[:, 0], qv_grad[:, 2]]).reshape(2, n_dp, qv_cols)
    qv_grad = jnp.pad(
        qv_grad.transpose(1, 0, 2).reshape(n_dp, 1, 2 * qv_cols),
        ((0, 0), (0, 7), (0, -2 * qv_cols % 128)),
    )
    vector_blocks = jnp.pad(
        vector_part.reshape(8, n_dp, rows).transpose(1, 0, 2), ((0, 0), (0, 0), (0, -rows % 128))
    )
    late_sum, attn_part, qv_sum, vector_sum, input_grad = collect(
        [("sum", "tensor"), ("sum", "dp"), ("sum", "dp"), ("sum", "dp")],
        [late_part, attn_grad.reshape(n_dp, rows, -1), qv_grad, vector_blocks],
        sizes,
        3,
        (grad_tokens, grad_one, attn_all),
    )
    vector_sum = lax.dynamic_slice_in_dim(
        vector_sum[:6], tensor_pos * slice_width, slice_width, 1
    )
    glu_sum = late_sum[:, : 2 * hidden_cols]
    rest_sum = late_sum[:, 2 * hidden_cols :]
    glu_sum = glu_sum.reshape(rows, 2, hidden_cols).transpose(1, 0, 2)
    down_sum = rest_sum[:, :hidden_cols]
    out_sum = rest_sum[:, hidden_cols : hidden_cols + head_cols].T
    attn_sum = (
        attn_part.reshape(rows, head_count, 3, HEAD)
        .transpose(2, 0, 1, 3)
        .reshape(3, rows, head_cols)
    )
    qv_sum = qv_sum[0, : 2 * qv_cols].reshape(2, qv_cols)

    vector_own = lax.dynamic_slice_in_dim(vectors, tensor_pos * slice_width, slice_width, 1)
    owned_parts = (attn_w, out_w, glu_w, down_w.T, qv_bias, vector_own)
    gradients = (attn_sum, out_sum, glu_sum, down_sum, qv_sum, vector_sum)
    moments = (attn_mom, out_mom, glu_mom, down_mom.swapaxes(1, 2), qv_mom, vector_mom)
    stack_flags = (True, False, True, False, True, True)
    new_moments, directions, sums = lamb_directions(owned_parts, gradients, moments, stack_flags)
    new_weights, norms = lamb_update(
        owned_parts, directions, sums, stack_flags, n_dp, n_tensor, 9
    )
    gradients, new_moments, new_weights = [
        (*group[:3], group[3].swapaxes(-1, -2), *group[4:])
        for group in (gradients, new_moments, new_weights)
    ]
    norm_values = norms[:2, :15]
    ratios = norms[2, :15]
    return (
        output,
        input_grad,
        *gradients,
        *new_moments,
        *new_weights,
        norm_values,
        ratios,
    )


def solution(mesh):
    tokens = P(("dp", "tensor"), None)
    attn = P(None, "dp", "tensor")
    cols = P("tensor", "dp")
    moments = (
        P(None, None, "dp", "tensor"),
        P(None, "tensor", "dp"),
        P(None, None, "dp", "tensor"),
        P(None, "tensor", "dp"),
        P(None, None, ("tensor", "dp")),
        P(None, None, ("dp", "tensor")),
    )
    weights = (attn, cols, attn, cols, P(None, ("tensor", "dp")))
    split = P(None, ("dp", "tensor"))
    return jax.shard_map(
        functools.partial(local, n_dp=mesh.shape["dp"], n_tensor=mesh.shape["tensor"]),
        mesh=mesh,
        in_specs=(tokens, tokens, *weights, P(None, "dp"), *moments),
        out_specs=(tokens, tokens, *weights, split, *moments, *weights, split, P(), P()),
        check_vma=False,
    )
```
